32 devices in a mesh: seq: 2 (over y), dp: 16 (over z, x, core).
Axes of the slice: x: 2, y: 2, z: 4, core: 2. Of those that a mesh axis runs over, the one named last changes fastest.
Arguments:
- inputs: bfloat16 [16, 2, 1024, 768], P('dp', None, 'seq'), may hold values from -6 to 6
- query_weight: bfloat16 [768, 768], P(('seq', 'dp')), may hold values from -0.21875 to 0.21875
- key_weight: bfloat16 [768, 768], P(('seq', 'dp')), may hold values from -0.21875 to 0.21875
- value_weight: bfloat16 [768, 768], P(('seq', 'dp')), may hold values from -0.21875 to 0.21875
- query_bias: bfloat16 [768], P(('seq', 'dp')), may hold values from -3 to 3
- value_bias: bfloat16 [768], P(('seq', 'dp')), may hold values from -3 to 3
- output_weight: bfloat16 [768, 768], P(('seq', 'dp')), may hold values from -2.5 to 2.5
- output_bias: bfloat16 [768], P(('seq', 'dp')), may hold values from -3 to 3
- first_gain: bfloat16 [768], P(('seq', 'dp')), may hold values from 0.099609375 to 1.8984375
- first_shift: bfloat16 [768], P(('seq', 'dp')), may hold values from -3 to 3
- inner_weight: bfloat16 [768, 3072], P(('seq', 'dp')), may hold values from -0.21875 to 0.21875
- inner_bias: bfloat16 [3072], P(('seq', 'dp')), may hold values from -3 to 3
- outer_weight: bfloat16 [3072, 768], P(('seq', 'dp')), may hold values from -0.109375 to 0.109375
- outer_bias: bfloat16 [768], P(('seq', 'dp')), may hold values from -3 to 3
- second_gain: bfloat16 [768], P(('seq', 'dp')), may hold values from 0.099609375 to 1.8984375
- second_shift: bfloat16 [768], P(('seq', 'dp')), may hold values from -3 to 3
- prefix: int32 [16, 2], P('dp'), may hold values from 102 to 512, as said below
- cotangent: bfloat16 [16, 2, 1024, 768], P('dp', None, 'seq'), may hold values from -6 to 6
Outputs:
- outputs: bfloat16 [16, 2, 1024, 768], P('dp', None, 'seq')
- input_grad: float32 [16, 2, 1024, 768], P('dp', None, 'seq')
- grad_query_weight: float32 [768, 768], P(('seq', 'dp'))
- grad_key_weight: float32 [768, 768], P(('seq', 'dp'))
- grad_value_weight: float32 [768, 768], P(('seq', 'dp'))
- grad_query_bias: float32 [768], P(('seq', 'dp'))
- grad_value_bias: float32 [768], P(('seq', 'dp'))
- grad_output_weight: float32 [768, 768], P(('seq', 'dp'))
- grad_output_bias: float32 [768], P(('seq', 'dp'))
- grad_first_gain: float32 [768], P(('seq', 'dp'))
- grad_first_shift: float32 [768], P(('seq', 'dp'))
- grad_inner_weight: float32 [768, 3072], P(('seq', 'dp'))
- grad_inner_bias: float32 [3072], P(('seq', 'dp'))
- grad_outer_weight: float32 [3072, 768], P(('seq', 'dp'))
- grad_outer_bias: float32 [768], P(('seq', 'dp'))
- grad_second_gain: float32 [768], P(('seq', 'dp'))
- grad_second_shift: float32 [768], P(('seq', 'dp'))
The draws below stay inside these ranges and needn't reach their ends.
Inputs may be any that keep to these rules, and one draw needn't show every extreme that they name: `prefix`: the number of leading tokens of each sequence that attend to one another both ways; some sequence has 512 and some 1024 // 10.
All inputs are finite; a program needn't handle non-finite values.
Results may differ from the reference program's by a relative error of at most 0.017.
Values may be sent and summed in bfloat16 or wider, within the bound.
A program may use at most 384 MiB of HBM per device.

```python
import jax
import jax.numpy as jnp
from jax import lax

D = 768
HEADS = 12
HEAD_DIM = 64
FF = 3072
MB = 2
LENGTH = 1024
GROUPS = 16


def draw_prefix(key, part):
    low_end = LENGTH // 10
    high_end = LENGTH // 2
    values = jax.random.randint(jax.random.fold_in(key, 11), (GROUPS * MB,), low_end, high_end + 1)
    places = jax.random.permutation(jax.random.fold_in(key, 13), GROUPS * MB)
    values = values.at[places[0]].set(high_end).at[places[1]].set(low_end)
    return values.reshape(GROUPS, MB).astype(jnp.int32)


def level_of(own_key, shape, shards, low, top_value):
    def one(axis_at, parts):
        steps = jax.random.uniform(jax.random.fold_in(jax.random.fold_in(own_key, 6), axis_at), (parts,), jnp.float32, low / len(shards), top_value / len(shards))
        return jnp.repeat(jnp.exp(steps), shape[axis_at] // parts).reshape((-1,) + (1,) * (len(shape) - axis_at - 1))

    gain = one(*shards[0])
    for cut in shards[1:]:
        gain = gain * one(*cut)
    return gain


def normal_values(stream_key, extent, scale, reach, split=(), held_as=jnp.bfloat16):
    values = jax.random.normal(stream_key, extent, jnp.float32) * scale
    if len(split) > 0:
        values = level_of(stream_key, extent, split, -0.22, 0.18) * values
    return jnp.clip(values, min=-reach, max=reach).astype(held_as)


def setup_inputs(seed: int = 0) -> dict:
    streams_of = jax.random.split(jax.random.key(seed), 19)
    return {
        "inputs": normal_values(streams_of[0], (GROUPS, MB, LENGTH, D), 1.0, 6.0, ((0, 16), (2, 2))),
        "query_weight": normal_values(streams_of[1], (D, D), D ** -0.5, 0.21875, ((0, 32),)),
        "key_weight": normal_values(streams_of[2], (D, D), D ** -0.5, 0.21875, ((0, 32),)),
        "value_weight": normal_values(streams_of[3], (D, D), D ** -0.5, 0.21875, ((0, 32),)),
        "query_bias": normal_values(streams_of[4], (D,), 0.5, 3.0, ((0, 32),)),
        "value_bias": normal_values(streams_of[5], (D,), 0.5, 3.0, ((0, 32),)),
        "output_weight": normal_values(streams_of[6], (D, D), (D // 128) ** -0.5, 2.5, ((0, 32),)),
        "output_bias": normal_values(streams_of[7], (D,), 0.5, 3.0, ((0, 32),)),
        "first_gain": jnp.clip(1.0 + 0.18 * jax.random.normal(streams_of[8], (D,), jnp.float32), 0.099609375, 1.8984375).astype(jnp.bfloat16),
        "first_shift": normal_values(streams_of[9], (D,), 0.5, 3.0, ((0, 32),)),
        "inner_weight": normal_values(streams_of[10], (D, FF), D ** -0.5, 0.21875, ((0, 32),)),
        "inner_bias": normal_values(streams_of[11], (FF,), 0.5, 3.0, ((0, 32),)),
        "outer_weight": normal_values(streams_of[12], (FF, D), FF ** -0.5, 0.109375, ((0, 32),)),
        "outer_bias": normal_values(streams_of[13], (D,), 0.5, 3.0, ((0, 32),)),
        "second_gain": jnp.clip(1.0 + 0.18 * jax.random.normal(streams_of[14], (D,), jnp.float32), 0.099609375, 1.8984375).astype(jnp.bfloat16),
        "second_shift": normal_values(streams_of[15], (D,), 0.5, 3.0, ((0, 32),)),
        "prefix": draw_prefix(jax.random.fold_in(streams_of[18], 71), 0),
        "cotangent": normal_values(streams_of[17], (GROUPS, MB, LENGTH, D), 1.0, 6.0, ((0, 16), (2, 2))),
    }


@jax.custom_vjp
def low(v):
    return lax.optimization_barrier(v.astype(jnp.bfloat16)).astype(jnp.float32)

@jax.custom_vjp
def low_back(v):
    return v

def low_keep(v):
    return (low(v), None)

def low_pass(kept, grad):
    return (grad,)

def back_keep(v):
    return (v, None)

def back_low(kept, grad):
    return (low(grad),)
low.defvjp(low_keep, low_pass)
low_back.defvjp(back_keep, back_low)
epsilon = 1e-05
highest = lax.Precision.HIGHEST

def matmul(left_side, right_side):
    return jnp.dot(left_side, right_side, precision=highest)

def normalize(hidden, gain_vec, shift_vec):
    center = hidden - lax.optimization_barrier(jnp.mean(hidden, axis=-1, keepdims=True))
    spread = lax.optimization_barrier(jnp.mean(center * center, axis=-1, keepdims=True))
    return center * lax.rsqrt(spread + epsilon) * gain_vec + shift_vec

def attend(queries, key_rows, value_rows, prefix_len):
    length = queries.shape[0]
    block_rows = min(512, length)
    block_count = length // block_rows
    head_keys = key_rows.reshape(length, HEADS, HEAD_DIM)
    head_values = value_rows.reshape(length, HEADS, HEAD_DIM)
    key_pos = jnp.arange(length, dtype=jnp.int32)

    def one_block(block_item):
        query_block, first_row = block_item
        scores = jnp.einsum('qhd,khd->hqk', query_block, head_keys, precision=highest) * 0.125
        query_pos = first_row + jnp.arange(block_rows, dtype=jnp.int32)
        allowed = (key_pos[None, :] <= query_pos[:, None]) | (key_pos[None, :] < prefix_len)
        scores = low_back(jnp.where(allowed[None], scores, -1e+30))
        weights = low(jax.nn.softmax(scores, axis=-1))
        mixed_heads = jnp.einsum('hqk,khd->qhd', weights, head_values, precision=highest)
        return mixed_heads.reshape(block_rows, HEADS * HEAD_DIM)
    first_rows = (jnp.arange(block_count, dtype=jnp.int32) * block_rows).astype(jnp.int32)
    query_blocks = queries.reshape(block_count, block_rows, HEADS, HEAD_DIM)
    mixed_blocks = lax.map(jax.checkpoint(one_block), (query_blocks, first_rows))
    return mixed_blocks.reshape(length, HEADS * HEAD_DIM)

def layer(inputs, prefix_len, params):
    query_weight, key_weight, value_weight, query_bias, value_bias, output_weight, output_bias, first_gain, first_shift, inner_weight, inner_bias, outer_weight, outer_bias, second_gain, second_shift = params
    queries = low_back(low(matmul(inputs, query_weight) + query_bias))
    key_rows = low_back(low(matmul(inputs, key_weight)))
    value_rows = low_back(low(matmul(inputs, value_weight) + value_bias))
    mixed = low_back(low(attend(queries, key_rows, value_rows, prefix_len)))
    branch = low_back(matmul(mixed, output_weight) + output_bias)
    middle = normalize(inputs + branch, first_gain, first_shift)
    inner_act = low_back(matmul(low(middle), inner_weight) + inner_bias)
    hidden = low_back(low(jax.nn.gelu(inner_act, approximate=False)))
    outer_act = low_back(matmul(hidden, outer_weight) + outer_bias)
    return normalize(middle + outer_act, second_gain, second_shift)

def reference(inputs, query_weight, key_weight, value_weight, query_bias, value_bias, output_weight, output_bias, first_gain, first_shift, inner_weight, inner_bias, outer_weight, outer_bias, second_gain, second_shift, prefix, cotangent):
    params = tuple((weight.astype(jnp.float32) for weight in (query_weight, key_weight, value_weight, query_bias, value_bias, output_weight, output_bias, first_gain, first_shift, inner_weight, inner_bias, outer_weight, outer_bias, second_gain, second_shift)))
    model_width = inputs.shape[3]
    seq_length = inputs.shape[2]
    flat_inputs = inputs.reshape(-1, seq_length, model_width).astype(jnp.float32)
    flat_cot = cotangent.reshape(-1, seq_length, model_width).astype(jnp.float32)
    flat_prefix = prefix.reshape(-1).astype(jnp.int32)

    def one_sequence(totals, seq_item):
        seq_in, seq_prefix, seq_cot = seq_item
        result, pull = jax.vjp(lambda values, weights: layer(values, seq_prefix, weights), seq_in, params)
        grad_in, grad_weights = pull(seq_cot)
        totals = jax.tree.map(jnp.add, totals, grad_weights)
        return (totals, (result.astype(jnp.bfloat16), grad_in))
    zero_grads = tuple((jnp.zeros(weight.shape, jnp.float32) for weight in params))
    totals, (results, input_grads) = lax.scan(one_sequence, zero_grads, (flat_inputs, flat_prefix, flat_cot))
    return (results.reshape(inputs.shape), input_grads.reshape(inputs.shape), totals[0], totals[1], totals[2], totals[3], totals[4], totals[5], totals[6], totals[7], totals[8], totals[9], totals[10], totals[11], totals[12], totals[13], totals[14])
```

```python
import jax
import jax.numpy as jnp
from jax import lax
from jax.sharding import PartitionSpec as P

HEADS = 12
HEAD_DIM = 64
EPS = 1e-05
FAR = 1 << 20
BOTH = ("seq", "dp")
F32 = jnp.float32
BF16 = jnp.bfloat16


def dot(a, b):
    return jnp.dot(a, b, preferred_element_type=F32)


def dot_t(a, b):
    return lax.dot_general(a, b, (((1,), (1,)), ((), ())), preferred_element_type=F32)


def t_dot(a, b):
    return lax.dot_general(a, b, (((0,), (0,)), ((), ())), preferred_element_type=F32)


def norm_parts(v):
    center = v - jnp.mean(v, axis=-1, keepdims=True)
    inv = lax.rsqrt(jnp.mean(center * center, axis=-1, keepdims=True) + EPS)
    return center * inv, inv


def norm_grad(grad, unit, inv, gain):
    g = grad * gain
    mean_g = jnp.mean(g, axis=-1, keepdims=True)
    mean_gu = jnp.mean(g * unit, axis=-1, keepdims=True)
    return inv * (g - mean_g - unit * mean_gu)


def heads_of(v):
    return v.reshape(v.shape[0], HEADS, HEAD_DIM)


def attend(q, k, v, key_pos, limit):
    scores = jnp.einsum("qhd,khd->hqk", heads_of(q), heads_of(k), preferred_element_type=F32) * 0.125
    scores = jnp.where((key_pos[None, :] <= limit[:, None])[None], scores, -1e30)
    top = jnp.max(scores, axis=-1, keepdims=True)
    lse = top[..., 0] + jnp.log(jnp.sum(jnp.exp(scores - top), axis=-1))
    probs = jnp.exp(scores - lse[..., None])
    low = probs.astype(BF16)
    mixed = jnp.einsum("hqk,khd->qhd", low, heads_of(v), preferred_element_type=F32)
    return mixed.reshape(q.shape).astype(BF16), (probs, low)


def attend_back(saved, q, k, v, mixed, grad):
    probs, low = saved
    grad_h = heads_of(grad)
    grad_probs = jnp.einsum("qhd,khd->hqk", grad_h, heads_of(v), preferred_element_type=F32)
    row_dot = jnp.sum(grad_probs * probs, axis=-1, keepdims=True)
    grad_scores = (probs * (grad_probs - row_dot)).astype(BF16)
    gq = jnp.einsum("hqk,khd->qhd", grad_scores, heads_of(k), preferred_element_type=F32) * 0.125
    gk = jnp.einsum("hqk,qhd->khd", grad_scores, heads_of(q), preferred_element_type=F32) * 0.125
    gv = jnp.einsum("hqk,qhd->khd", low, grad_h, preferred_element_type=F32)
    return (
        gq.reshape(q.shape).astype(BF16),
        gk.reshape(k.shape).astype(BF16),
        gv.reshape(v.shape).astype(BF16),
    )


def on_device(
    inputs,
    query_weight,
    key_weight,
    value_weight,
    query_bias,
    value_bias,
    output_weight,
    output_bias,
    first_gain,
    first_shift,
    inner_weight,
    inner_bias,
    outer_weight,
    outer_bias,
    second_gain,
    second_shift,
    prefix,
    cotangent,
):
    micros, rows, width = inputs.shape[1:]
    own = query_weight.shape[0]
    hidden_width = inner_weight.shape[1]
    per = hidden_width // width
    seqs = lax.axis_size("seq")
    seq_at = lax.axis_index("seq")
    first_pos = seq_at * rows
    x = inputs[0]
    flat_x = x.reshape(micros * rows, width)
    row_pos = first_pos + jnp.arange(rows, dtype=jnp.int32)

    if seqs == 2:
        before = lax.ppermute(x, "seq", [(0, 1)])
        key_x = jnp.concatenate([x, before], axis=1)
        key_pos = jnp.concatenate(
            [row_pos, jnp.where(seq_at == 1, jnp.arange(rows, dtype=jnp.int32), FAR)]
        )
    else:
        key_x = lax.all_gather(x, "seq", axis=1, tiled=True)
        key_pos = jnp.arange(seqs * rows, dtype=jnp.int32)
    total_rows = key_x.shape[1]
    flat_key_x = key_x.reshape(micros * total_rows, width)

    vectors = (query_bias, value_bias, output_bias, first_gain, first_shift, outer_bias, second_gain, second_shift)
    small = jnp.concatenate(
        [jnp.stack(vectors, axis=1), inner_bias.reshape(own, per)], axis=1
    )
    small_count = small.shape[1]
    small = jnp.pad(small, ((0, 0), (0, 128 - small_count)))
    first_pack = lax.all_gather(
        jnp.concatenate([query_weight, key_weight, value_weight, small], axis=1), BOTH, axis=0, tiled=True
    )
    second_pack = lax.all_gather(
        jnp.concatenate([output_weight, inner_weight], axis=1), BOTH, axis=0, tiled=True
    )
    full_outer = lax.all_gather(outer_weight, BOTH, axis=0, tiled=True)
    full_query = first_pack[:, :width]
    full_kv = first_pack[:, width : 3 * width]
    small_all = first_pack[:, 3 * width : 3 * width + small_count].astype(F32)
    qb, vb, ob, fg, fs, ub, sg, ss = [small_all[:, i] for i in range(8)]
    ib = small_all[:, 8:].reshape(hidden_width)
    full_output = second_pack[:, :width]
    full_inner = second_pack[:, width:]

    queries = (dot(flat_x, full_query) + qb).astype(BF16).reshape(micros, rows, width)
    kv_bias = jnp.concatenate([jnp.zeros_like(vb), vb])
    keys_values = (dot(flat_key_x, full_kv) + kv_bias).astype(BF16).reshape(micros, total_rows, 2 * width)
    keys, values = keys_values[..., :width], keys_values[..., width:]

    mixed_parts, saved = [], []
    for m in range(micros):
        limit = jnp.maximum(row_pos, prefix[0, m] - 1)
        mixed_m, saved_m = attend(queries[m], keys[m], values[m], key_pos, limit)
        mixed_parts.append(mixed_m)
        saved.append(saved_m)
    mixed = jnp.concatenate(mixed_parts, axis=0)

    unit1, inv1 = norm_parts(flat_x.astype(F32) + dot(mixed, full_output) + ob)
    middle = unit1 * fg + fs
    middle_low = middle.astype(BF16)
    inner = dot(middle_low, full_inner) + ib
    half_cdf = 0.5 * (1.0 + lax.erf(inner * (0.5**0.5)))
    hidden = (inner * half_cdf).astype(BF16)
    slope = half_cdf + inner * jnp.exp(-0.5 * inner * inner) * 0.3989422804014327
    unit2, inv2 = norm_parts(middle + dot(hidden, full_outer) + ub)
    result = (unit2 * sg + ss).astype(BF16)

    cot = cotangent[0].reshape(micros * rows, width).astype(F32)
    g_sgain = jnp.sum(cot * unit2, axis=0)
    g_sshift = jnp.sum(cot, axis=0)
    grad_mid2 = norm_grad(cot, unit2, inv2, sg)
    grad_outer = grad_mid2.astype(BF16)
    g_ubias = jnp.sum(grad_outer.astype(F32), axis=0)
    g_outer = t_dot(hidden, grad_outer).astype(BF16)
    own_outer = lax.psum_scatter(g_outer, BOTH, scatter_dimension=0, tiled=True).astype(F32)
    grad_hidden = dot_t(grad_outer, full_outer).astype(BF16)
    grad_inner = (grad_hidden.astype(F32) * slope).astype(BF16)
    g_ibias = jnp.sum(grad_inner.astype(F32), axis=0)
    g_inner = t_dot(middle_low, grad_inner)
    grad_middle = grad_mid2 + dot_t(grad_inner, full_inner)
    g_fgain = jnp.sum(grad_middle * unit1, axis=0)
    g_fshift = jnp.sum(grad_middle, axis=0)
    grad_sum1 = norm_grad(grad_middle, unit1, inv1, fg)
    grad_branch = grad_sum1.astype(BF16)
    g_obias = jnp.sum(grad_branch.astype(F32), axis=0)
    g_output = t_dot(mixed, grad_branch)
    own_second = lax.psum_scatter(
        jnp.concatenate([g_output, g_inner], axis=1).astype(BF16), BOTH, scatter_dimension=0, tiled=True
    ).astype(F32)
    grad_mixed = dot_t(grad_branch, full_output).astype(BF16).reshape(micros, rows, width)

    gq_parts, gk_parts, gv_parts = [], [], []
    for m in range(micros):
        gq, gk, gv = attend_back(
            saved[m], queries[m], keys[m], values[m], mixed_parts[m], grad_mixed[m]
        )
        gq_parts.append(gq)
        gk_parts.append(gk)
        gv_parts.append(gv)
    grad_q = jnp.concatenate(gq_parts, axis=0)
    grad_kv = jnp.concatenate([jnp.stack(gk_parts), jnp.stack(gv_parts)], axis=-1)
    flat_kv = grad_kv.reshape(micros * total_rows, 2 * width)
    g_qbias = jnp.sum(grad_q.astype(F32), axis=0)
    g_vbias = jnp.sum(flat_kv[:, width:].astype(F32), axis=0)
    g_query = t_dot(flat_x, grad_q)
    g_kv = t_dot(flat_key_x, flat_kv)
    g_small = jnp.concatenate(
        [
            jnp.stack([g_qbias, g_vbias, g_obias, g_fgain, g_fshift, g_ubias, g_sgain, g_sshift], axis=1),
            g_ibias.reshape(width, per),
        ],
        axis=1,
    )
    g_small = jnp.pad(g_small, ((0, 0), (0, 128 - small_count)))
    own_first = lax.psum_scatter(
        jnp.concatenate([g_query, g_kv, g_small], axis=1).astype(BF16), BOTH, scatter_dimension=0, tiled=True
    ).astype(F32)

    via_kv = dot_t(flat_kv, full_kv).reshape(micros, total_rows, width)
    grad_x = (grad_sum1 + dot_t(grad_q, full_query)).reshape(micros, rows, width)
    if seqs == 2:
        grad_x = grad_x + via_kv[:, :rows]
        grad_x = grad_x + lax.ppermute(via_kv[:, rows:].astype(BF16), "seq", [(1, 0)]).astype(F32)
    else:
        grad_x = grad_x + lax.psum_scatter(via_kv, "seq", scatter_dimension=1, tiled=True)

    vec = own_first[:, 3 * width : 3 * width + small_count]
    v_of = [vec[:, i] for i in range(8)]
    outputs = result.reshape(micros, rows, width)[None]
    return (
        outputs,
        grad_x[None],
        own_first[:, :width],
        own_first[:, width : 2 * width],
        own_first[:, 2 * width : 3 * width],
        v_of[0],
        v_of[1],
        own_second[:, :width],
        v_of[2],
        v_of[3],
        v_of[4],
        own_second[:, width:],
        vec[:, 8:].reshape(own * per),
        own_outer,
        v_of[5],
        v_of[6],
        v_of[7],
    )


def solution(mesh):
    act = P("dp", None, "seq", None)
    mat = P(BOTH, None)
    vec = P(BOTH)
    params = (mat, mat, mat, vec, vec, mat, vec, vec, vec, mat, vec, mat, vec, vec, vec)
    return jax.shard_map(
        on_device,
        mesh=mesh,
        in_specs=(act,) + params + (P("dp", None), act),
        out_specs=(act, act) + params,
        check_vma=False,
    )
```

```python
import functools

import jax
import jax.numpy as jnp
from jax import lax
from jax.experimental import pallas as pl
from jax.experimental.pallas import tpu as pltpu
from jax.sharding import PartitionSpec as P

HEADS = 12
HEAD_DIM = 64
EPS = 1e-05
FAR = 1 << 20
BOTH = ("seq", "dp")
F32 = jnp.float32
BF16 = jnp.bfloat16
MESH = pl.DeviceIdType.MESH
RING = 16
FW = 8
BW = 7


def ring_place():
    y, dp = lax.axis_index("seq"), lax.axis_index("dp")
    z, x, core = dp // 4, (dp // 2) % 2, dp % 2
    column = 2 * x + (x + y) % 2
    return 4 * column + jnp.where(column % 2 == 0, z, 3 - z), core


def ring_coords(t, core):
    column, k = t // 4, t % 4
    z = jnp.where(column % 2 == 0, k, 3 - k)
    return ((column + 1) // 2) % 2, 4 * z + 2 * (column // 2) + core


def ring_device(t, core):
    y, dp = ring_coords(t, core)
    return y * RING + dp


def meet(targets):
    barrier = pltpu.get_barrier_semaphore()
    for target in targets:
        pl.semaphore_signal(barrier, inc=1, device_id=target, device_id_type=MESH)
    pl.semaphore_wait(barrier, len(targets))


def remote(src, dst, send, recv, target):
    return pltpu.make_async_remote_copy(
        src_ref=src, dst_ref=dst, send_sem=send, recv_sem=recv, device_id=target, device_id_type=MESH
    )


def scatter_kernel(count, *refs):
    g, out = refs[:count], refs[count : 2 * count]
    own, pair, fw, bw = [refs[(2 + i) * count : (3 + i) * count] for i in range(4)]
    local_sem, pair_send, pair_recv, fw_send, fw_recv, bw_send, bw_recv = refs[6 * count :]
    r, core = ring_place()
    after, before = (r + 1) % RING, (r + RING - 1) % RING
    right, left, partner = ring_coords(after, core), ring_coords(before, core), ring_coords(r, 1 - core)

    def local(k, t):
        return pltpu.make_async_copy(g[k].at[ring_device(t, core)], own[k].at[t], local_sem.at[k, t])

    def to_pair(k, t):
        return remote(
            g[k].at[ring_device(t, 1 - core)], pair[k].at[t], pair_send.at[k, t], pair_recv.at[k, t], partner
        )

    def forth(k, h, src):
        return remote(src, fw[k].at[h], fw_send.at[k, h], fw_recv.at[k, h], right)

    def back(k, h, src):
        return remote(src, bw[k].at[h], bw_send.at[k, h], bw_recv.at[k, h], left)

    def term(k, t):
        local(k, t).wait()
        to_pair(k, t).wait_recv()
        return own[k][t].astype(F32) + pair[k][t].astype(F32)

    meet((right, left, partner))

    def begin(i, _):
        t = (r + jnp.where(i % 2 == 0, FW - i // 2, FW + 1 + i // 2)) % RING
        for k in range(count):
            to_pair(k, t).start()
            local(k, t).start()
        return 0

    lax.fori_loop(0, RING, begin, 0)

    for k in range(count):
        t = (r + FW) % RING
        pair[k][t] = term(k, t).astype(BF16)
        forth(k, 0, pair[k].at[t]).start()
        t = (r + RING - BW) % RING
        pair[k][t] = term(k, t).astype(BF16)
        back(k, 0, pair[k].at[t]).start()

    def forth_step(k, h):
        t = (r + FW - h) % RING
        mine = term(k, t)
        forth(k, h - 1, pair[k].at[t]).wait_recv()
        fw[k][h - 1] = (fw[k][h - 1].astype(F32) + mine).astype(BF16)
        forth(k, h, fw[k].at[h - 1]).start()

    def back_step(k, h):
        t = (r + RING - BW + h) % RING
        mine = term(k, t)
        back(k, h - 1, pair[k].at[t]).wait_recv()
        bw[k][h - 1] = (bw[k][h - 1].astype(F32) + mine).astype(BF16)
        back(k, h, bw[k].at[h - 1]).start()

    def hop(h, _):
        for k in range(count):
            forth_step(k, h)
            back_step(k, h)
        return 0

    lax.fori_loop(1, BW, hop, 0)
    for k in range(count):
        forth_step(k, FW - 1)
    for k in range(count):
        mine = term(k, r)
        back(k, BW - 1, pair[k].at[r]).wait_recv()
        mine = mine + bw[k][BW - 1].astype(F32)
        forth(k, FW - 1, pair[k].at[r]).wait_recv()
        out[k][...] = mine + fw[k][FW - 1].astype(F32)

    def drain(i, _):
        for k in range(count):
            to_pair(k, i).wait_send()
        return 0

    lax.fori_loop(0, RING, drain, 0)
    for k in range(count):
        for h in range(FW):
            forth(k, h, pair[k].at[0]).wait_send()
        for h in range(BW):
            back(k, h, pair[k].at[0]).wait_send()


def ring_scatter(parts, collective_id):
    count = len(parts)
    slots = lambda n: [pltpu.VMEM((n,) + p.shape[1:], BF16) for p in parts]
    dma = lambda n: pltpu.SemaphoreType.DMA((count, n))
    return pl.pallas_call(
        functools.partial(scatter_kernel, count),
        out_shape=[jax.ShapeDtypeStruct(p.shape[1:], F32) for p in parts],
        in_specs=[pl.BlockSpec(memory_space=pl.ANY)] * count,
        out_specs=[pl.BlockSpec(memory_space=pltpu.VMEM)] * count,
        scratch_shapes=slots(RING) + slots(RING) + slots(FW) + slots(BW)
        + [dma(RING), dma(RING), dma(RING), dma(FW), dma(FW), dma(BW), dma(BW)],
        compiler_params=pltpu.CompilerParams(
            collective_id=collective_id, has_side_effects=True, vmem_limit_bytes=60 * 2**20
        ),
        name="ring_scatter",
    )(*parts)


def gather_kernel(count, *refs):
    s, o = refs[:count], refs[count : 2 * count]
    local_sem, pair_send, pair_recv, fw_send, fw_recv, bw_send, bw_recv = refs[2 * count :]
    r, core = ring_place()
    after, before = (r + 1) % RING, (r + RING - 1) % RING
    right, left, partner = ring_coords(after, core), ring_coords(before, core), ring_coords(r, 1 - core)

    def place(k, t):
        return o[k].at[ring_device(t, core)]

    def local(k):
        return pltpu.make_async_copy(s[k], place(k, r), local_sem.at[k])

    def to_pair(k, t, src):
        return remote(src, place(k, t), pair_send.at[k, t], pair_recv.at[k, t], partner)

    def forth(k, h, t, src):
        return remote(src, place(k, t), fw_send.at[k, h], fw_recv.at[k, h], right)

    def back(k, h, t, src):
        return remote(src, place(k, t), bw_send.at[k, h], bw_recv.at[k, h], left)

    meet((right, left, partner))
    for k in range(count):
        forth(k, 0, r, s[k]).start()
        back(k, 0, r, s[k]).start()
        to_pair(k, r, s[k]).start()
        local(k).start()

    def forth_step(k, h):
        t = (r + RING - h) % RING
        forth(k, h - 1, t, place(k, t)).wait_recv()
        return t

    def back_step(k, h):
        t = (r + h) % RING
        back(k, h - 1, t, place(k, t)).wait_recv()
        return t

    def hop(h, _):
        for k in range(count):
            t = forth_step(k, h)
            forth(k, h, t, place(k, t)).start()
            to_pair(k, t, place(k, t)).start()
            t = back_step(k, h)
            back(k, h, t, place(k, t)).start()
            to_pair(k, t, place(k, t)).start()
        return 0

    lax.fori_loop(1, BW, hop, 0)
    for k in range(count):
        t = forth_step(k, FW - 1)
        forth(k, FW - 1, t, place(k, t)).start()
        to_pair(k, t, place(k, t)).start()
        t = back_step(k, BW)
        to_pair(k, t, place(k, t)).start()
    for k in range(count):
        t = forth_step(k, FW)
        to_pair(k, t, place(k, t)).start()

    def drain(t, _):
        for k in range(count):
            copy = to_pair(k, t, place(k, t))
            copy.wait_send()
            copy.wait_recv()
        return 0

    lax.fori_loop(0, RING, drain, 0)
    for k in range(count):
        local(k).wait()
        for h in range(FW):
            forth(k, h, r, s[k]).wait_send()
        for h in range(BW):
            back(k, h, r, s[k]).wait_send()


def ring_gather(parts, collective_id):
    count = len(parts)
    dma = lambda n: pltpu.SemaphoreType.DMA((count, n))
    return pl.pallas_call(
        functools.partial(gather_kernel, count),
        out_shape=[jax.ShapeDtypeStruct((2 * RING,) + p.shape, p.dtype) for p in parts],
        in_specs=[pl.BlockSpec(memory_space=pltpu.VMEM)] * count,
        out_specs=[pl.BlockSpec(memory_space=pl.ANY)] * count,
        scratch_shapes=[pltpu.SemaphoreType.DMA((count,))]
        + [dma(RING), dma(RING), dma(FW), dma(FW), dma(BW), dma(BW)],
        compiler_params=pltpu.CompilerParams(collective_id=collective_id, has_side_effects=True),
        name="ring_gather",
    )(*parts)


def use_ring():
    return lax.axis_size("seq") == 2 and lax.axis_size("dp") == RING


def gather_all(parts, collective_id):
    if use_ring():
        full = ring_gather(parts, collective_id)
        return [f.reshape((-1,) + f.shape[2:]) for f in full]
    return [lax.all_gather(p, BOTH, axis=0, tiled=True) for p in parts]


def scatter_all(parts, collective_id):
    if use_ring():
        split = [p.astype(BF16).reshape(2 * RING, -1, p.shape[1]) for p in parts]
        return ring_scatter(split, collective_id)
    return [lax.psum_scatter(p.astype(BF16), BOTH, scatter_dimension=0, tiled=True).astype(F32) for p in parts]


def dot(a, b):
    return jnp.dot(a, b, preferred_element_type=F32)


def dot_t(a, b):
    return lax.dot_general(a, b, (((1,), (1,)), ((), ())), preferred_element_type=F32)


def t_dot(a, b):
    return lax.dot_general(a, b, (((0,), (0,)), ((), ())), preferred_element_type=F32)


def norm_parts(v):
    center = v - jnp.mean(v, axis=-1, keepdims=True)
    inv = lax.rsqrt(jnp.mean(center * center, axis=-1, keepdims=True) + EPS)
    return center * inv, inv


def norm_grad(grad, unit, inv, gain):
    g = grad * gain
    mean_g = jnp.mean(g, axis=-1, keepdims=True)
    mean_gu = jnp.mean(g * unit, axis=-1, keepdims=True)
    return inv * (g - mean_g - unit * mean_gu)


def heads_of(v):
    return v.reshape(v.shape[0], HEADS, HEAD_DIM)


def attend(q, k, v, key_pos, limit):
    scores = jnp.einsum("qhd,khd->hqk", heads_of(q), heads_of(k), preferred_element_type=F32) * 0.125
    scores = jnp.where((key_pos[None, :] <= limit[:, None])[None], scores, -1e30)
    top = jnp.max(scores, axis=-1, keepdims=True)
    lse = top[..., 0] + jnp.log(jnp.sum(jnp.exp(scores - top), axis=-1))
    probs = jnp.exp(scores - lse[..., None])
    low = probs.astype(BF16)
    mixed = jnp.einsum("hqk,khd->qhd", low, heads_of(v), preferred_element_type=F32)
    return mixed.reshape(q.shape).astype(BF16), (probs, low)


def attend_back(saved, q, k, v, mixed, grad):
    probs, low = saved
    grad_h = heads_of(grad)
    grad_probs = jnp.einsum("qhd,khd->hqk", grad_h, heads_of(v), preferred_element_type=F32)
    row_dot = jnp.sum(grad_probs * probs, axis=-1, keepdims=True)
    grad_scores = (probs * (grad_probs - row_dot)).astype(BF16)
    gq = jnp.einsum("hqk,khd->qhd", grad_scores, heads_of(k), preferred_element_type=F32) * 0.125
    gk = jnp.einsum("hqk,qhd->khd", grad_scores, heads_of(q), preferred_element_type=F32) * 0.125
    gv = jnp.einsum("hqk,qhd->khd", low, grad_h, preferred_element_type=F32)
    return (
        gq.reshape(q.shape).astype(BF16),
        gk.reshape(k.shape).astype(BF16),
        gv.reshape(v.shape).astype(BF16),
    )


def on_device(
    inputs,
    query_weight,
    key_weight,
    value_weight,
    query_bias,
    value_bias,
    output_weight,
    output_bias,
    first_gain,
    first_shift,
    inner_weight,
    inner_bias,
    outer_weight,
    outer_bias,
    second_gain,
    second_shift,
    prefix,
    cotangent,
):
    micros, rows, width = inputs.shape[1:]
    own = query_weight.shape[0]
    hidden_width = inner_weight.shape[1]
    per = hidden_width // width
    seqs = lax.axis_size("seq")
    seq_at = lax.axis_index("seq")
    first_pos = seq_at * rows
    x = inputs[0]
    flat_x = x.reshape(micros * rows, width)
    row_pos = first_pos + jnp.arange(rows, dtype=jnp.int32)

    if seqs == 2:
        before = lax.ppermute(x, "seq", [(0, 1)])
        key_x = jnp.concatenate([x, before], axis=1)
        key_pos = jnp.concatenate(
            [row_pos, jnp.where(seq_at == 1, jnp.arange(rows, dtype=jnp.int32), FAR)]
        )
    else:
        key_x = lax.all_gather(x, "seq", axis=1, tiled=True)
        key_pos = jnp.arange(seqs * rows, dtype=jnp.int32)
    total_rows = key_x.shape[1]
    flat_key_x = key_x.reshape(micros * total_rows, width)

    vectors = (query_bias, value_bias, output_bias, first_gain, first_shift, outer_bias, second_gain, second_shift)
    small = jnp.concatenate([jnp.stack(vectors, axis=1), inner_bias.reshape(own, per)], axis=1)
    small_count = small.shape[1]
    small = jnp.pad(small, ((0, 0), (0, 128 - small_count)))
    full_query, full_key, full_value, small_all = gather_all([query_weight, key_weight, value_weight, small], 1)
    full_output, full_inner, full_outer = [
        lax.all_gather(w, BOTH, axis=0, tiled=True) for w in (output_weight, inner_weight, outer_weight)
    ]
    small_all = small_all[:, :small_count].astype(F32)
    qb, vb, ob, fg, fs, ub, sg, ss = [small_all[:, i] for i in range(8)]
    ib = small_all[:, 8:].reshape(hidden_width)

    queries = (dot(flat_x, full_query) + qb).astype(BF16).reshape(micros, rows, width)
    keys = dot(flat_key_x, full_key).astype(BF16).reshape(micros, total_rows, width)
    values = (dot(flat_key_x, full_value) + vb).astype(BF16).reshape(micros, total_rows, width)

    mixed_parts, saved = [], []
    for m in range(micros):
        limit = jnp.maximum(row_pos, prefix[0, m] - 1)
        mixed_m, saved_m = attend(queries[m], keys[m], values[m], key_pos, limit)
        mixed_parts.append(mixed_m)
        saved.append(saved_m)
    mixed = jnp.concatenate(mixed_parts, axis=0)

    unit1, inv1 = norm_parts(flat_x.astype(F32) + dot(mixed, full_output) + ob)
    middle = unit1 * fg + fs
    middle_low = middle.astype(BF16)
    inner = dot(middle_low, full_inner) + ib
    half_cdf = 0.5 * (1.0 + lax.erf(inner * (0.5**0.5)))
    hidden = (inner * half_cdf).astype(BF16)
    slope = half_cdf + inner * jnp.exp(-0.5 * inner * inner) * 0.3989422804014327
    unit2, inv2 = norm_parts(middle + dot(hidden, full_outer) + ub)
    result = (unit2 * sg + ss).astype(BF16)

    cot = cotangent[0].reshape(micros * rows, width).astype(F32)
    g_sgain = jnp.sum(cot * unit2, axis=0)
    g_sshift = jnp.sum(cot, axis=0)
    grad_mid2 = norm_grad(cot, unit2, inv2, sg)
    grad_outer = grad_mid2.astype(BF16)
    g_ubias = jnp.sum(grad_outer.astype(F32), axis=0)
    g_outer = t_dot(hidden, grad_outer).astype(BF16)
    grad_hidden = dot_t(grad_outer, full_outer).astype(BF16)
    grad_inner = (grad_hidden.astype(F32) * slope).astype(BF16)
    g_ibias = jnp.sum(grad_inner.astype(F32), axis=0)
    g_inner = t_dot(middle_low, grad_inner)
    grad_middle = grad_mid2 + dot_t(grad_inner, full_inner)
    g_fgain = jnp.sum(grad_middle * unit1, axis=0)
    g_fshift = jnp.sum(grad_middle, axis=0)
    grad_sum1 = norm_grad(grad_middle, unit1, inv1, fg)
    grad_branch = grad_sum1.astype(BF16)
    g_obias = jnp.sum(grad_branch.astype(F32), axis=0)
    g_output = t_dot(mixed, grad_branch)
    grad_mixed = dot_t(grad_branch, full_output).astype(BF16).reshape(micros, rows, width)

    gq_parts, gk_parts, gv_parts = [], [], []
    for m in range(micros):
        gq, gk, gv = attend_back(
            saved[m], queries[m], keys[m], values[m], mixed_parts[m], grad_mixed[m]
        )
        gq_parts.append(gq)
        gk_parts.append(gk)
        gv_parts.append(gv)
    grad_q = jnp.concatenate(gq_parts, axis=0)
    grad_k = jnp.stack(gk_parts).reshape(micros * total_rows, width)
    grad_v = jnp.stack(gv_parts).reshape(micros * total_rows, width)
    g_qbias = jnp.sum(grad_q.astype(F32), axis=0)
    g_vbias = jnp.sum(grad_v.astype(F32), axis=0)
    g_query = t_dot(flat_x, grad_q)
    g_key = t_dot(flat_key_x, grad_k)
    g_value = t_dot(flat_key_x, grad_v)
    g_small = jnp.concatenate(
        [
            jnp.stack([g_qbias, g_vbias, g_obias, g_fgain, g_fshift, g_ubias, g_sgain, g_sshift], axis=1),
            g_ibias.reshape(width, per),
        ],
        axis=1,
    )
    g_small = jnp.pad(g_small, ((0, 0), (0, 128 - small_count)))
    own_grads = scatter_all([g_outer, g_inner, g_output, g_query, g_key, g_value, g_small], 3)
    own_outer, own_inner, own_output, own_query, own_key, own_value, own_small = own_grads

    via_kv = (dot_t(grad_k, full_key) + dot_t(grad_v, full_value)).reshape(micros, total_rows, width)
    grad_x = (grad_sum1 + dot_t(grad_q, full_query)).reshape(micros, rows, width)
    if seqs == 2:
        grad_x = grad_x + via_kv[:, :rows]
        grad_x = grad_x + lax.ppermute(via_kv[:, rows:].astype(BF16), "seq", [(1, 0)]).astype(F32)
    else:
        grad_x = grad_x + lax.psum_scatter(via_kv, "seq", scatter_dimension=1, tiled=True)

    vec = own_small[:, :small_count]
    v_of = [vec[:, i] for i in range(8)]
    outputs = result.reshape(micros, rows, width)[None]
    return (
        outputs,
        grad_x[None],
        own_query,
        own_key,
        own_value,
        v_of[0],
        v_of[1],
        own_output,
        v_of[2],
        v_of[3],
        v_of[4],
        own_inner,
        vec[:, 8:].reshape(own * per),
        own_outer,
        v_of[5],
        v_of[6],
        v_of[7],
    )


def solution(mesh):
    act = P("dp", None, "seq", None)
    mat = P(BOTH, None)
    vec = P(BOTH)
    params = (mat, mat, mat, vec, vec, mat, vec, vec, vec, mat, vec, mat, vec, vec, vec)
    return jax.shard_map(
        on_device,
        mesh=mesh,
        in_specs=(act,) + params + (P("dp", None), act),
        out_specs=(act, act) + params,
        check_vma=False,
    )
```

```python
import functools

import jax
import jax.numpy as jnp
from jax import lax
from jax.experimental import pallas as pl
from jax.experimental.pallas import tpu as pltpu
from jax.sharding import PartitionSpec as P

HEADS = 12
HEAD_DIM = 64
EPS = 1e-05
BOTH = ("seq", "dp")
F32 = jnp.float32
BF16 = jnp.bfloat16
MESH = pl.DeviceIdType.MESH
RING = 16
FW = 8
BW = 7


def ring_place():
    y, dp = lax.axis_index("seq"), lax.axis_index("dp")
    z, x, core = dp // 4, (dp // 2) % 2, dp % 2
    column = 2 * x + (x + y) % 2
    return 4 * column + jnp.where(column % 2 == 0, z, 3 - z), core


def ring_coords(t, core):
    column, k = t // 4, t % 4
    z = jnp.where(column % 2 == 0, k, 3 - k)
    return ((column + 1) // 2) % 2, 4 * z + 2 * (column // 2) + core


def ring_device(t, core):
    y, dp = ring_coords(t, core)
    return y * RING + dp


def meet(targets):
    barrier = pltpu.get_barrier_semaphore()
    for target in targets:
        pl.semaphore_signal(barrier, inc=1, device_id=target, device_id_type=MESH)
    pl.semaphore_wait(barrier, len(targets))


def remote(src, dst, send, recv, target):
    return pltpu.make_async_remote_copy(
        src_ref=src, dst_ref=dst, send_sem=send, recv_sem=recv, device_id=target, device_id_type=MESH
    )


def scatter_kernel(count, *refs):
    g, out = refs[:count], refs[count : 2 * count]
    own, pair, fw, bw = [refs[(2 + i) * count : (3 + i) * count] for i in range(4)]
    local_sem, pair_send, pair_recv, fw_send, fw_recv, bw_send, bw_recv = refs[6 * count :]
    r, core = ring_place()
    after, before = (r + 1) % RING, (r + RING - 1) % RING
    right, left, partner = ring_coords(after, core), ring_coords(before, core), ring_coords(r, 1 - core)

    def local(k, t):
        return pltpu.make_async_copy(g[k].at[ring_device(t, core)], own[k].at[t], local_sem.at[k, t])

    def to_pair(k, t):
        return remote(
            g[k].at[ring_device(t, 1 - core)], pair[k].at[t], pair_send.at[k, t], pair_recv.at[k, t], partner
        )

    def forth(k, h, src):
        return remote(src, fw[k].at[h], fw_send.at[k, h], fw_recv.at[k, h], right)

    def back(k, h, src):
        return remote(src, bw[k].at[h], bw_send.at[k, h], bw_recv.at[k, h], left)

    def term(k, t):
        local(k, t).wait()
        to_pair(k, t).wait_recv()
        return own[k][t].astype(F32) + pair[k][t].astype(F32)

    meet((right, left, partner))

    def begin(i, _):
        t = (r + jnp.where(i % 2 == 0, FW - i // 2, FW + 1 + i // 2)) % RING
        for k in range(count):
            to_pair(k, t).start()
            local(k, t).start()
        return 0

    lax.fori_loop(0, RING, begin, 0)

    for k in range(count):
        t = (r + FW) % RING
        pair[k][t] = term(k, t).astype(BF16)
        forth(k, 0, pair[k].at[t]).start()
        t = (r + RING - BW) % RING
        pair[k][t] = term(k, t).astype(BF16)
        back(k, 0, pair[k].at[t]).start()

    def forth_step(k, h):
        t = (r + FW - h) % RING
        mine = term(k, t)
        forth(k, h - 1, pair[k].at[t]).wait_recv()
        fw[k][h - 1] = (fw[k][h - 1].astype(F32) + mine).astype(BF16)
        forth(k, h, fw[k].at[h - 1]).start()

    def back_step(k, h):
        t = (r + RING - BW + h) % RING
        mine = term(k, t)
        back(k, h - 1, pair[k].at[t]).wait_recv()
        bw[k][h - 1] = (bw[k][h - 1].astype(F32) + mine).astype(BF16)
        back(k, h, bw[k].at[h - 1]).start()

    def hop(h, _):
        for k in range(count):
            forth_step(k, h)
            back_step(k, h)
        return 0

    lax.fori_loop(1, BW, hop, 0)
    for k in range(count):
        forth_step(k, FW - 1)
    for k in range(count):
        mine = term(k, r)
        back(k, BW - 1, pair[k].at[r]).wait_recv()
        mine = mine + bw[k][BW - 1].astype(F32)
        forth(k, FW - 1, pair[k].at[r]).wait_recv()
        out[k][...] = mine + fw[k][FW - 1].astype(F32)

    def drain(i, _):
        for k in range(count):
            to_pair(k, i).wait_send()
        return 0

    lax.fori_loop(0, RING, drain, 0)
    for k in range(count):
        for h in range(FW):
            forth(k, h, pair[k].at[0]).wait_send()
        for h in range(BW):
            back(k, h, pair[k].at[0]).wait_send()


def ring_scatter(parts, collective_id):
    count = len(parts)
    slots = lambda n: [pltpu.VMEM((n,) + p.shape[1:], BF16) for p in parts]
    dma = lambda n: pltpu.SemaphoreType.DMA((count, n))
    return pl.pallas_call(
        functools.partial(scatter_kernel, count),
        out_shape=[jax.ShapeDtypeStruct(p.shape[1:], F32) for p in parts],
        in_specs=[pl.BlockSpec(memory_space=pl.ANY)] * count,
        out_specs=[pl.BlockSpec(memory_space=pltpu.VMEM)] * count,
        scratch_shapes=slots(RING) + slots(RING) + slots(FW) + slots(BW)
        + [dma(RING), dma(RING), dma(RING), dma(FW), dma(FW), dma(BW), dma(BW)],
        compiler_params=pltpu.CompilerParams(
            collective_id=collective_id, has_side_effects=True, vmem_limit_bytes=60 * 2**20
        ),
        name="ring_scatter",
    )(*parts)


def gather_kernel(count, *refs):
    s, o = refs[:count], refs[count : 2 * count]
    local_sem, pair_send, pair_recv, fw_send, fw_recv, bw_send, bw_recv = refs[2 * count :]
    r, core = ring_place()
    after, before = (r + 1) % RING, (r + RING - 1) % RING
    right, left, partner = ring_coords(after, core), ring_coords(before, core), ring_coords(r, 1 - core)

    def place(k, t):
        return o[k].at[ring_device(t, core)]

    def local(k):
        return pltpu.make_async_copy(s[k], place(k, r), local_sem.at[k])

    def to_pair(k, t, src):
        return remote(src, place(k, t), pair_send.at[k, t], pair_recv.at[k, t], partner)

    def forth(k, h, t, src):
        return remote(src, place(k, t), fw_send.at[k, h], fw_recv.at[k, h], right)

    def back(k, h, t, src):
        return remote(src, place(k, t), bw_send.at[k, h], bw_recv.at[k, h], left)

    meet((right, left, partner))
    for k in range(count):
        forth(k, 0, r, s[k]).start()
        back(k, 0, r, s[k]).start()
        to_pair(k, r, s[k]).start()
        local(k).start()

    def forth_step(k, h):
        t = (r + RING - h) % RING
        forth(k, h - 1, t, place(k, t)).wait_recv()
        return t

    def back_step(k, h):
        t = (r + h) % RING
        back(k, h - 1, t, place(k, t)).wait_recv()
        return t

    def hop(h, _):
        for k in range(count):
            t = forth_step(k, h)
            forth(k, h, t, place(k, t)).start()
            to_pair(k, t, place(k, t)).start()
            t = back_step(k, h)
            back(k, h, t, place(k, t)).start()
            to_pair(k, t, place(k, t)).start()
        return 0

    lax.fori_loop(1, BW, hop, 0)
    for k in range(count):
        t = forth_step(k, FW - 1)
        forth(k, FW - 1, t, place(k, t)).start()
        to_pair(k, t, place(k, t)).start()
        t = back_step(k, BW)
        to_pair(k, t, place(k, t)).start()
    for k in range(count):
        t = forth_step(k, FW)
        to_pair(k, t, place(k, t)).start()

    def drain(t, _):
        for k in range(count):
            copy = to_pair(k, t, place(k, t))
            copy.wait_send()
            copy.wait_recv()
        return 0

    lax.fori_loop(0, RING, drain, 0)
    for k in range(count):
        local(k).wait()
        for h in range(FW):
            forth(k, h, r, s[k]).wait_send()
        for h in range(BW):
            back(k, h, r, s[k]).wait_send()


def ring_gather(parts, collective_id):
    count = len(parts)
    dma = lambda n: pltpu.SemaphoreType.DMA((count, n))
    return pl.pallas_call(
        functools.partial(gather_kernel, count),
        out_shape=[jax.ShapeDtypeStruct((2 * RING,) + p.shape, p.dtype) for p in parts],
        in_specs=[pl.BlockSpec(memory_space=pltpu.VMEM)] * count,
        out_specs=[pl.BlockSpec(memory_space=pl.ANY)] * count,
        scratch_shapes=[pltpu.SemaphoreType.DMA((count,))]
        + [dma(RING), dma(RING), dma(FW), dma(FW), dma(BW), dma(BW)],
        compiler_params=pltpu.CompilerParams(collective_id=collective_id, has_side_effects=True),
        name="ring_gather",
    )(*parts)


def use_ring():
    return lax.axis_size("seq") == 2 and lax.axis_size("dp") == RING


def gather_all(parts, collective_id):
    if use_ring():
        full = ring_gather(parts, collective_id)
        return [f.reshape((-1,) + f.shape[2:]) for f in full]
    return [lax.all_gather(p, BOTH, axis=0, tiled=True) for p in parts]


def scatter_all(parts, collective_id):
    if use_ring():
        split = [p.astype(BF16).reshape(2 * RING, -1, p.shape[1]) for p in parts]
        return ring_scatter(split, collective_id)
    return [lax.psum_scatter(p.astype(BF16), BOTH, scatter_dimension=0, tiled=True).astype(F32) for p in parts]


def dot(a, b):
    return jnp.dot(a, b, preferred_element_type=F32)


def dot_t(a, b):
    return lax.dot_general(a, b, (((1,), (1,)), ((), ())), preferred_element_type=F32)


def t_dot(a, b):
    return lax.dot_general(a, b, (((0,), (0,)), ((), ())), preferred_element_type=F32)


def norm_parts(v):
    center = v - jnp.mean(v, axis=-1, keepdims=True)
    inv = lax.rsqrt(jnp.mean(center * center, axis=-1, keepdims=True) + EPS)
    return center * inv, inv


def norm_grad(grad, unit, inv, gain):
    g = grad * gain
    mean_g = jnp.mean(g, axis=-1, keepdims=True)
    mean_gu = jnp.mean(g * unit, axis=-1, keepdims=True)
    return inv * (g - mean_g - unit * mean_gu)


BLOCK = 256


def head_lanes(v, a):
    lane = lax.broadcasted_iota(jnp.int32, v.shape, 1)
    return jnp.where(lane // HEAD_DIM == a, v, jnp.zeros_like(v))


def row_plans(rows, total, first):
    if total != 2 * rows or rows % BLOCK:
        return [(0, rows, [(0, total, True)])]
    if first:
        return [(0, rows, [(0, rows, True)])]
    plans = []
    for r0 in range(0, rows, BLOCK):
        parts = [(rows, rows, False)]
        if r0:
            parts.append((0, r0, False))
        plans.append((r0, BLOCK, parts + [(r0, BLOCK, True)]))
    return plans


def key_plans(rows, total, first):
    if total != 2 * rows or rows % BLOCK:
        return [(0, total, 0, rows, True)]
    if first:
        return [(k0, BLOCK, 0, rows, True) for k0 in range(0, rows, BLOCK)]
    plans = [(k0, BLOCK, 0, rows, False) for k0 in range(rows, total, BLOCK)]
    return plans + [(k0, BLOCK, k0, rows - k0, True) for k0 in range(0, rows, BLOCK)]


def by_half(rows, total, run):
    if total != 2 * rows or rows % BLOCK:
        run(False)
    else:
        pl.when(lax.axis_index("seq") == 0)(lambda: run(True))
        pl.when(lax.axis_index("seq") != 0)(lambda: run(False))


def allowed_of(own_first, k0, keys, r0, rows, first_pos, prefix_len, key_axis):
    shape = (keys, rows) if key_axis == 0 else (rows, keys)
    key_base = first_pos if own_first else 0
    key_at = key_base + k0 + lax.broadcasted_iota(jnp.int32, shape, key_axis)
    row_at = first_pos + r0 + lax.broadcasted_iota(jnp.int32, shape, 1 - key_axis)
    return key_at <= jnp.maximum(row_at, prefix_len - 1)


def forward_kernel(prefix_ref, q_ref, k_ref, v_ref, o_ref, lse_ref):
    rows, total = q_ref.shape[1], k_ref.shape[1]
    prefix_len = prefix_ref[pl.program_id(0)]
    first_pos = lax.axis_index("seq") * rows
    own_first = total == 2 * rows

    def run(first):
        for r0, n, parts in row_plans(rows, total, first):
            q = q_ref[0, r0 : r0 + n] * jnp.asarray(HEAD_DIM**-0.5, BF16)
            mixed = jnp.zeros((n, 2 * HEAD_DIM), F32)
            logs = jnp.zeros((n, 2 * HEAD_DIM), F32)
            lane = lax.broadcasted_iota(jnp.int32, mixed.shape, 1)
            for a in range(2):
                q_a = head_lanes(q, a)
                scores = []
                for k0, keys, masked in parts:
                    s = dot_t(q_a, k_ref[0, k0 : k0 + keys])
                    if masked:
                        ok = allowed_of(own_first, k0, keys, r0, n, first_pos, prefix_len, 1)
                        s = jnp.where(ok, s, -1e30)
                    scores.append(s)
                top = functools.reduce(jnp.maximum, [jnp.max(s, axis=1, keepdims=True) for s in scores])
                total_exp = jnp.zeros_like(top)
                out = jnp.zeros_like(mixed)
                for s, (k0, keys, _) in zip(scores, parts):
                    p = jnp.exp(s - top)
                    total_exp = total_exp + jnp.sum(p, axis=1, keepdims=True)
                    out = out + dot(p.astype(BF16), v_ref[0, k0 : k0 + keys])
                mine = lane // HEAD_DIM == a
                mixed = jnp.where(mine, out / total_exp, mixed)
                logs = jnp.where(mine, top + jnp.log(total_exp), logs)
            o_ref[0, r0 : r0 + n] = mixed.astype(BF16)
            logs = logs.T
            lse_ref[0, 0, 0:1, r0 : r0 + n] = logs[0:1]
            lse_ref[0, 0, 1:2, r0 : r0 + n] = logs[HEAD_DIM : HEAD_DIM + 1]

    by_half(rows, total, run)


def backward_kernel(prefix_ref, q_ref, k_ref, v_ref, o_ref, lse_ref, g_ref, gq_ref, gk_ref, gv_ref, dots, acc):
    rows, total = q_ref.shape[1], k_ref.shape[1]
    prefix_len = prefix_ref[pl.program_id(0)]
    first_pos = lax.axis_index("seq") * rows
    own_first = total == 2 * rows
    scale = HEAD_DIM**-0.5
    product = (g_ref[0].astype(F32) * o_ref[0].astype(F32)).T
    for a in range(2):
        dots[a : a + 1] = jnp.sum(product[a * HEAD_DIM : (a + 1) * HEAD_DIM], axis=0, keepdims=True)
    acc[...] = jnp.zeros_like(acc)

    def run(first):
        for k0, keys, r0, n, masked in key_plans(rows, total, first):
            k = k_ref[0, k0 : k0 + keys]
            v = v_ref[0, k0 : k0 + keys]
            q = q_ref[0, r0 : r0 + n] * jnp.asarray(scale, BF16)
            g = g_ref[0, r0 : r0 + n]
            gk = jnp.zeros((keys, 2 * HEAD_DIM), F32)
            gv = jnp.zeros((keys, 2 * HEAD_DIM), F32)
            gq = jnp.zeros((n, 2 * HEAD_DIM), F32)
            for a in range(2):
                q_a, g_a = head_lanes(q, a), head_lanes(g, a)
                s = dot_t(k, q_a)
                if masked:
                    ok = allowed_of(own_first, k0, keys, r0, n, first_pos, prefix_len, 0)
                    s = jnp.where(ok, s, -1e30)
                p = jnp.exp(s - lse_ref[0, 0, a : a + 1, r0 : r0 + n])
                gv = gv + dot(p.astype(BF16), g_a)
                grad_p = dot_t(v, g_a)
                grad_s = (p * (grad_p - dots[a : a + 1, r0 : r0 + n])).astype(BF16)
                gk = gk + dot(grad_s, q_a)
                gq = gq + t_dot(grad_s, head_lanes(k, a))
            gk_ref[0, k0 : k0 + keys] = gk.astype(BF16)
            gv_ref[0, k0 : k0 + keys] = gv.astype(BF16)
            acc[r0 : r0 + n] = acc[r0 : r0 + n] + gq
        if first:
            gk_ref[0, rows:] = jnp.zeros((total - rows, 2 * HEAD_DIM), BF16)
            gv_ref[0, rows:] = jnp.zeros((total - rows, 2 * HEAD_DIM), BF16)

    by_half(rows, total, run)
    gq_ref[0] = (acc[...] * scale).astype(BF16)


def pair_spec(length):
    return pl.BlockSpec((1, length, 2 * HEAD_DIM), lambda m, h, prefix: (m, 0, h))


def attention(q, k, v, prefix):
    micros, rows, width = q.shape
    total = k.shape[1]
    pairs = HEADS // 2
    return pl.pallas_call(
        forward_kernel,
        out_shape=[
            jax.ShapeDtypeStruct(q.shape, BF16),
            jax.ShapeDtypeStruct((micros, pairs, 8, rows), F32),
        ],
        grid_spec=pltpu.PrefetchScalarGridSpec(
            num_scalar_prefetch=1,
            grid=(micros, pairs),
            in_specs=[pair_spec(rows), pair_spec(total), pair_spec(total)],
            out_specs=[pair_spec(rows), pl.BlockSpec((1, 1, 8, rows), lambda m, h, prefix: (m, h, 0, 0))],
        ),
        compiler_params=pltpu.CompilerParams(vmem_limit_bytes=48 * 2**20),
        cost_estimate=pl.CostEstimate(
            flops=8 * micros * rows * total * width,
            bytes_accessed=4 * micros * (rows + total) * width,
            transcendentals=micros * rows * total * HEADS,
        ),
        name="attention_forward",
    )(prefix, q, k, v)


def attention_back(q, k, v, mixed, lse, grad, prefix):
    micros, rows, width = q.shape
    total = k.shape[1]
    pairs = HEADS // 2
    return pl.pallas_call(
        backward_kernel,
        out_shape=[jax.ShapeDtypeStruct(t.shape, BF16) for t in (q, k, v)],
        grid_spec=pltpu.PrefetchScalarGridSpec(
            num_scalar_prefetch=1,
            grid=(micros, pairs),
            in_specs=[
                pair_spec(rows),
                pair_spec(total),
                pair_spec(total),
                pair_spec(rows),
                pl.BlockSpec((1, 1, 8, rows), lambda m, h, prefix: (m, h, 0, 0)),
                pair_spec(rows),
            ],
            out_specs=[pair_spec(rows), pair_spec(total), pair_spec(total)],
            scratch_shapes=[pltpu.VMEM((8, rows), F32), pltpu.VMEM((rows, 2 * HEAD_DIM), F32)],
        ),
        compiler_params=pltpu.CompilerParams(vmem_limit_bytes=48 * 2**20),
        cost_estimate=pl.CostEstimate(
            flops=20 * micros * rows * total * width,
            bytes_accessed=8 * micros * (rows + total) * width,
            transcendentals=micros * rows * total * HEADS,
        ),
        name="attention_backward",
    )(prefix, q, k, v, mixed, lse, grad)


def on_device(
    inputs,
    query_weight,
    key_weight,
    value_weight,
    query_bias,
    value_bias,
    output_weight,
    output_bias,
    first_gain,
    first_shift,
    inner_weight,
    inner_bias,
    outer_weight,
    outer_bias,
    second_gain,
    second_shift,
    prefix,
    cotangent,
):
    micros, rows, width = inputs.shape[1:]
    own = query_weight.shape[0]
    hidden_width = inner_weight.shape[1]
    per = hidden_width // width
    seqs = lax.axis_size("seq")
    x = inputs[0]
    flat_x = x.reshape(micros * rows, width)

    if seqs == 2:
        before = lax.ppermute(x, "seq", [(0, 1)])
        key_x = jnp.concatenate([x, before], axis=1)
    else:
        key_x = lax.all_gather(x, "seq", axis=1, tiled=True)
    total_rows = key_x.shape[1]
    flat_key_x = key_x.reshape(micros * total_rows, width)

    vectors = (query_bias, value_bias, output_bias, first_gain, first_shift, outer_bias, second_gain, second_shift)
    small = jnp.concatenate([jnp.stack(vectors, axis=1), inner_bias.reshape(own, per)], axis=1)
    small_count = small.shape[1]
    small = jnp.pad(small, ((0, 0), (0, 128 - small_count)))
    full_query, full_key, full_value, small_all = gather_all([query_weight, key_weight, value_weight, small], 1)
    full_output, full_inner, full_outer = [
        lax.all_gather(w, BOTH, axis=0, tiled=True) for w in (output_weight, inner_weight, outer_weight)
    ]
    small_all = small_all[:, :small_count].astype(F32)
    qb, vb, ob, fg, fs, ub, sg, ss = [small_all[:, i] for i in range(8)]
    ib = small_all[:, 8:].reshape(hidden_width)

    queries = (dot(flat_x, full_query) + qb).astype(BF16).reshape(micros, rows, width)
    keys = dot(flat_key_x, full_key).astype(BF16).reshape(micros, total_rows, width)
    values = (dot(flat_key_x, full_value) + vb).astype(BF16).reshape(micros, total_rows, width)

    mixed_parts, lse = attention(queries, keys, values, prefix[0])
    mixed = mixed_parts.reshape(micros * rows, width)

    unit1, inv1 = norm_parts(flat_x.astype(F32) + dot(mixed, full_output) + ob)
    middle = unit1 * fg + fs
    middle_low = middle.astype(BF16)
    inner = dot(middle_low, full_inner) + ib
    half_cdf = 0.5 * (1.0 + lax.erf(inner * (0.5**0.5)))
    hidden = (inner * half_cdf).astype(BF16)
    slope = half_cdf + inner * jnp.exp(-0.5 * inner * inner) * 0.3989422804014327
    unit2, inv2 = norm_parts(middle + dot(hidden, full_outer) + ub)
    result = (unit2 * sg + ss).astype(BF16)

    cot = cotangent[0].reshape(micros * rows, width).astype(F32)
    g_sgain = jnp.sum(cot * unit2, axis=0)
    g_sshift = jnp.sum(cot, axis=0)
    grad_mid2 = norm_grad(cot, unit2, inv2, sg)
    grad_outer = grad_mid2.astype(BF16)
    g_ubias = jnp.sum(grad_outer.astype(F32), axis=0)
    g_outer = t_dot(hidden, grad_outer).astype(BF16)
    grad_hidden = dot_t(grad_outer, full_outer).astype(BF16)
    grad_inner = (grad_hidden.astype(F32) * slope).astype(BF16)
    g_ibias = jnp.sum(grad_inner.astype(F32), axis=0)
    g_inner = t_dot(middle_low, grad_inner)
    grad_middle = grad_mid2 + dot_t(grad_inner, full_inner)
    g_fgain = jnp.sum(grad_middle * unit1, axis=0)
    g_fshift = jnp.sum(grad_middle, axis=0)
    grad_sum1 = norm_grad(grad_middle, unit1, inv1, fg)
    grad_branch = grad_sum1.astype(BF16)
    g_obias = jnp.sum(grad_branch.astype(F32), axis=0)
    g_output = t_dot(mixed, grad_branch)
    grad_mixed = dot_t(grad_branch, full_output).astype(BF16).reshape(micros, rows, width)

    grad_q, grad_k, grad_v = attention_back(
        queries, keys, values, mixed_parts, lse, grad_mixed, prefix[0]
    )
    grad_q = grad_q.reshape(micros * rows, width)
    grad_k = grad_k.reshape(micros * total_rows, width)
    grad_v = grad_v.reshape(micros * total_rows, width)
    g_qbias = jnp.sum(grad_q.astype(F32), axis=0)
    g_vbias = jnp.sum(grad_v.astype(F32), axis=0)
    g_query = t_dot(flat_x, grad_q)
    g_key = t_dot(flat_key_x, grad_k)
    g_value = t_dot(flat_key_x, grad_v)
    g_small = jnp.concatenate(
        [
            jnp.stack([g_qbias, g_vbias, g_obias, g_fgain, g_fshift, g_ubias, g_sgain, g_sshift], axis=1),
            g_ibias.reshape(width, per),
        ],
        axis=1,
    )
    g_small = jnp.pad(g_small, ((0, 0), (0, 128 - small_count)))
    own_grads = scatter_all([g_outer, g_inner, g_output, g_query, g_key, g_value, g_small], 3)
    own_outer, own_inner, own_output, own_query, own_key, own_value, own_small = own_grads

    via_kv = (dot_t(grad_k, full_key) + dot_t(grad_v, full_value)).reshape(micros, total_rows, width)
    grad_x = (grad_sum1 + dot_t(grad_q, full_query)).reshape(micros, rows, width)
    if seqs == 2:
        grad_x = grad_x + via_kv[:, :rows]
        grad_x = grad_x + lax.ppermute(via_kv[:, rows:].astype(BF16), "seq", [(1, 0)]).astype(F32)
    else:
        grad_x = grad_x + lax.psum_scatter(via_kv, "seq", scatter_dimension=1, tiled=True)

    vec = own_small[:, :small_count]
    v_of = [vec[:, i] for i in range(8)]
    outputs = result.reshape(micros, rows, width)[None]
    return (
        outputs,
        grad_x[None],
        own_query,
        own_key,
        own_value,
        v_of[0],
        v_of[1],
        own_output,
        v_of[2],
        v_of[3],
        v_of[4],
        own_inner,
        vec[:, 8:].reshape(own * per),
        own_outer,
        v_of[5],
        v_of[6],
        v_of[7],
    )


def solution(mesh):
    act = P("dp", None, "seq", None)
    mat = P(BOTH, None)
    vec = P(BOTH)
    params = (mat, mat, mat, vec, vec, mat, vec, vec, vec, mat, vec, mat, vec, vec, vec)
    return jax.shard_map(
        on_device,
        mesh=mesh,
        in_specs=(act,) + params + (P("dp", None), act),
        out_specs=(act, act) + params,
        check_vma=False,
    )
```

```python
import functools

import jax
import jax.numpy as jnp
from jax import lax
from jax.experimental import pallas as pl
from jax.experimental.pallas import tpu as pltpu
from jax.sharding import PartitionSpec as P

HEADS = 12
HEAD_DIM = 64
EPS = 1e-05
BOTH = ("seq", "dp")
F32 = jnp.float32
BF16 = jnp.bfloat16
MESH = pl.DeviceIdType.MESH
LINE = 4
SQUARE = 4
CHIPS = LINE * SQUARE


def device_coords(p, z, core):
    return ((p + 1) // 2) % 2, 4 * z + 2 * (p // 2) + core


def device_index(p, z, core):
    y, dp = device_coords(p, z, core)
    return y * CHIPS + dp


def whereabouts():
    y, dp = lax.axis_index("seq"), lax.axis_index("dp")
    z, x, core = dp // 4, (dp // 2) % 2, dp % 2
    return 2 * x + (x + y) % 2, z, core


def heights(z):
    code = jnp.where(z == 0, 1 + 4 * 2 + 16 * 3, jnp.where(z == 1, 0 + 4 * 2 + 16 * 3, jnp.where(z == 2, 1 + 4 * 3, 2 + 4 * 1)))
    return [z, code % 4, (code // 4) % 4, (code // 16) % 4]


def meet(z, always, up, down):
    barrier = pltpu.get_barrier_semaphore()

    def greet(target):
        pl.semaphore_signal(barrier, inc=1, device_id=target, device_id_type=MESH)

    for target in always:
        greet(target)
    pl.when(z < LINE - 1)(lambda: greet(up))
    pl.when(z > 0)(lambda: greet(down))
    ends = jnp.where(z == 0, 1, 0) + jnp.where(z == LINE - 1, 1, 0)
    pl.semaphore_wait(barrier, len(always) + 2 - ends)


def remote(src, dst, send, recv, target):
    return pltpu.make_async_remote_copy(
        src_ref=src, dst_ref=dst, send_sem=send, recv_sem=recv, device_id=target, device_id_type=MESH
    )


def neighbours():
    p, z, core = whereabouts()
    turn = 1 + 2 * core
    ahead, behind, across = (p + turn) % SQUARE, (p + SQUARE - turn) % SQUARE, (p + 2) % SQUARE
    to_ahead, to_behind = device_coords(ahead, z, core), device_coords(behind, z, core)
    partner = device_coords(p, z, 1 - core)
    up = device_coords(p, jnp.minimum(z + 1, LINE - 1), core)
    down = device_coords(p, jnp.maximum(z - 1, 0), core)
    return p, z, core, ahead, behind, across, to_ahead, to_behind, partner, up, down


def gather_kernel(count, *refs):
    s, o = refs[:count], refs[count : 2 * count]
    sems = refs[2 * count :]
    local_sem, pair_send, pair_recv, up_send, down_send, line_recv = sems[:6]
    one_send, one_recv, two_send, two_recv, far_send, far_recv = sems[6:]
    p, z, core, ahead, behind, across, to_ahead, to_behind, partner, up, down = neighbours()

    def place(k, q, t):
        return o[k].at[device_index(q, t, core)]

    def local(k):
        return pltpu.make_async_copy(s[k], place(k, p, z), local_sem.at[k])

    def to_pair(k, q, t, src):
        return remote(src, place(k, q, t), pair_send.at[k, q, t], pair_recv.at[k, q, t], partner)

    def rise(k, t, src):
        return remote(src, place(k, p, t), up_send.at[k, t], line_recv.at[k, t], up)

    def sink(k, t, src):
        return remote(src, place(k, p, t), down_send.at[k, t], line_recv.at[k, t], down)

    def one(k, t, src):
        return remote(src, place(k, p, t), one_send.at[k, t], one_recv.at[k, t], to_ahead)

    def two(k, t, src):
        return remote(src, place(k, p, t), two_send.at[k, t], two_recv.at[k, t], to_behind)

    def far(k, t, src):
        return remote(src, place(k, behind, t), far_send.at[k, t], far_recv.at[k, t], to_ahead)

    meet(z, (to_ahead, to_behind, partner), up, down)
    order = heights(z)

    def spread(k, t, src):
        pl.when((t <= z) & (z < LINE - 1))(lambda: rise(k, t, src).start())
        pl.when((t >= z) & (z > 0))(lambda: sink(k, t, src).start())
        one(k, t, src).start()
        two(k, t, src).start()
        to_pair(k, p, t, src).start()

    def column(k, t):
        rise(k, t, place(k, p, t)).wait_recv()
        spread(k, t, place(k, p, t))

    def sides(k, t):
        one(k, t, place(k, behind, t)).wait_recv()
        far(k, t, place(k, behind, t)).start()
        to_pair(k, behind, t, place(k, behind, t)).start()
        two(k, t, place(k, ahead, t)).wait_recv()
        to_pair(k, ahead, t, place(k, ahead, t)).start()

    def corner(k, t):
        far(k, t, place(k, across, t)).wait_recv()
        to_pair(k, across, t, place(k, across, t)).start()

    for k in range(count):
        spread(k, z, s[k])
        local(k).start()
    for i in range(1, LINE):
        for k in range(count):
            column(k, order[i])
            sides(k, order[i - 1])
            if i > 1:
                corner(k, order[i - 2])
    for k in range(count):
        sides(k, order[LINE - 1])
        corner(k, order[LINE - 2])
    for k in range(count):
        corner(k, order[LINE - 1])

    def drain(i, _):
        q, t = i // LINE, i % LINE
        for k in range(count):
            copy = to_pair(k, q, t, place(k, q, t))
            copy.wait_send()
            copy.wait_recv()
        return 0

    lax.fori_loop(0, CHIPS, drain, 0)

    def drain_line(t, _):
        for k in range(count):
            src = place(k, p, t)
            pl.when((t <= z) & (z < LINE - 1))(lambda: rise(k, t, src).wait_send())
            pl.when((t >= z) & (z > 0))(lambda: sink(k, t, src).wait_send())
            one(k, t, src).wait_send()
            two(k, t, src).wait_send()
            far(k, t, src).wait_send()
        return 0

    lax.fori_loop(0, LINE, drain_line, 0)
    for k in range(count):
        local(k).wait()


def grid_gather(parts, collective_id):
    count = len(parts)
    dma = lambda *n: pltpu.SemaphoreType.DMA((count,) + n)
    return pl.pallas_call(
        functools.partial(gather_kernel, count),
        out_shape=[jax.ShapeDtypeStruct((2 * CHIPS,) + p.shape, p.dtype) for p in parts],
        in_specs=[pl.BlockSpec(memory_space=pltpu.VMEM)] * count,
        out_specs=[pl.BlockSpec(memory_space=pl.ANY)] * count,
        scratch_shapes=[dma(), dma(SQUARE, LINE), dma(SQUARE, LINE)] + [dma(LINE)] * 9,
        compiler_params=pltpu.CompilerParams(collective_id=collective_id, has_side_effects=True),
        name="grid_gather",
    )(*parts)


def scatter_kernel(count, *refs):
    g, out = refs[:count], refs[count : 2 * count]
    own, pair, far_in, one_in, two_in, up_in, down_in = [
        refs[(2 + i) * count : (3 + i) * count] for i in range(7)
    ]
    sems = refs[9 * count :]
    local_sem, pair_send, pair_recv = sems[:3]
    far_send, far_recv, one_send, one_recv, two_send, two_recv, up_send, up_recv, down_send, down_recv = sems[3:]
    p, z, core, ahead, behind, across, to_ahead, to_behind, partner, up, down = neighbours()

    def local(k, q, t):
        return pltpu.make_async_copy(g[k].at[device_index(q, t, core)], own[k].at[q, t], local_sem.at[k, q, t])

    def to_pair(k, q, t):
        return remote(
            g[k].at[device_index(q, t, 1 - core)],
            pair[k].at[q, t],
            pair_send.at[k, q, t],
            pair_recv.at[k, q, t],
            partner,
        )

    def far(k, t, src):
        return remote(src, far_in[k].at[t], far_send.at[k, t], far_recv.at[k, t], to_behind)

    def one(k, t, src):
        return remote(src, one_in[k].at[t], one_send.at[k, t], one_recv.at[k, t], to_behind)

    def two(k, t, src):
        return remote(src, two_in[k].at[t], two_send.at[k, t], two_recv.at[k, t], to_ahead)

    def rise(k, t, src):
        return remote(src, up_in[k].at[t], up_send.at[k, t], up_recv.at[k, t], up)

    def sink(k, t, src):
        return remote(src, down_in[k].at[t], down_send.at[k, t], down_recv.at[k, t], down)

    def term(k, q, t):
        local(k, q, t).wait()
        to_pair(k, q, t).wait_recv()
        return own[k][q, t].astype(F32) + pair[k][q, t].astype(F32)

    meet(z, (to_ahead, to_behind, partner), up, down)
    order = heights(z)[::-1]
    for t in order:
        for q in (across, behind, ahead, p):
            for k in range(count):
                to_pair(k, q, t).start()
                local(k, q, t).start()

    def open_square(k, t):
        pair[k][across, t] = term(k, across, t).astype(BF16)
        far(k, t, pair[k].at[across, t]).start()
        pair[k][ahead, t] = term(k, ahead, t).astype(BF16)
        two(k, t, pair[k].at[ahead, t]).start()

    def pass_square(k, t):
        mine = term(k, behind, t)
        far(k, t, pair[k].at[across, t]).wait_recv()
        far_in[k][t] = (far_in[k][t].astype(F32) + mine).astype(BF16)
        one(k, t, far_in[k].at[t]).start()

    def close_square(k, t):
        mine = term(k, p, t)
        two(k, t, pair[k].at[ahead, t]).wait_recv()
        mine = mine + two_in[k][t].astype(F32)
        one(k, t, far_in[k].at[t]).wait_recv()
        return mine + one_in[k][t].astype(F32)

    def column(k, t):
        mine = close_square(k, t)

        @pl.when((t > z) & (z > 0))
        def _():
            rise(k, t, one_in[k].at[t]).wait_recv()

        @pl.when((t < z) & (z < LINE - 1))
        def _():
            sink(k, t, one_in[k].at[t]).wait_recv()

        @pl.when(((t > z) & (z == 0)) | ((t < z) & (z == LINE - 1)))
        def _():
            one_in[k][t] = mine.astype(BF16)

        @pl.when((t > z) & (z > 0))
        def _():
            one_in[k][t] = (mine + up_in[k][t].astype(F32)).astype(BF16)

        @pl.when((t < z) & (z < LINE - 1))
        def _():
            one_in[k][t] = (mine + down_in[k][t].astype(F32)).astype(BF16)

        pl.when(t > z)(lambda: rise(k, t, one_in[k].at[t]).start())
        pl.when(t < z)(lambda: sink(k, t, one_in[k].at[t]).start())

    def finish(k):
        out[k][...] = close_square(k, z)

        @pl.when(z > 0)
        def _():
            rise(k, z, one_in[k].at[z]).wait_recv()
            out[k][...] += up_in[k][z].astype(F32)

        @pl.when(z < LINE - 1)
        def _():
            sink(k, z, one_in[k].at[z]).wait_recv()
            out[k][...] += down_in[k][z].astype(F32)

    for k in range(count):
        open_square(k, order[0])

    code = order[0] + 4 * order[1] + 16 * order[2] + 64 * order[3]

    def at(i):
        return (code // jnp.where(i == 0, 1, jnp.where(i == 1, 4, jnp.where(i == 2, 16, 64)))) % 4

    def step(i, _):
        for k in range(count):
            open_square(k, at(i + 1))
            pass_square(k, at(i))
        for k in range(count):
            column(k, at(i))
        return 0

    lax.fori_loop(0, LINE - 1, step, 0)
    for k in range(count):
        pass_square(k, z)
    for k in range(count):
        finish(k)

    def drain(i, _):
        q, t = i // LINE, i % LINE
        for k in range(count):
            to_pair(k, q, t).wait_send()
        return 0

    lax.fori_loop(0, CHIPS, drain, 0)

    def drain_line(t, _):
        for k in range(count):
            src = one_in[k].at[t]
            far(k, t, src).wait_send()
            one(k, t, src).wait_send()
            two(k, t, src).wait_send()
            pl.when(t > z)(lambda: rise(k, t, src).wait_send())
            pl.when(t < z)(lambda: sink(k, t, src).wait_send())
        return 0

    lax.fori_loop(0, LINE, drain_line, 0)


def grid_scatter(parts, collective_id):
    count = len(parts)
    slots = lambda *n: [pltpu.VMEM(n + p.shape[1:], BF16) for p in parts]
    dma = lambda *n: pltpu.SemaphoreType.DMA((count,) + n)
    return pl.pallas_call(
        functools.partial(scatter_kernel, count),
        out_shape=[jax.ShapeDtypeStruct(p.shape[1:], F32) for p in parts],
        in_specs=[pl.BlockSpec(memory_space=pl.ANY)] * count,
        out_specs=[pl.BlockSpec(memory_space=pltpu.VMEM)] * count,
        scratch_shapes=slots(SQUARE, LINE) * 2 + slots(LINE) * 5 + [dma(SQUARE, LINE)] * 3 + [dma(LINE)] * 10,
        compiler_params=pltpu.CompilerParams(
            collective_id=collective_id, has_side_effects=True, vmem_limit_bytes=60 * 2**20
        ),
        name="grid_scatter",
    )(*parts)


def on_grid():
    return lax.axis_size("seq") == 2 and lax.axis_size("dp") == CHIPS


def gather_all(parts, collective_id):
    if on_grid():
        full = grid_gather(parts, collective_id)
        return [f.reshape((-1,) + f.shape[2:]) for f in full]
    return [lax.all_gather(p, BOTH, axis=0, tiled=True) for p in parts]


def scatter_all(parts, collective_id):
    if on_grid():
        split = [p.astype(BF16).reshape(2 * CHIPS, -1, p.shape[1]) for p in parts]
        return grid_scatter(split, collective_id)
    return [lax.psum_scatter(p.astype(BF16), BOTH, scatter_dimension=0, tiled=True).astype(F32) for p in parts]


def dot(a, b):
    return jnp.dot(a, b, preferred_element_type=F32)


def dot_t(a, b):
    return lax.dot_general(a, b, (((1,), (1,)), ((), ())), preferred_element_type=F32)


def t_dot(a, b):
    return lax.dot_general(a, b, (((0,), (0,)), ((), ())), preferred_element_type=F32)


def norm_parts(v):
    center = v - jnp.mean(v, axis=-1, keepdims=True)
    inv = lax.rsqrt(jnp.mean(center * center, axis=-1, keepdims=True) + EPS)
    return center * inv, inv


def norm_grad(grad, unit, inv, gain):
    g = grad * gain
    mean_g = jnp.mean(g, axis=-1, keepdims=True)
    mean_gu = jnp.mean(g * unit, axis=-1, keepdims=True)
    return inv * (g - mean_g - unit * mean_gu)


BLOCK = 256


def head_lanes(v, a):
    lane = lax.broadcasted_iota(jnp.int32, v.shape, 1)
    return jnp.where(lane // HEAD_DIM == a, v, jnp.zeros_like(v))


def row_plans(rows, blocks, total, first):
    if blocks == 1:
        return [(0, rows, [(0, 0, total, True)])]
    if first:
        return [(0, rows, [(0, 0, rows, True)])]
    plans = []
    for r0 in range(0, rows, BLOCK):
        parts = [(1, 0, rows, False)]
        if r0:
            parts.append((0, 0, r0, False))
        plans.append((r0, BLOCK, parts + [(0, r0, BLOCK, True)]))
    return plans


def key_plans(rows, blocks, total, first):
    if blocks == 1:
        return [(0, 0, total, 0, rows, True)]
    if first:
        return [(0, k0, BLOCK, 0, rows, True) for k0 in range(0, rows, BLOCK)]
    plans = [(1, k0, BLOCK, 0, rows, False) for k0 in range(0, rows, BLOCK)]
    return plans + [(0, k0, BLOCK, k0, rows - k0, True) for k0 in range(0, rows, BLOCK)]


def by_half(blocks, run):
    if blocks == 1:
        run(False)
    else:
        pl.when(lax.axis_index("seq") == 0)(lambda: run(True))
        pl.when(lax.axis_index("seq") != 0)(lambda: run(False))


def allowed_of(own_first, k0, keys, r0, rows, first_pos, prefix_len, key_axis):
    shape = (keys, rows) if key_axis == 0 else (rows, keys)
    key_base = first_pos if own_first else 0
    key_at = key_base + k0 + lax.broadcasted_iota(jnp.int32, shape, key_axis)
    row_at = first_pos + r0 + lax.broadcasted_iota(jnp.int32, shape, 1 - key_axis)
    return key_at <= jnp.maximum(row_at, prefix_len - 1)


def forward_kernel(blocks, prefix_ref, q_ref, *refs):
    k_refs, v_refs, (o_ref, lse_ref) = refs[:blocks], refs[blocks : 2 * blocks], refs[2 * blocks :]
    rows, total = q_ref.shape[1], k_refs[0].shape[1]
    prefix_len = prefix_ref[pl.program_id(0)]
    first_pos = lax.axis_index("seq") * rows
    own_first = blocks == 2

    def run(first):
        for r0, n, parts in row_plans(rows, blocks, total, first):
            q = q_ref[0, r0 : r0 + n] * jnp.asarray(HEAD_DIM**-0.5, BF16)
            mixed = jnp.zeros((n, 2 * HEAD_DIM), F32)
            logs = jnp.zeros((n, 2 * HEAD_DIM), F32)
            lane = lax.broadcasted_iota(jnp.int32, mixed.shape, 1)
            for a in range(2):
                q_a = head_lanes(q, a)
                scores = []
                for b, k0, keys, masked in parts:
                    s = dot_t(q_a, k_refs[b][0, k0 : k0 + keys])
                    if masked:
                        ok = allowed_of(own_first, k0, keys, r0, n, first_pos, prefix_len, 1)
                        s = jnp.where(ok, s, -1e30)
                    scores.append(s)
                top = functools.reduce(jnp.maximum, [jnp.max(s, axis=1, keepdims=True) for s in scores])
                total_exp = jnp.zeros_like(top)
                out = jnp.zeros_like(mixed)
                for s, (b, k0, keys, _) in zip(scores, parts):
                    p = jnp.exp(s - top)
                    total_exp = total_exp + jnp.sum(p, axis=1, keepdims=True)
                    out = out + dot(p.astype(BF16), v_refs[b][0, k0 : k0 + keys])
                mine = lane // HEAD_DIM == a
                mixed = jnp.where(mine, out / total_exp, mixed)
                logs = jnp.where(mine, top + jnp.log(total_exp), logs)
            o_ref[0, r0 : r0 + n] = mixed.astype(BF16)
            logs = logs.T
            lse_ref[0, 0, 0:1, r0 : r0 + n] = logs[0:1]
            lse_ref[0, 0, 1:2, r0 : r0 + n] = logs[HEAD_DIM : HEAD_DIM + 1]

    by_half(blocks, run)


def backward_kernel(blocks, prefix_ref, q_ref, o_ref, lse_ref, g_ref, *refs):
    k_refs, v_refs, gq_ref = refs[:blocks], refs[blocks : 2 * blocks], refs[2 * blocks]
    gk_refs, gv_refs = refs[2 * blocks + 1 : 3 * blocks + 1], refs[3 * blocks + 1 : 4 * blocks + 1]
    dots, acc = refs[4 * blocks + 1 :]
    rows, total = q_ref.shape[1], k_refs[0].shape[1]
    prefix_len = prefix_ref[pl.program_id(0)]
    first_pos = lax.axis_index("seq") * rows
    own_first = blocks == 2
    scale = HEAD_DIM**-0.5
    product = (g_ref[0].astype(F32) * o_ref[0].astype(F32)).T
    for a in range(2):
        dots[a : a + 1] = jnp.sum(product[a * HEAD_DIM : (a + 1) * HEAD_DIM], axis=0, keepdims=True)
    acc[...] = jnp.zeros_like(acc)

    def run(first):
        for b, k0, keys, r0, n, masked in key_plans(rows, blocks, total, first):
            k = k_refs[b][0, k0 : k0 + keys]
            v = v_refs[b][0, k0 : k0 + keys]
            q = q_ref[0, r0 : r0 + n] * jnp.asarray(scale, BF16)
            g = g_ref[0, r0 : r0 + n]
            gk = jnp.zeros((keys, 2 * HEAD_DIM), F32)
            gv = jnp.zeros((keys, 2 * HEAD_DIM), F32)
            gq = jnp.zeros((n, 2 * HEAD_DIM), F32)
            for a in range(2):
                q_a, g_a = head_lanes(q, a), head_lanes(g, a)
                s = dot_t(k, q_a)
                if masked:
                    ok = allowed_of(own_first, k0, keys, r0, n, first_pos, prefix_len, 0)
                    s = jnp.where(ok, s, -1e30)
                p = jnp.exp(s - lse_ref[0, 0, a : a + 1, r0 : r0 + n])
                gv = gv + dot(p.astype(BF16), g_a)
                grad_p = dot_t(v, g_a)
                grad_s = (p * (grad_p - dots[a : a + 1, r0 : r0 + n])).astype(BF16)
                gk = gk + dot(grad_s, q_a)
                gq = gq + t_dot(grad_s, head_lanes(k, a))
            gk_refs[b][0, k0 : k0 + keys] = gk.astype(BF16)
            gv_refs[b][0, k0 : k0 + keys] = gv.astype(BF16)
            acc[r0 : r0 + n] = acc[r0 : r0 + n] + gq
        if first:
            gk_refs[1][...] = jnp.zeros_like(gk_refs[1])
            gv_refs[1][...] = jnp.zeros_like(gv_refs[1])

    by_half(blocks, run)
    gq_ref[0] = (acc[...] * scale).astype(BF16)


def pair_spec(length):
    return pl.BlockSpec((1, length, 2 * HEAD_DIM), lambda m, h, prefix: (m, 0, h))


def attention(q, keys, values, prefix):
    micros, rows, width = q.shape
    blocks, total = len(keys), keys[0].shape[1]
    pairs = HEADS // 2
    return pl.pallas_call(
        functools.partial(forward_kernel, blocks),
        out_shape=[
            jax.ShapeDtypeStruct(q.shape, BF16),
            jax.ShapeDtypeStruct((micros, pairs, 8, rows), F32),
        ],
        grid_spec=pltpu.PrefetchScalarGridSpec(
            num_scalar_prefetch=1,
            grid=(micros, pairs),
            in_specs=[pair_spec(rows)] + [pair_spec(total)] * (2 * blocks),
            out_specs=[pair_spec(rows), pl.BlockSpec((1, 1, 8, rows), lambda m, h, prefix: (m, h, 0, 0))],
        ),
        compiler_params=pltpu.CompilerParams(vmem_limit_bytes=48 * 2**20),
        cost_estimate=pl.CostEstimate(
            flops=8 * micros * rows * blocks * total * width,
            bytes_accessed=4 * micros * (rows + blocks * total) * width,
            transcendentals=micros * rows * blocks * total * HEADS,
        ),
        name="attention_forward",
    )(prefix, q, *keys, *values)


def attention_back(q, keys, values, mixed, lse, grad, prefix):
    micros, rows, width = q.shape
    blocks, total = len(keys), keys[0].shape[1]
    pairs = HEADS // 2
    grads = pl.pallas_call(
        functools.partial(backward_kernel, blocks),
        out_shape=[jax.ShapeDtypeStruct(t.shape, BF16) for t in (q, *keys, *values)],
        grid_spec=pltpu.PrefetchScalarGridSpec(
            num_scalar_prefetch=1,
            grid=(micros, pairs),
            in_specs=[
                pair_spec(rows),
                pair_spec(rows),
                pl.BlockSpec((1, 1, 8, rows), lambda m, h, prefix: (m, h, 0, 0)),
                pair_spec(rows),
            ]
            + [pair_spec(total)] * (2 * blocks),
            out_specs=[pair_spec(rows)] + [pair_spec(total)] * (2 * blocks),
            scratch_shapes=[pltpu.VMEM((8, rows), F32), pltpu.VMEM((rows, 2 * HEAD_DIM), F32)],
        ),
        compiler_params=pltpu.CompilerParams(vmem_limit_bytes=48 * 2**20),
        cost_estimate=pl.CostEstimate(
            flops=20 * micros * rows * blocks * total * width,
            bytes_accessed=8 * micros * (rows + blocks * total) * width,
            transcendentals=micros * rows * blocks * total * HEADS,
        ),
        name="attention_backward",
    )(prefix, q, mixed, lse, grad, *keys, *values)
    return grads[0], grads[1 : 1 + blocks], grads[1 + blocks :]


def on_device(
    inputs,
    query_weight,
    key_weight,
    value_weight,
    query_bias,
    value_bias,
    output_weight,
    output_bias,
    first_gain,
    first_shift,
    inner_weight,
    inner_bias,
    outer_weight,
    outer_bias,
    second_gain,
    second_shift,
    prefix,
    cotangent,
):
    micros, rows, width = inputs.shape[1:]
    own = query_weight.shape[0]
    hidden_width = inner_weight.shape[1]
    per = hidden_width // width
    seqs = lax.axis_size("seq")
    x = inputs[0]
    flat_x = x.reshape(micros * rows, width)

    if seqs == 2:
        before = lax.ppermute(x, "seq", [(0, 1)])
        key_x = [flat_x, before.reshape(micros * rows, width)]
    else:
        key_x = [lax.all_gather(x, "seq", axis=1, tiled=True).reshape(-1, width)]

    vectors = (query_bias, value_bias, output_bias, first_gain, first_shift, outer_bias, second_gain, second_shift)
    small = jnp.concatenate([jnp.stack(vectors, axis=1), inner_bias.reshape(own, per)], axis=1)
    small_count = small.shape[1]
    small = jnp.pad(small, ((0, 0), (0, 128 - small_count)))
    full = gather_all(
        [query_weight, key_weight, value_weight, small, output_weight, inner_weight, outer_weight], 1
    )
    full_query, full_key, full_value, small_all, full_output, full_inner, full_outer = full
    small_all = small_all[:, :small_count].astype(F32)
    qb, vb, ob, fg, fs, ub, sg, ss = [small_all[:, i] for i in range(8)]
    ib = small_all[:, 8:].reshape(hidden_width)

    queries = (dot(flat_x, full_query) + qb).astype(BF16).reshape(micros, rows, width)
    keys = [dot(t, full_key).astype(BF16).reshape(micros, -1, width) for t in key_x]
    values = [(dot(t, full_value) + vb).astype(BF16).reshape(micros, -1, width) for t in key_x]

    mixed_parts, lse = attention(queries, keys, values, prefix[0])
    mixed = mixed_parts.reshape(micros * rows, width)

    unit1, inv1 = norm_parts(flat_x.astype(F32) + dot(mixed, full_output) + ob)
    middle = unit1 * fg + fs
    middle_low = middle.astype(BF16)
    inner = dot(middle_low, full_inner) + ib
    half_cdf = 0.5 * (1.0 + lax.erf(inner * (0.5**0.5)))
    hidden = (inner * half_cdf).astype(BF16)
    slope = half_cdf + inner * jnp.exp(-0.5 * inner * inner) * 0.3989422804014327
    unit2, inv2 = norm_parts(middle + dot(hidden, full_outer) + ub)
    result = (unit2 * sg + ss).astype(BF16)

    cot = cotangent[0].reshape(micros * rows, width).astype(F32)
    g_sgain = jnp.sum(cot * unit2, axis=0)
    g_sshift = jnp.sum(cot, axis=0)
    grad_mid2 = norm_grad(cot, unit2, inv2, sg)
    grad_outer = grad_mid2.astype(BF16)
    g_ubias = jnp.sum(grad_outer.astype(F32), axis=0)
    g_outer = t_dot(hidden, grad_outer).astype(BF16)
    grad_hidden = dot_t(grad_outer, full_outer).astype(BF16)
    grad_inner = (grad_hidden.astype(F32) * slope).astype(BF16)
    g_ibias = jnp.sum(grad_inner.astype(F32), axis=0)
    g_inner = t_dot(middle_low, grad_inner)
    grad_middle = grad_mid2 + dot_t(grad_inner, full_inner)
    g_fgain = jnp.sum(grad_middle * unit1, axis=0)
    g_fshift = jnp.sum(grad_middle, axis=0)
    grad_sum1 = norm_grad(grad_middle, unit1, inv1, fg)
    grad_branch = grad_sum1.astype(BF16)
    g_obias = jnp.sum(grad_branch.astype(F32), axis=0)
    g_output = t_dot(mixed, grad_branch)
    grad_mixed = dot_t(grad_branch, full_output).astype(BF16).reshape(micros, rows, width)

    grad_q, grad_k, grad_v = attention_back(
        queries, keys, values, mixed_parts, lse, grad_mixed, prefix[0]
    )
    grad_q = grad_q.reshape(micros * rows, width)
    grad_k = [t.reshape(-1, width) for t in grad_k]
    grad_v = [t.reshape(-1, width) for t in grad_v]
    g_qbias = jnp.sum(grad_q.astype(F32), axis=0)
    g_vbias = sum(jnp.sum(t.astype(F32), axis=0) for t in grad_v)
    g_query = t_dot(flat_x, grad_q)
    g_key = sum(t_dot(t, g) for t, g in zip(key_x, grad_k))
    g_value = sum(t_dot(t, g) for t, g in zip(key_x, grad_v))
    g_small = jnp.concatenate(
        [
            jnp.stack([g_qbias, g_vbias, g_obias, g_fgain, g_fshift, g_ubias, g_sgain, g_sshift], axis=1),
            g_ibias.reshape(width, per),
        ],
        axis=1,
    )
    g_small = jnp.pad(g_small, ((0, 0), (0, 128 - small_count)))
    own_grads = scatter_all([g_outer, g_inner, g_output, g_query, g_key, g_value, g_small], 3)
    own_outer, own_inner, own_output, own_query, own_key, own_value, own_small = own_grads

    via_kv = [dot_t(k, full_key) + dot_t(v, full_value) for k, v in zip(grad_k, grad_v)]
    via_kv = [t.reshape(micros, -1, width) for t in via_kv]
    grad_x = (grad_sum1 + dot_t(grad_q, full_query)).reshape(micros, rows, width)
    if seqs == 2:
        grad_x = grad_x + via_kv[0]
        grad_x = grad_x + lax.ppermute(via_kv[1].astype(BF16), "seq", [(1, 0)]).astype(F32)
    else:
        grad_x = grad_x + lax.psum_scatter(via_kv[0], "seq", scatter_dimension=1, tiled=True)

    vec = own_small[:, :small_count]
    v_of = [vec[:, i] for i in range(8)]
    outputs = result.reshape(micros, rows, width)[None]
    return (
        outputs,
        grad_x[None],
        own_query,
        own_key,
        own_value,
        v_of[0],
        v_of[1],
        own_output,
        v_of[2],
        v_of[3],
        v_of[4],
        own_inner,
        vec[:, 8:].reshape(own * per),
        own_outer,
        v_of[5],
        v_of[6],
        v_of[7],
    )


def solution(mesh):
    act = P("dp", None, "seq", None)
    mat = P(BOTH, None)
    vec = P(BOTH)
    params = (mat, mat, mat, vec, vec, mat, vec, vec, vec, mat, vec, mat, vec, vec, vec)
    return jax.shard_map(
        on_device,
        mesh=mesh,
        in_specs=(act,) + params + (P("dp", None), act),
        out_specs=(act, act) + params,
        check_vma=False,
    )
```

```python
import functools

import jax
import jax.numpy as jnp
from jax import lax
from jax.experimental import pallas as pl
from jax.experimental.pallas import tpu as pltpu
from jax.sharding import PartitionSpec as P

HEADS = 12
HEAD_DIM = 64
EPS = 1e-05
BOTH = ("seq", "dp")
F32 = jnp.float32
BF16 = jnp.bfloat16
MESH = pl.DeviceIdType.MESH
LINE = 4
SQUARE = 4
CHIPS = LINE * SQUARE


def device_coords(p, z, core):
    return ((p + 1) // 2) % 2, 4 * z + 2 * (p // 2) + core


def device_index(p, z, core):
    y, dp = device_coords(p, z, core)
    return y * CHIPS + dp


def whereabouts():
    y, dp = lax.axis_index("seq"), lax.axis_index("dp")
    z, x, core = dp // 4, (dp // 2) % 2, dp % 2
    return 2 * x + (x + y) % 2, z, core


def heights(z):
    code = jnp.where(z == 0, 1 + 4 * 2 + 16 * 3, jnp.where(z == 1, 0 + 4 * 2 + 16 * 3, jnp.where(z == 2, 1 + 4 * 3, 2 + 4 * 1)))
    return [z, code % 4, (code // 4) % 4, (code // 16) % 4]


def meet(z, always, up, down):
    barrier = pltpu.get_barrier_semaphore()

    def greet(target):
        pl.semaphore_signal(barrier, inc=1, device_id=target, device_id_type=MESH)

    for target in always:
        greet(target)
    pl.when(z < LINE - 1)(lambda: greet(up))
    pl.when(z > 0)(lambda: greet(down))
    ends = jnp.where(z == 0, 1, 0) + jnp.where(z == LINE - 1, 1, 0)
    pl.semaphore_wait(barrier, len(always) + 2 - ends)


def remote(src, dst, send, recv, target):
    return pltpu.make_async_remote_copy(
        src_ref=src, dst_ref=dst, send_sem=send, recv_sem=recv, device_id=target, device_id_type=MESH
    )


def neighbours():
    p, z, core = whereabouts()
    turn = 1 + 2 * core
    ahead, behind, across = (p + turn) % SQUARE, (p + SQUARE - turn) % SQUARE, (p + 2) % SQUARE
    to_ahead, to_behind = device_coords(ahead, z, core), device_coords(behind, z, core)
    partner = device_coords(p, z, 1 - core)
    up = device_coords(p, jnp.minimum(z + 1, LINE - 1), core)
    down = device_coords(p, jnp.maximum(z - 1, 0), core)
    return p, z, core, ahead, behind, across, to_ahead, to_behind, partner, up, down


def gather_kernel(count, *refs):
    s, o = refs[:count], refs[count : 2 * count]
    sems = refs[2 * count :]
    local_sem, pair_send, pair_recv, up_send, down_send, line_recv = sems[:6]
    one_send, one_recv, two_send, two_recv, far_send, far_recv = sems[6:]
    p, z, core, ahead, behind, across, to_ahead, to_behind, partner, up, down = neighbours()

    def place(k, q, t):
        return o[k].at[device_index(q, t, core)]

    def local(k):
        return pltpu.make_async_copy(s[k], place(k, p, z), local_sem.at[k])

    def to_pair(k, q, t, src):
        return remote(src, place(k, q, t), pair_send.at[k, q, t], pair_recv.at[k, q, t], partner)

    def rise(k, t, src):
        return remote(src, place(k, p, t), up_send.at[k, t], line_recv.at[k, t], up)

    def sink(k, t, src):
        return remote(src, place(k, p, t), down_send.at[k, t], line_recv.at[k, t], down)

    def one(k, t, src):
        return remote(src, place(k, p, t), one_send.at[k, t], one_recv.at[k, t], to_ahead)

    def two(k, t, src):
        return remote(src, place(k, p, t), two_send.at[k, t], two_recv.at[k, t], to_behind)

    def far(k, t, src):
        return remote(src, place(k, behind, t), far_send.at[k, t], far_recv.at[k, t], to_ahead)

    meet(z, (to_ahead, to_behind, partner), up, down)
    order = heights(z)

    def spread(k, t, src):
        pl.when((t <= z) & (z < LINE - 1))(lambda: rise(k, t, src).start())
        pl.when((t >= z) & (z > 0))(lambda: sink(k, t, src).start())
        one(k, t, src).start()
        two(k, t, src).start()
        to_pair(k, p, t, src).start()

    def column(k, t):
        rise(k, t, place(k, p, t)).wait_recv()
        spread(k, t, place(k, p, t))

    def sides(k, t):
        one(k, t, place(k, behind, t)).wait_recv()
        far(k, t, place(k, behind, t)).start()
        to_pair(k, behind, t, place(k, behind, t)).start()
        two(k, t, place(k, ahead, t)).wait_recv()
        to_pair(k, ahead, t, place(k, ahead, t)).start()

    def corner(k, t):
        far(k, t, place(k, across, t)).wait_recv()
        to_pair(k, across, t, place(k, across, t)).start()

    for k in range(count):
        spread(k, z, s[k])
        local(k).start()
    for i in range(1, LINE):
        for k in range(count):
            column(k, order[i])
            sides(k, order[i - 1])
            if i > 1:
                corner(k, order[i - 2])
    for k in range(count):
        sides(k, order[LINE - 1])
        corner(k, order[LINE - 2])
    for k in range(count):
        corner(k, order[LINE - 1])

    def drain(i, _):
        q, t = i // LINE, i % LINE
        for k in range(count):
            copy = to_pair(k, q, t, place(k, q, t))
            copy.wait_send()
            copy.wait_recv()
        return 0

    lax.fori_loop(0, CHIPS, drain, 0)

    def drain_line(t, _):
        for k in range(count):
            src = place(k, p, t)
            pl.when((t <= z) & (z < LINE - 1))(lambda: rise(k, t, src).wait_send())
            pl.when((t >= z) & (z > 0))(lambda: sink(k, t, src).wait_send())
            one(k, t, src).wait_send()
            two(k, t, src).wait_send()
            far(k, t, src).wait_send()
        return 0

    lax.fori_loop(0, LINE, drain_line, 0)
    for k in range(count):
        local(k).wait()


def grid_gather(parts, collective_id):
    count = len(parts)
    dma = lambda *n: pltpu.SemaphoreType.DMA((count,) + n)
    return pl.pallas_call(
        functools.partial(gather_kernel, count),
        out_shape=[jax.ShapeDtypeStruct((2 * CHIPS,) + p.shape, p.dtype) for p in parts],
        in_specs=[pl.BlockSpec(memory_space=pltpu.VMEM)] * count,
        out_specs=[pl.BlockSpec(memory_space=pl.ANY)] * count,
        scratch_shapes=[dma(), dma(SQUARE, LINE), dma(SQUARE, LINE)] + [dma(LINE)] * 9,
        compiler_params=pltpu.CompilerParams(collective_id=collective_id, has_side_effects=True),
        name="grid_gather",
    )(*parts)


def scatter_kernel(count, *refs):
    g, out = refs[:count], refs[count : 2 * count]
    own, pair, far_in, one_in, two_in, up_in, down_in = [
        refs[(2 + i) * count : (3 + i) * count] for i in range(7)
    ]
    sems = refs[9 * count :]
    local_sem, pair_send, pair_recv = sems[:3]
    far_send, far_recv, one_send, one_recv, two_send, two_recv, up_send, up_recv, down_send, down_recv = sems[3:]
    p, z, core, ahead, behind, across, to_ahead, to_behind, partner, up, down = neighbours()

    def local(k, q, t):
        return pltpu.make_async_copy(g[k].at[device_index(q, t, core)], own[k].at[q, t], local_sem.at[k, q, t])

    def to_pair(k, q, t):
        return remote(
            g[k].at[device_index(q, t, 1 - core)],
            pair[k].at[q, t],
            pair_send.at[k, q, t],
            pair_recv.at[k, q, t],
            partner,
        )

    def far(k, t, src):
        return remote(src, far_in[k].at[t], far_send.at[k, t], far_recv.at[k, t], to_behind)

    def one(k, t, src):
        return remote(src, one_in[k].at[t], one_send.at[k, t], one_recv.at[k, t], to_behind)

    def two(k, t, src):
        return remote(src, two_in[k].at[t], two_send.at[k, t], two_recv.at[k, t], to_ahead)

    def rise(k, t, src):
        return remote(src, up_in[k].at[t], up_send.at[k, t], up_recv.at[k, t], up)

    def sink(k, t, src):
        return remote(src, down_in[k].at[t], down_send.at[k, t], down_recv.at[k, t], down)

    def term(k, q, t):
        local(k, q, t).wait()
        to_pair(k, q, t).wait_recv()
        return own[k][q, t].astype(F32) + pair[k][q, t].astype(F32)

    meet(z, (to_ahead, to_behind, partner), up, down)
    order = heights(z)[::-1]
    for t in order:
        for q in (across, behind, ahead, p):
            for k in range(count):
                to_pair(k, q, t).start()
                local(k, q, t).start()

    def open_square(k, t):
        pair[k][across, t] = term(k, across, t).astype(BF16)
        far(k, t, pair[k].at[across, t]).start()
        pair[k][ahead, t] = term(k, ahead, t).astype(BF16)
        two(k, t, pair[k].at[ahead, t]).start()

    def pass_square(k, t):
        mine = term(k, behind, t)
        far(k, t, pair[k].at[across, t]).wait_recv()
        far_in[k][t] = (far_in[k][t].astype(F32) + mine).astype(BF16)
        one(k, t, far_in[k].at[t]).start()

    def close_square(k, t):
        mine = term(k, p, t)
        two(k, t, pair[k].at[ahead, t]).wait_recv()
        mine = mine + two_in[k][t].astype(F32)
        one(k, t, far_in[k].at[t]).wait_recv()
        return mine + one_in[k][t].astype(F32)

    def column(k, t):
        mine = close_square(k, t)

        @pl.when((t > z) & (z > 0))
        def _():
            rise(k, t, one_in[k].at[t]).wait_recv()

        @pl.when((t < z) & (z < LINE - 1))
        def _():
            sink(k, t, one_in[k].at[t]).wait_recv()

        @pl.when(((t > z) & (z == 0)) | ((t < z) & (z == LINE - 1)))
        def _():
            one_in[k][t] = mine.astype(BF16)

        @pl.when((t > z) & (z > 0))
        def _():
            one_in[k][t] = (mine + up_in[k][t].astype(F32)).astype(BF16)

        @pl.when((t < z) & (z < LINE - 1))
        def _():
            one_in[k][t] = (mine + down_in[k][t].astype(F32)).astype(BF16)

        pl.when(t > z)(lambda: rise(k, t, one_in[k].at[t]).start())
        pl.when(t < z)(lambda: sink(k, t, one_in[k].at[t]).start())

    def finish(k):
        out[k][...] = close_square(k, z)

        @pl.when(z > 0)
        def _():
            rise(k, z, one_in[k].at[z]).wait_recv()
            out[k][...] += up_in[k][z].astype(F32)

        @pl.when(z < LINE - 1)
        def _():
            sink(k, z, one_in[k].at[z]).wait_recv()
            out[k][...] += down_in[k][z].astype(F32)

    for k in range(count):
        open_square(k, order[0])

    code = order[0] + 4 * order[1] + 16 * order[2] + 64 * order[3]

    def at(i):
        return (code // jnp.where(i == 0, 1, jnp.where(i == 1, 4, jnp.where(i == 2, 16, 64)))) % 4

    def step(i, _):
        for k in range(count):
            open_square(k, at(i + 1))
            pass_square(k, at(i))
        for k in range(count):
            column(k, at(i))
        return 0

    lax.fori_loop(0, LINE - 1, step, 0)
    for k in range(count):
        pass_square(k, z)
    for k in range(count):
        finish(k)

    def drain(i, _):
        q, t = i // LINE, i % LINE
        for k in range(count):
            to_pair(k, q, t).wait_send()
        return 0

    lax.fori_loop(0, CHIPS, drain, 0)

    def drain_line(t, _):
        for k in range(count):
            src = one_in[k].at[t]
            far(k, t, src).wait_send()
            one(k, t, src).wait_send()
            two(k, t, src).wait_send()
            pl.when(t > z)(lambda: rise(k, t, src).wait_send())
            pl.when(t < z)(lambda: sink(k, t, src).wait_send())
        return 0

    lax.fori_loop(0, LINE, drain_line, 0)


def grid_scatter(parts, collective_id):
    count = len(parts)
    slots = lambda *n: [pltpu.VMEM(n + p.shape[1:], BF16) for p in parts]
    dma = lambda *n: pltpu.SemaphoreType.DMA((count,) + n)
    return pl.pallas_call(
        functools.partial(scatter_kernel, count),
        out_shape=[jax.ShapeDtypeStruct(p.shape[1:], F32) for p in parts],
        in_specs=[pl.BlockSpec(memory_space=pl.ANY)] * count,
        out_specs=[pl.BlockSpec(memory_space=pltpu.VMEM)] * count,
        scratch_shapes=slots(SQUARE, LINE) * 2 + slots(LINE) * 5 + [dma(SQUARE, LINE)] * 3 + [dma(LINE)] * 10,
        compiler_params=pltpu.CompilerParams(
            collective_id=collective_id, has_side_effects=True, vmem_limit_bytes=60 * 2**20
        ),
        name="grid_scatter",
    )(*parts)


def on_grid():
    return lax.axis_size("seq") == 2 and lax.axis_size("dp") == CHIPS


def gather_all(parts, collective_id):
    if on_grid():
        full = grid_gather(parts, collective_id)
        return [f.reshape((-1,) + f.shape[2:]) for f in full]
    return [lax.all_gather(p, BOTH, axis=0, tiled=True) for p in parts]


def scatter_all(parts, collective_id):
    if on_grid():
        split = [p.astype(BF16).reshape(2 * CHIPS, -1, p.shape[1]) for p in parts]
        return grid_scatter(split, collective_id)
    return [lax.psum_scatter(p.astype(BF16), BOTH, scatter_dimension=0, tiled=True).astype(F32) for p in parts]


def dot(a, b):
    return jnp.dot(a, b, preferred_element_type=F32)


def dot_t(a, b):
    return lax.dot_general(a, b, (((1,), (1,)), ((), ())), preferred_element_type=F32)


def t_dot(a, b):
    return lax.dot_general(a, b, (((0,), (0,)), ((), ())), preferred_element_type=F32)


def norm_parts(v):
    center = v - jnp.mean(v, axis=-1, keepdims=True)
    inv = lax.rsqrt(jnp.mean(center * center, axis=-1, keepdims=True) + EPS)
    return center * inv, inv


def norm_grad(grad, unit, inv, gain):
    g = grad * gain
    mean_g = jnp.mean(g, axis=-1, keepdims=True)
    mean_gu = jnp.mean(g * unit, axis=-1, keepdims=True)
    return inv * (g - mean_g - unit * mean_gu)


BLOCK = 256


def head_lanes(v, a):
    lane = lax.broadcasted_iota(jnp.int32, v.shape, 1)
    return jnp.where(lane // HEAD_DIM == a, v, jnp.zeros_like(v))


def row_plans(rows, blocks, total, first):
    if blocks == 1:
        return [(0, rows, [(0, 0, total, True)])]
    if first:
        return [(0, rows, [(0, 0, rows, True)])]
    plans = []
    for r0 in range(0, rows, BLOCK):
        parts = [(1, 0, rows, False)]
        if r0:
            parts.append((0, 0, r0, False))
        plans.append((r0, BLOCK, parts + [(0, r0, BLOCK, True)]))
    return plans


def key_plans(rows, blocks, total, first):
    if blocks == 1:
        return [(0, 0, total, 0, rows, True)]
    if first:
        return [(0, k0, BLOCK, 0, rows, True) for k0 in range(0, rows, BLOCK)]
    plans = [(1, k0, BLOCK, 0, rows, False) for k0 in range(0, rows, BLOCK)]
    return plans + [(0, k0, BLOCK, k0, rows - k0, True) for k0 in range(0, rows, BLOCK)]


def by_half(blocks, run):
    if blocks == 1:
        run(False)
    else:
        pl.when(lax.axis_index("seq") == 0)(lambda: run(True))
        pl.when(lax.axis_index("seq") != 0)(lambda: run(False))


def allowed_of(own_first, k0, keys, r0, rows, first_pos, prefix_len, key_axis):
    shape = (keys, rows) if key_axis == 0 else (rows, keys)
    key_base = first_pos if own_first else 0
    key_at = key_base + k0 + lax.broadcasted_iota(jnp.int32, shape, key_axis)
    row_at = first_pos + r0 + lax.broadcasted_iota(jnp.int32, shape, 1 - key_axis)
    return key_at <= jnp.maximum(row_at, prefix_len - 1)


def forward_kernel(blocks, prefix_ref, q_ref, *refs):
    k_refs, v_refs, (o_ref, lse_ref) = refs[:blocks], refs[blocks : 2 * blocks], refs[2 * blocks :]
    rows, total = q_ref.shape[1], k_refs[0].shape[1]
    prefix_len = prefix_ref[pl.program_id(0)]
    first_pos = lax.axis_index("seq") * rows
    own_first = blocks == 2

    def run(first):
        for r0, n, parts in row_plans(rows, blocks, total, first):
            q = q_ref[0, r0 : r0 + n] * jnp.asarray(HEAD_DIM**-0.5, BF16)
            mixed = jnp.zeros((n, 2 * HEAD_DIM), F32)
            logs = jnp.zeros((n, 2 * HEAD_DIM), F32)
            lane = lax.broadcasted_iota(jnp.int32, mixed.shape, 1)
            for a in range(2):
                q_a = head_lanes(q, a)
                scores = []
                for b, k0, keys, masked in parts:
                    s = dot_t(q_a, k_refs[b][0, k0 : k0 + keys])
                    if masked:
                        ok = allowed_of(own_first, k0, keys, r0, n, first_pos, prefix_len, 1)
                        s = jnp.where(ok, s, -1e30)
                    scores.append(s)
                top = functools.reduce(jnp.maximum, [jnp.max(s, axis=1, keepdims=True) for s in scores])
                total_exp = jnp.zeros_like(top)
                out = jnp.zeros_like(mixed)
                for s, (b, k0, keys, _) in zip(scores, parts):
                    p = jnp.exp(s - top)
                    total_exp = total_exp + jnp.sum(p, axis=1, keepdims=True)
                    out = out + dot(p.astype(BF16), v_refs[b][0, k0 : k0 + keys])
                mine = lane // HEAD_DIM == a
                mixed = jnp.where(mine, out / total_exp, mixed)
                logs = jnp.where(mine, top + jnp.log(total_exp), logs)
            o_ref[0, r0 : r0 + n] = mixed.astype(BF16)
            logs = logs.T
            lse_ref[0, 0, 0:1, r0 : r0 + n] = logs[0:1]
            lse_ref[0, 0, 1:2, r0 : r0 + n] = logs[HEAD_DIM : HEAD_DIM + 1]

    by_half(blocks, run)


def backward_kernel(blocks, prefix_ref, q_ref, o_ref, lse_ref, g_ref, *refs):
    k_refs, v_refs, gq_ref = refs[:blocks], refs[blocks : 2 * blocks], refs[2 * blocks]
    gk_refs, gv_refs = refs[2 * blocks + 1 : 3 * blocks + 1], refs[3 * blocks + 1 : 4 * blocks + 1]
    dots, acc = refs[4 * blocks + 1 :]
    rows, total = q_ref.shape[1], k_refs[0].shape[1]
    prefix_len = prefix_ref[pl.program_id(0)]
    first_pos = lax.axis_index("seq") * rows
    own_first = blocks == 2
    scale = HEAD_DIM**-0.5
    product = (g_ref[0].astype(F32) * o_ref[0].astype(F32)).T
    for a in range(2):
        dots[a : a + 1] = jnp.sum(product[a * HEAD_DIM : (a + 1) * HEAD_DIM], axis=0, keepdims=True)
    acc[...] = jnp.zeros_like(acc)

    def run(first):
        for b, k0, keys, r0, n, masked in key_plans(rows, blocks, total, first):
            k = k_refs[b][0, k0 : k0 + keys]
            v = v_refs[b][0, k0 : k0 + keys]
            q = q_ref[0, r0 : r0 + n] * jnp.asarray(scale, BF16)
            g = g_ref[0, r0 : r0 + n]
            gk = jnp.zeros((keys, 2 * HEAD_DIM), F32)
            gv = jnp.zeros((keys, 2 * HEAD_DIM), F32)
            gq = jnp.zeros((n, 2 * HEAD_DIM), F32)
            for a in range(2):
                q_a, g_a = head_lanes(q, a), head_lanes(g, a)
                s = dot_t(k, q_a)
                if masked:
                    ok = allowed_of(own_first, k0, keys, r0, n, first_pos, prefix_len, 0)
                    s = jnp.where(ok, s, -1e30)
                p = jnp.exp(s - lse_ref[0, 0, a : a + 1, r0 : r0 + n])
                gv = gv + dot(p.astype(BF16), g_a)
                grad_p = dot_t(v, g_a)
                grad_s = (p * (grad_p - dots[a : a + 1, r0 : r0 + n])).astype(BF16)
                gk = gk + dot(grad_s, q_a)
                gq = gq + t_dot(grad_s, head_lanes(k, a))
            gk_refs[b][0, k0 : k0 + keys] = gk.astype(BF16)
            gv_refs[b][0, k0 : k0 + keys] = gv.astype(BF16)
            acc[r0 : r0 + n] = acc[r0 : r0 + n] + gq
        if first:
            gk_refs[1][...] = jnp.zeros_like(gk_refs[1])
            gv_refs[1][...] = jnp.zeros_like(gv_refs[1])

    by_half(blocks, run)
    gq_ref[0] = (acc[...] * scale).astype(BF16)


def pair_spec(length):
    return pl.BlockSpec((1, length, 2 * HEAD_DIM), lambda m, h, prefix: (m, 0, h))


def attention(q, keys, values, prefix):
    micros, rows, width = q.shape
    blocks, total = len(keys), keys[0].shape[1]
    pairs = HEADS // 2
    return pl.pallas_call(
        functools.partial(forward_kernel, blocks),
        out_shape=[
            jax.ShapeDtypeStruct(q.shape, BF16),
            jax.ShapeDtypeStruct((micros, pairs, 8, rows), F32),
        ],
        grid_spec=pltpu.PrefetchScalarGridSpec(
            num_scalar_prefetch=1,
            grid=(micros, pairs),
            in_specs=[pair_spec(rows)] + [pair_spec(total)] * (2 * blocks),
            out_specs=[pair_spec(rows), pl.BlockSpec((1, 1, 8, rows), lambda m, h, prefix: (m, h, 0, 0))],
        ),
        compiler_params=pltpu.CompilerParams(vmem_limit_bytes=48 * 2**20),
        cost_estimate=pl.CostEstimate(
            flops=8 * micros * rows * blocks * total * width,
            bytes_accessed=4 * micros * (rows + blocks * total) * width,
            transcendentals=micros * rows * blocks * total * HEADS,
        ),
        name="attention_forward",
    )(prefix, q, *keys, *values)


def attention_back(q, keys, values, mixed, lse, grad, prefix):
    micros, rows, width = q.shape
    blocks, total = len(keys), keys[0].shape[1]
    pairs = HEADS // 2
    grads = pl.pallas_call(
        functools.partial(backward_kernel, blocks),
        out_shape=[jax.ShapeDtypeStruct(t.shape, BF16) for t in (q, *keys, *values)],
        grid_spec=pltpu.PrefetchScalarGridSpec(
            num_scalar_prefetch=1,
            grid=(micros, pairs),
            in_specs=[
                pair_spec(rows),
                pair_spec(rows),
                pl.BlockSpec((1, 1, 8, rows), lambda m, h, prefix: (m, h, 0, 0)),
                pair_spec(rows),
            ]
            + [pair_spec(total)] * (2 * blocks),
            out_specs=[pair_spec(rows)] + [pair_spec(total)] * (2 * blocks),
            scratch_shapes=[pltpu.VMEM((8, rows), F32), pltpu.VMEM((rows, 2 * HEAD_DIM), F32)],
        ),
        compiler_params=pltpu.CompilerParams(vmem_limit_bytes=48 * 2**20),
        cost_estimate=pl.CostEstimate(
            flops=20 * micros * rows * blocks * total * width,
            bytes_accessed=8 * micros * (rows + blocks * total) * width,
            transcendentals=micros * rows * blocks * total * HEADS,
        ),
        name="attention_backward",
    )(prefix, q, mixed, lse, grad, *keys, *values)
    return grads[0], grads[1 : 1 + blocks], grads[1 + blocks :]


def project_kernel(x_ref, before_ref, wq_ref, wk_ref, wv_ref, qb_ref, vb_ref, q_ref, k0_ref, k1_ref, v0_ref, v1_ref):
    x = x_ref[...]
    q_ref[...] = (dot(x, wq_ref[...]) + qb_ref[...]).astype(BF16)
    for rows_in, k_ref, v_ref in ((x, k0_ref, v0_ref), (before_ref[...], k1_ref, v1_ref)):
        k_ref[...] = dot(rows_in, wk_ref[...]).astype(BF16)
        v_ref[...] = (dot(rows_in, wv_ref[...]) + vb_ref[...]).astype(BF16)


def project(x, before, wq, wk, wv, qb, vb):
    count, width = x.shape
    rows = pl.BlockSpec((2 * BLOCK, width), lambda i: (i, 0))
    whole = pl.BlockSpec((width, width), lambda i: (0, 0))
    vector = pl.BlockSpec((1, width), lambda i: (0, 0))
    return pl.pallas_call(
        project_kernel,
        out_shape=[jax.ShapeDtypeStruct(x.shape, BF16)] * 5,
        grid=(count // (2 * BLOCK),),
        in_specs=[rows, rows, whole, whole, whole, vector, vector],
        out_specs=[rows] * 5,
        compiler_params=pltpu.CompilerParams(vmem_limit_bytes=48 * 2**20),
        cost_estimate=pl.CostEstimate(
            flops=10 * count * width * width, bytes_accessed=14 * count * width + 6 * width * width, transcendentals=0
        ),
        name="project",
    )(x, before, wq, wk, wv, qb[None], vb[None])


def unproject_kernel(
    x_ref, before_ref, sum1_ref, gq_ref, gk0_ref, gk1_ref, gv0_ref, gv1_ref, wq_ref, wk_ref, wv_ref,
    gx_ref, via_ref, gwq_ref, gwk_ref, gwv_ref, sums_ref, acc_q, acc_k, acc_v,
):
    step = pl.program_id(0)

    @pl.when(step == 0)
    def _():
        for ref in (acc_q, acc_k, acc_v, sums_ref):
            ref[...] = jnp.zeros_like(ref)

    x, before = x_ref[...], before_ref[...]
    gq, gk0, gk1, gv0, gv1 = gq_ref[...], gk0_ref[...], gk1_ref[...], gv0_ref[...], gv1_ref[...]
    via_ref[...] = (dot_t(gk1, wk_ref[...]) + dot_t(gv1, wv_ref[...])).astype(BF16)
    gx_ref[...] = sum1_ref[...] + dot_t(gq, wq_ref[...]) + dot_t(gk0, wk_ref[...]) + dot_t(gv0, wv_ref[...])
    acc_q[...] += t_dot(x, gq)
    acc_k[...] += t_dot(x, gk0) + t_dot(before, gk1)
    acc_v[...] += t_dot(x, gv0) + t_dot(before, gv1)
    sums_ref[0:1] += jnp.sum(gq.astype(F32), axis=0, keepdims=True)
    sums_ref[1:2] += jnp.sum(gv0.astype(F32) + gv1.astype(F32), axis=0, keepdims=True)

    @pl.when(step == pl.num_programs(0) - 1)
    def _():
        gwq_ref[...] = acc_q[...].astype(BF16)
        gwk_ref[...] = acc_k[...].astype(BF16)
        gwv_ref[...] = acc_v[...].astype(BF16)


def unproject(x, before, sum1, gq, gk, gv, wq, wk, wv):
    count, width = x.shape
    rows = pl.BlockSpec((BLOCK, width), lambda i: (i, 0))
    whole = pl.BlockSpec((width, width), lambda i: (0, 0))
    return pl.pallas_call(
        unproject_kernel,
        out_shape=[jax.ShapeDtypeStruct(x.shape, F32), jax.ShapeDtypeStruct(x.shape, BF16)]
        + [jax.ShapeDtypeStruct(wq.shape, BF16)] * 3
        + [jax.ShapeDtypeStruct((8, width), F32)],
        grid=(count // BLOCK,),
        in_specs=[rows] * 8 + [whole] * 3,
        out_specs=[rows] * 2 + [whole] * 3 + [pl.BlockSpec((8, width), lambda i: (0, 0))],
        scratch_shapes=[pltpu.VMEM(wq.shape, F32)] * 3,
        compiler_params=pltpu.CompilerParams(vmem_limit_bytes=56 * 2**20),
        cost_estimate=pl.CostEstimate(
            flops=20 * count * width * width, bytes_accessed=24 * count * width + 12 * width * width, transcendentals=0
        ),
        name="unproject",
    )(x, before, sum1, gq, *gk, *gv, wq, wk, wv)


def on_device(
    inputs,
    query_weight,
    key_weight,
    value_weight,
    query_bias,
    value_bias,
    output_weight,
    output_bias,
    first_gain,
    first_shift,
    inner_weight,
    inner_bias,
    outer_weight,
    outer_bias,
    second_gain,
    second_shift,
    prefix,
    cotangent,
):
    micros, rows, width = inputs.shape[1:]
    own = query_weight.shape[0]
    hidden_width = inner_weight.shape[1]
    per = hidden_width // width
    seqs = lax.axis_size("seq")
    x = inputs[0]
    flat_x = x.reshape(micros * rows, width)

    if seqs == 2:
        before = lax.ppermute(x, "seq", [(0, 1)])
        key_x = [flat_x, before.reshape(micros * rows, width)]
    else:
        key_x = [lax.all_gather(x, "seq", axis=1, tiled=True).reshape(-1, width)]

    vectors = (query_bias, value_bias, output_bias, first_gain, first_shift, outer_bias, second_gain, second_shift)
    small = jnp.concatenate([jnp.stack(vectors, axis=1), inner_bias.reshape(own, per)], axis=1)
    small_count = small.shape[1]
    small = jnp.pad(small, ((0, 0), (0, 128 - small_count)))
    full = gather_all(
        [query_weight, key_weight, value_weight, small, output_weight, inner_weight, outer_weight], 1
    )
    full_query, full_key, full_value, small_all, full_output, full_inner, full_outer = full
    small_all = small_all[:, :small_count].astype(F32)
    qb, vb, ob, fg, fs, ub, sg, ss = [small_all[:, i] for i in range(8)]
    ib = small_all[:, 8:].reshape(hidden_width)

    if seqs == 2:
        queries, *kv = project(flat_x, key_x[1], full_query, full_key, full_value, qb, vb)
        keys, values = kv[:2], kv[2:]
    else:
        queries = (dot(flat_x, full_query) + qb).astype(BF16)
        keys = [dot(t, full_key).astype(BF16) for t in key_x]
        values = [(dot(t, full_value) + vb).astype(BF16) for t in key_x]
    queries = queries.reshape(micros, rows, width)
    keys = [t.reshape(micros, -1, width) for t in keys]
    values = [t.reshape(micros, -1, width) for t in values]

    mixed_parts, lse = attention(queries, keys, values, prefix[0])
    mixed = mixed_parts.reshape(micros * rows, width)

    unit1, inv1 = norm_parts(flat_x.astype(F32) + dot(mixed, full_output) + ob)
    middle = unit1 * fg + fs
    middle_low = middle.astype(BF16)
    inner = dot(middle_low, full_inner) + ib
    half_cdf = 0.5 * (1.0 + lax.erf(inner * (0.5**0.5)))
    hidden = (inner * half_cdf).astype(BF16)
    slope = half_cdf + inner * jnp.exp(-0.5 * inner * inner) * 0.3989422804014327
    unit2, inv2 = norm_parts(middle + dot(hidden, full_outer) + ub)
    result = (unit2 * sg + ss).astype(BF16)

    cot = cotangent[0].reshape(micros * rows, width).astype(F32)
    g_sgain = jnp.sum(cot * unit2, axis=0)
    g_sshift = jnp.sum(cot, axis=0)
    grad_mid2 = norm_grad(cot, unit2, inv2, sg)
    grad_outer = grad_mid2.astype(BF16)
    g_ubias = jnp.sum(grad_outer.astype(F32), axis=0)
    g_outer = t_dot(hidden, grad_outer).astype(BF16)
    grad_hidden = dot_t(grad_outer, full_outer).astype(BF16)
    grad_inner = (grad_hidden.astype(F32) * slope).astype(BF16)
    g_ibias = jnp.sum(grad_inner.astype(F32), axis=0)
    g_inner = t_dot(middle_low, grad_inner)
    grad_middle = grad_mid2 + dot_t(grad_inner, full_inner)
    g_fgain = jnp.sum(grad_middle * unit1, axis=0)
    g_fshift = jnp.sum(grad_middle, axis=0)
    grad_sum1 = norm_grad(grad_middle, unit1, inv1, fg)
    grad_branch = grad_sum1.astype(BF16)
    g_obias = jnp.sum(grad_branch.astype(F32), axis=0)
    g_output = t_dot(mixed, grad_branch)
    grad_mixed = dot_t(grad_branch, full_output).astype(BF16).reshape(micros, rows, width)

    grad_q, grad_k, grad_v = attention_back(
        queries, keys, values, mixed_parts, lse, grad_mixed, prefix[0]
    )
    grad_q = grad_q.reshape(micros * rows, width)
    grad_k = [t.reshape(-1, width) for t in grad_k]
    grad_v = [t.reshape(-1, width) for t in grad_v]
    if seqs == 2:
        grad_x, via_kv, g_query, g_key, g_value, sums = unproject(
            flat_x, key_x[1], grad_sum1, grad_q, grad_k, grad_v, full_query, full_key, full_value
        )
        g_qbias, g_vbias = sums[0], sums[1]
        sent = lax.ppermute(via_kv, "seq", [(1, 0)])
    else:
        g_qbias = jnp.sum(grad_q.astype(F32), axis=0)
        g_vbias = sum(jnp.sum(t.astype(F32), axis=0) for t in grad_v)
        g_query = t_dot(flat_x, grad_q)
        g_key = sum(t_dot(t, g) for t, g in zip(key_x, grad_k))
        g_value = sum(t_dot(t, g) for t, g in zip(key_x, grad_v))
        via_kv = sum(dot_t(k, full_key) + dot_t(v, full_value) for k, v in zip(grad_k, grad_v))
        grad_x = grad_sum1 + dot_t(grad_q, full_query)
        sent = lax.psum_scatter(via_kv.reshape(micros, -1, width), "seq", scatter_dimension=1, tiled=True)
    g_small = jnp.concatenate(
        [
            jnp.stack([g_qbias, g_vbias, g_obias, g_fgain, g_fshift, g_ubias, g_sgain, g_sshift], axis=1),
            g_ibias.reshape(width, per),
        ],
        axis=1,
    )
    g_small = jnp.pad(g_small, ((0, 0), (0, 128 - small_count)))
    own_grads = scatter_all([g_outer, g_inner, g_output, g_query, g_key, g_value, g_small], 3)
    own_outer, own_inner, own_output, own_query, own_key, own_value, own_small = own_grads

    grad_x = grad_x.reshape(micros, rows, width) + sent.reshape(micros, rows, width).astype(F32)

    vec = own_small[:, :small_count]
    v_of = [vec[:, i] for i in range(8)]
    outputs = result.reshape(micros, rows, width)[None]
    return (
        outputs,
        grad_x[None],
        own_query,
        own_key,
        own_value,
        v_of[0],
        v_of[1],
        own_output,
        v_of[2],
        v_of[3],
        v_of[4],
        own_inner,
        vec[:, 8:].reshape(own * per),
        own_outer,
        v_of[5],
        v_of[6],
        v_of[7],
    )


def solution(mesh):
    act = P("dp", None, "seq", None)
    mat = P(BOTH, None)
    vec = P(BOTH)
    params = (mat, mat, mat, vec, vec, mat, vec, vec, vec, mat, vec, mat, vec, vec, vec)
    return jax.shard_map(
        on_device,
        mesh=mesh,
        in_specs=(act,) + params + (P("dp", None), act),
        out_specs=(act, act) + params,
        check_vma=False,
    )
```

```python
import functools

import jax
import jax.numpy as jnp
from jax import lax
from jax.experimental import pallas as pl
from jax.experimental.pallas import tpu as pltpu
from jax.sharding import PartitionSpec as P

HEADS = 12
HEAD_DIM = 64
EPS = 1e-05
BOTH = ("seq", "dp")
F32 = jnp.float32
BF16 = jnp.bfloat16
MESH = pl.DeviceIdType.MESH
LINE = 4
SQUARE = 4
CHIPS = LINE * SQUARE


def device_coords(p, z, core):
    return ((p + 1) // 2) % 2, 4 * z + 2 * (p // 2) + core


def device_index(p, z, core):
    y, dp = device_coords(p, z, core)
    return y * CHIPS + dp


def whereabouts():
    y, dp = lax.axis_index("seq"), lax.axis_index("dp")
    z, x, core = dp // 4, (dp // 2) % 2, dp % 2
    return 2 * x + (x + y) % 2, z, core


def heights(z):
    code = jnp.where(z == 0, 1 + 4 * 2 + 16 * 3, jnp.where(z == 1, 0 + 4 * 2 + 16 * 3, jnp.where(z == 2, 1 + 4 * 3, 2 + 4 * 1)))
    return [z, code % 4, (code // 4) % 4, (code // 16) % 4]


def meet(z, always, up, down):
    barrier = pltpu.get_barrier_semaphore()

    def greet(target):
        pl.semaphore_signal(barrier, inc=1, device_id=target, device_id_type=MESH)

    for target in always:
        greet(target)
    pl.when(z < LINE - 1)(lambda: greet(up))
    pl.when(z > 0)(lambda: greet(down))
    ends = jnp.where(z == 0, 1, 0) + jnp.where(z == LINE - 1, 1, 0)
    pl.semaphore_wait(barrier, len(always) + 2 - ends)


def remote(src, dst, send, recv, target):
    return pltpu.make_async_remote_copy(
        src_ref=src, dst_ref=dst, send_sem=send, recv_sem=recv, device_id=target, device_id_type=MESH
    )


def neighbours():
    p, z, core = whereabouts()
    turn = 1 + 2 * core
    ahead, behind, across = (p + turn) % SQUARE, (p + SQUARE - turn) % SQUARE, (p + 2) % SQUARE
    to_ahead, to_behind = device_coords(ahead, z, core), device_coords(behind, z, core)
    partner = device_coords(p, z, 1 - core)
    up = device_coords(p, jnp.minimum(z + 1, LINE - 1), core)
    down = device_coords(p, jnp.maximum(z - 1, 0), core)
    return p, z, core, ahead, behind, across, to_ahead, to_behind, partner, up, down


def gather_kernel(count, *refs):
    s, o = refs[:count], refs[count : 2 * count]
    sems = refs[2 * count :]
    local_sem, pair_send, pair_recv, up_send, down_send, line_recv = sems[:6]
    one_send, one_recv, two_send, two_recv, far_send, far_recv = sems[6:]
    p, z, core, ahead, behind, across, to_ahead, to_behind, partner, up, down = neighbours()

    def place(k, q, t):
        return o[k].at[device_index(q, t, core)]

    def local(k):
        return pltpu.make_async_copy(s[k], place(k, p, z), local_sem.at[k])

    def to_pair(k, q, t, src):
        return remote(src, place(k, q, t), pair_send.at[k, q, t], pair_recv.at[k, q, t], partner)

    def rise(k, t, src):
        return remote(src, place(k, p, t), up_send.at[k, t], line_recv.at[k, t], up)

    def sink(k, t, src):
        return remote(src, place(k, p, t), down_send.at[k, t], line_recv.at[k, t], down)

    def one(k, t, src):
        return remote(src, place(k, p, t), one_send.at[k, t], one_recv.at[k, t], to_ahead)

    def two(k, t, src):
        return remote(src, place(k, p, t), two_send.at[k, t], two_recv.at[k, t], to_behind)

    def far(k, t, src):
        return remote(src, place(k, behind, t), far_send.at[k, t], far_recv.at[k, t], to_ahead)

    meet(z, (to_ahead, to_behind, partner), up, down)
    order = heights(z)

    def spread(k, t, src):
        pl.when((t <= z) & (z < LINE - 1))(lambda: rise(k, t, src).start())
        pl.when((t >= z) & (z > 0))(lambda: sink(k, t, src).start())
        one(k, t, src).start()
        two(k, t, src).start()
        to_pair(k, p, t, src).start()

    def column(k, t):
        rise(k, t, place(k, p, t)).wait_recv()
        spread(k, t, place(k, p, t))

    def sides(k, t):
        one(k, t, place(k, behind, t)).wait_recv()
        far(k, t, place(k, behind, t)).start()
        to_pair(k, behind, t, place(k, behind, t)).start()
        two(k, t, place(k, ahead, t)).wait_recv()
        to_pair(k, ahead, t, place(k, ahead, t)).start()

    def corner(k, t):
        far(k, t, place(k, across, t)).wait_recv()
        to_pair(k, across, t, place(k, across, t)).start()

    for k in range(count):
        spread(k, z, s[k])
        local(k).start()
    for i in range(1, LINE):
        for k in range(count):
            column(k, order[i])
            sides(k, order[i - 1])
            if i > 1:
                corner(k, order[i - 2])
    for k in range(count):
        sides(k, order[LINE - 1])
        corner(k, order[LINE - 2])
    for k in range(count):
        corner(k, order[LINE - 1])

    def drain(i, _):
        q, t = i // LINE, i % LINE
        for k in range(count):
            copy = to_pair(k, q, t, place(k, q, t))
            copy.wait_send()
            copy.wait_recv()
        return 0

    lax.fori_loop(0, CHIPS, drain, 0)

    def drain_line(t, _):
        for k in range(count):
            src = place(k, p, t)
            pl.when((t <= z) & (z < LINE - 1))(lambda: rise(k, t, src).wait_send())
            pl.when((t >= z) & (z > 0))(lambda: sink(k, t, src).wait_send())
            one(k, t, src).wait_send()
            two(k, t, src).wait_send()
            far(k, t, src).wait_send()
        return 0

    lax.fori_loop(0, LINE, drain_line, 0)
    for k in range(count):
        local(k).wait()


def grid_gather(parts, collective_id):
    count = len(parts)
    dma = lambda *n: pltpu.SemaphoreType.DMA((count,) + n)
    return pl.pallas_call(
        functools.partial(gather_kernel, count),
        out_shape=[jax.ShapeDtypeStruct((2 * CHIPS,) + p.shape, p.dtype) for p in parts],
        in_specs=[pl.BlockSpec(memory_space=pltpu.VMEM)] * count,
        out_specs=[pl.BlockSpec(memory_space=pl.ANY)] * count,
        scratch_shapes=[dma(), dma(SQUARE, LINE), dma(SQUARE, LINE)] + [dma(LINE)] * 9,
        compiler_params=pltpu.CompilerParams(collective_id=collective_id, has_side_effects=True),
        name="grid_gather",
    )(*parts)


def scatter_kernel(count, *refs):
    g, out = refs[:count], refs[count : 2 * count]
    own, pair, far_in, one_in, two_in, up_in, down_in = [
        refs[(2 + i) * count : (3 + i) * count] for i in range(7)
    ]
    sems = refs[9 * count :]
    local_sem, pair_send, pair_recv = sems[:3]
    far_send, far_recv, one_send, one_recv, two_send, two_recv, up_send, up_recv, down_send, down_recv = sems[3:]
    p, z, core, ahead, behind, across, to_ahead, to_behind, partner, up, down = neighbours()

    def local(k, q, t):
        return pltpu.make_async_copy(g[k].at[device_index(q, t, core)], own[k].at[q, t], local_sem.at[k, q, t])

    def to_pair(k, q, t):
        return remote(
            g[k].at[device_index(q, t, 1 - core)],
            pair[k].at[q, t],
            pair_send.at[k, q, t],
            pair_recv.at[k, q, t],
            partner,
        )

    def far(k, t, src):
        return remote(src, far_in[k].at[t], far_send.at[k, t], far_recv.at[k, t], to_behind)

    def one(k, t, src):
        return remote(src, one_in[k].at[t], one_send.at[k, t], one_recv.at[k, t], to_behind)

    def two(k, t, src):
        return remote(src, two_in[k].at[t], two_send.at[k, t], two_recv.at[k, t], to_ahead)

    def rise(k, t, src):
        return remote(src, up_in[k].at[t], up_send.at[k, t], up_recv.at[k, t], up)

    def sink(k, t, src):
        return remote(src, down_in[k].at[t], down_send.at[k, t], down_recv.at[k, t], down)

    def term(k, q, t):
        local(k, q, t).wait()
        to_pair(k, q, t).wait_recv()
        return own[k][q, t].astype(F32) + pair[k][q, t].astype(F32)

    meet(z, (to_ahead, to_behind, partner), up, down)
    order = heights(z)[::-1]
    for t in order:
        for q in (across, behind, ahead, p):
            for k in range(count):
                to_pair(k, q, t).start()
                local(k, q, t).start()

    def open_square(k, t):
        pair[k][across, t] = term(k, across, t).astype(BF16)
        far(k, t, pair[k].at[across, t]).start()
        pair[k][ahead, t] = term(k, ahead, t).astype(BF16)
        two(k, t, pair[k].at[ahead, t]).start()

    def pass_square(k, t):
        mine = term(k, behind, t)
        far(k, t, pair[k].at[across, t]).wait_recv()
        far_in[k][t] = (far_in[k][t].astype(F32) + mine).astype(BF16)
        one(k, t, far_in[k].at[t]).start()

    def close_square(k, t):
        mine = term(k, p, t)
        two(k, t, pair[k].at[ahead, t]).wait_recv()
        mine = mine + two_in[k][t].astype(F32)
        one(k, t, far_in[k].at[t]).wait_recv()
        return mine + one_in[k][t].astype(F32)

    def column(k, t):
        mine = close_square(k, t)

        @pl.when((t > z) & (z > 0))
        def _():
            rise(k, t, one_in[k].at[t]).wait_recv()

        @pl.when((t < z) & (z < LINE - 1))
        def _():
            sink(k, t, one_in[k].at[t]).wait_recv()

        @pl.when(((t > z) & (z == 0)) | ((t < z) & (z == LINE - 1)))
        def _():
            one_in[k][t] = mine.astype(BF16)

        @pl.when((t > z) & (z > 0))
        def _():
            one_in[k][t] = (mine + up_in[k][t].astype(F32)).astype(BF16)

        @pl.when((t < z) & (z < LINE - 1))
        def _():
            one_in[k][t] = (mine + down_in[k][t].astype(F32)).astype(BF16)

        pl.when(t > z)(lambda: rise(k, t, one_in[k].at[t]).start())
        pl.when(t < z)(lambda: sink(k, t, one_in[k].at[t]).start())

    def finish(k):
        out[k][...] = close_square(k, z)

        @pl.when(z > 0)
        def _():
            rise(k, z, one_in[k].at[z]).wait_recv()
            out[k][...] += up_in[k][z].astype(F32)

        @pl.when(z < LINE - 1)
        def _():
            sink(k, z, one_in[k].at[z]).wait_recv()
            out[k][...] += down_in[k][z].astype(F32)

    for k in range(count):
        open_square(k, order[0])

    code = order[0] + 4 * order[1] + 16 * order[2] + 64 * order[3]

    def at(i):
        return (code // jnp.where(i == 0, 1, jnp.where(i == 1, 4, jnp.where(i == 2, 16, 64)))) % 4

    def step(i, _):
        for k in range(count):
            open_square(k, at(i + 1))
            pass_square(k, at(i))
        for k in range(count):
            column(k, at(i))
        return 0

    lax.fori_loop(0, LINE - 1, step, 0)
    for k in range(count):
        pass_square(k, z)
    for k in range(count):
        finish(k)

    def drain(i, _):
        q, t = i // LINE, i % LINE
        for k in range(count):
            to_pair(k, q, t).wait_send()
        return 0

    lax.fori_loop(0, CHIPS, drain, 0)

    def drain_line(t, _):
        for k in range(count):
            src = one_in[k].at[t]
            far(k, t, src).wait_send()
            one(k, t, src).wait_send()
            two(k, t, src).wait_send()
            pl.when(t > z)(lambda: rise(k, t, src).wait_send())
            pl.when(t < z)(lambda: sink(k, t, src).wait_send())
        return 0

    lax.fori_loop(0, LINE, drain_line, 0)


def grid_scatter(parts, collective_id):
    count = len(parts)
    slots = lambda *n: [pltpu.VMEM(n + p.shape[1:], BF16) for p in parts]
    dma = lambda *n: pltpu.SemaphoreType.DMA((count,) + n)
    return pl.pallas_call(
        functools.partial(scatter_kernel, count),
        out_shape=[jax.ShapeDtypeStruct(p.shape[1:], F32) for p in parts],
        in_specs=[pl.BlockSpec(memory_space=pl.ANY)] * count,
        out_specs=[pl.BlockSpec(memory_space=pltpu.VMEM)] * count,
        scratch_shapes=slots(SQUARE, LINE) * 2 + slots(LINE) * 5 + [dma(SQUARE, LINE)] * 3 + [dma(LINE)] * 10,
        compiler_params=pltpu.CompilerParams(
            collective_id=collective_id, has_side_effects=True, vmem_limit_bytes=60 * 2**20
        ),
        name="grid_scatter",
    )(*parts)


def on_grid():
    return lax.axis_size("seq") == 2 and lax.axis_size("dp") == CHIPS


def gather_all(parts, collective_id):
    if on_grid():
        full = grid_gather(parts, collective_id)
        return [f.reshape((-1,) + f.shape[2:]) for f in full]
    return [lax.all_gather(p, BOTH, axis=0, tiled=True) for p in parts]


def scatter_all(parts, collective_id):
    if on_grid():
        split = [p.astype(BF16).reshape(2 * CHIPS, -1, p.shape[1]) for p in parts]
        return grid_scatter(split, collective_id)
    return [lax.psum_scatter(p.astype(BF16), BOTH, scatter_dimension=0, tiled=True).astype(F32) for p in parts]


def dot(a, b):
    return jnp.dot(a, b, preferred_element_type=F32)


def dot_t(a, b):
    return lax.dot_general(a, b, (((1,), (1,)), ((), ())), preferred_element_type=F32)


def t_dot(a, b):
    return lax.dot_general(a, b, (((0,), (0,)), ((), ())), preferred_element_type=F32)


def norm_parts(v):
    center = v - jnp.mean(v, axis=-1, keepdims=True)
    inv = lax.rsqrt(jnp.mean(center * center, axis=-1, keepdims=True) + EPS)
    return center * inv, inv


def norm_grad(grad, unit, inv, gain):
    g = grad * gain
    mean_g = jnp.mean(g, axis=-1, keepdims=True)
    mean_gu = jnp.mean(g * unit, axis=-1, keepdims=True)
    return inv * (g - mean_g - unit * mean_gu)


BLOCK = 256


def head_lanes(v, a):
    lane = lax.broadcasted_iota(jnp.int32, v.shape, 1)
    return jnp.where(lane // HEAD_DIM == a, v, jnp.zeros_like(v))


def row_plans(rows, blocks, total, first):
    if blocks == 1:
        return [(0, rows, [(0, 0, total, True)])]
    if first:
        return [(0, rows, [(0, 0, rows, True)])]
    plans = []
    for r0 in range(0, rows, BLOCK):
        parts = [(1, 0, rows, False)]
        if r0:
            parts.append((0, 0, r0, False))
        plans.append((r0, BLOCK, parts + [(0, r0, BLOCK, True)]))
    return plans


def key_plans(rows, blocks, total, first):
    if blocks == 1:
        return [(0, 0, total, 0, rows, True)]
    if first:
        return [(0, k0, BLOCK, 0, rows, True) for k0 in range(0, rows, BLOCK)]
    plans = [(1, k0, BLOCK, 0, rows, False) for k0 in range(0, rows, BLOCK)]
    return plans + [(0, k0, BLOCK, k0, rows - k0, True) for k0 in range(0, rows, BLOCK)]


def by_half(blocks, run):
    if blocks == 1:
        run(False)
    else:
        pl.when(lax.axis_index("seq") == 0)(lambda: run(True))
        pl.when(lax.axis_index("seq") != 0)(lambda: run(False))


def allowed_of(own_first, k0, keys, r0, rows, first_pos, prefix_len, key_axis):
    shape = (keys, rows) if key_axis == 0 else (rows, keys)
    key_base = first_pos if own_first else 0
    key_at = key_base + k0 + lax.broadcasted_iota(jnp.int32, shape, key_axis)
    row_at = first_pos + r0 + lax.broadcasted_iota(jnp.int32, shape, 1 - key_axis)
    return key_at <= jnp.maximum(row_at, prefix_len - 1)


def forward_kernel(blocks, prefix_ref, q_ref, *refs):
    k_refs, v_refs, (o_ref, lse_ref) = refs[:blocks], refs[blocks : 2 * blocks], refs[2 * blocks :]
    rows, total = q_ref.shape[1], k_refs[0].shape[1]
    prefix_len = prefix_ref[pl.program_id(0)]
    first_pos = lax.axis_index("seq") * rows
    own_first = blocks == 2

    def run(first):
        for r0, n, parts in row_plans(rows, blocks, total, first):
            q = q_ref[0, r0 : r0 + n] * jnp.asarray(HEAD_DIM**-0.5, BF16)
            mixed = jnp.zeros((n, 2 * HEAD_DIM), F32)
            logs = jnp.zeros((n, 2 * HEAD_DIM), F32)
            lane = lax.broadcasted_iota(jnp.int32, mixed.shape, 1)
            for a in range(2):
                q_a = head_lanes(q, a)
                scores = []
                for b, k0, keys, masked in parts:
                    s = dot_t(q_a, k_refs[b][0, k0 : k0 + keys])
                    if masked:
                        ok = allowed_of(own_first, k0, keys, r0, n, first_pos, prefix_len, 1)
                        s = jnp.where(ok, s, -1e30)
                    scores.append(s)
                top = functools.reduce(jnp.maximum, [jnp.max(s, axis=1, keepdims=True) for s in scores])
                total_exp = jnp.zeros_like(top)
                out = jnp.zeros_like(mixed)
                for s, (b, k0, keys, _) in zip(scores, parts):
                    p = jnp.exp(s - top)
                    total_exp = total_exp + jnp.sum(p, axis=1, keepdims=True)
                    out = out + dot(p.astype(BF16), v_refs[b][0, k0 : k0 + keys])
                mine = lane // HEAD_DIM == a
                mixed = jnp.where(mine, out / total_exp, mixed)
                logs = jnp.where(mine, top + jnp.log(total_exp), logs)
            o_ref[0, r0 : r0 + n] = mixed.astype(BF16)
            logs = logs.T
            lse_ref[0, 0, 0:1, r0 : r0 + n] = logs[0:1]
            lse_ref[0, 0, 1:2, r0 : r0 + n] = logs[HEAD_DIM : HEAD_DIM + 1]

    by_half(blocks, run)


def backward_kernel(blocks, prefix_ref, q_ref, o_ref, lse_ref, g_ref, *refs):
    k_refs, v_refs, gq_ref = refs[:blocks], refs[blocks : 2 * blocks], refs[2 * blocks]
    gk_refs, gv_refs = refs[2 * blocks + 1 : 3 * blocks + 1], refs[3 * blocks + 1 : 4 * blocks + 1]
    dots, acc = refs[4 * blocks + 1 :]
    rows, total = q_ref.shape[1], k_refs[0].shape[1]
    prefix_len = prefix_ref[pl.program_id(0)]
    first_pos = lax.axis_index("seq") * rows
    own_first = blocks == 2
    scale = HEAD_DIM**-0.5
    product = (g_ref[0].astype(F32) * o_ref[0].astype(F32)).T
    for a in range(2):
        dots[a : a + 1] = jnp.sum(product[a * HEAD_DIM : (a + 1) * HEAD_DIM], axis=0, keepdims=True)
    acc[...] = jnp.zeros_like(acc)

    def run(first):
        for b, k0, keys, r0, n, masked in key_plans(rows, blocks, total, first):
            k = k_refs[b][0, k0 : k0 + keys]
            v = v_refs[b][0, k0 : k0 + keys]
            q = q_ref[0, r0 : r0 + n] * jnp.asarray(scale, BF16)
            g = g_ref[0, r0 : r0 + n]
            gk = jnp.zeros((keys, 2 * HEAD_DIM), F32)
            gv = jnp.zeros((keys, 2 * HEAD_DIM), F32)
            gq = jnp.zeros((n, 2 * HEAD_DIM), F32)
            for a in range(2):
                q_a, g_a = head_lanes(q, a), head_lanes(g, a)
                s = dot_t(k, q_a)
                if masked:
                    ok = allowed_of(own_first, k0, keys, r0, n, first_pos, prefix_len, 0)
                    s = jnp.where(ok, s, -1e30)
                p = jnp.exp(s - lse_ref[0, 0, a : a + 1, r0 : r0 + n])
                gv = gv + dot(p.astype(BF16), g_a)
                grad_p = dot_t(v, g_a)
                grad_s = (p * (grad_p - dots[a : a + 1, r0 : r0 + n])).astype(BF16)
                gk = gk + dot(grad_s, q_a)
                gq = gq + t_dot(grad_s, head_lanes(k, a))
            gk_refs[b][0, k0 : k0 + keys] = gk.astype(BF16)
            gv_refs[b][0, k0 : k0 + keys] = gv.astype(BF16)
            acc[r0 : r0 + n] = acc[r0 : r0 + n] + gq
        if first:
            gk_refs[1][...] = jnp.zeros_like(gk_refs[1])
            gv_refs[1][...] = jnp.zeros_like(gv_refs[1])

    by_half(blocks, run)
    gq_ref[0] = (acc[...] * scale).astype(BF16)


def pair_spec(length):
    return pl.BlockSpec((1, length, 2 * HEAD_DIM), lambda m, h, prefix: (m, 0, h))


def attention(q, keys, values, prefix):
    micros, rows, width = q.shape
    blocks, total = len(keys), keys[0].shape[1]
    pairs = HEADS // 2
    return pl.pallas_call(
        functools.partial(forward_kernel, blocks),
        out_shape=[
            jax.ShapeDtypeStruct(q.shape, BF16),
            jax.ShapeDtypeStruct((micros, pairs, 8, rows), F32),
        ],
        grid_spec=pltpu.PrefetchScalarGridSpec(
            num_scalar_prefetch=1,
            grid=(micros, pairs),
            in_specs=[pair_spec(rows)] + [pair_spec(total)] * (2 * blocks),
            out_specs=[pair_spec(rows), pl.BlockSpec((1, 1, 8, rows), lambda m, h, prefix: (m, h, 0, 0))],
        ),
        compiler_params=pltpu.CompilerParams(vmem_limit_bytes=48 * 2**20),
        cost_estimate=pl.CostEstimate(
            flops=8 * micros * rows * blocks * total * width,
            bytes_accessed=4 * micros * (rows + blocks * total) * width,
            transcendentals=micros * rows * blocks * total * HEADS,
        ),
        name="attention_forward",
    )(prefix, q, *keys, *values)


def attention_back(q, keys, values, mixed, lse, grad, prefix):
    micros, rows, width = q.shape
    blocks, total = len(keys), keys[0].shape[1]
    pairs = HEADS // 2
    grads = pl.pallas_call(
        functools.partial(backward_kernel, blocks),
        out_shape=[jax.ShapeDtypeStruct(t.shape, BF16) for t in (q, *keys, *values)],
        grid_spec=pltpu.PrefetchScalarGridSpec(
            num_scalar_prefetch=1,
            grid=(micros, pairs),
            in_specs=[
                pair_spec(rows),
                pair_spec(rows),
                pl.BlockSpec((1, 1, 8, rows), lambda m, h, prefix: (m, h, 0, 0)),
                pair_spec(rows),
            ]
            + [pair_spec(total)] * (2 * blocks),
            out_specs=[pair_spec(rows)] + [pair_spec(total)] * (2 * blocks),
            scratch_shapes=[pltpu.VMEM((8, rows), F32), pltpu.VMEM((rows, 2 * HEAD_DIM), F32)],
        ),
        compiler_params=pltpu.CompilerParams(vmem_limit_bytes=48 * 2**20),
        cost_estimate=pl.CostEstimate(
            flops=20 * micros * rows * blocks * total * width,
            bytes_accessed=8 * micros * (rows + blocks * total) * width,
            transcendentals=micros * rows * blocks * total * HEADS,
        ),
        name="attention_backward",
    )(prefix, q, mixed, lse, grad, *keys, *values)
    return grads[0], grads[1 : 1 + blocks], grads[1 + blocks :]


def project_kernel(x_ref, before_ref, wq_ref, wk_ref, wv_ref, qb_ref, vb_ref, q_ref, k0_ref, k1_ref, v0_ref, v1_ref):
    x = x_ref[...]
    q_ref[...] = (dot(x, wq_ref[...]) + qb_ref[...]).astype(BF16)
    for rows_in, k_ref, v_ref in ((x, k0_ref, v0_ref), (before_ref[...], k1_ref, v1_ref)):
        k_ref[...] = dot(rows_in, wk_ref[...]).astype(BF16)
        v_ref[...] = (dot(rows_in, wv_ref[...]) + vb_ref[...]).astype(BF16)


def project(x, before, wq, wk, wv, qb, vb):
    count, width = x.shape
    rows = pl.BlockSpec((2 * BLOCK, width), lambda i: (i, 0))
    whole = pl.BlockSpec((width, width), lambda i: (0, 0))
    vector = pl.BlockSpec((1, width), lambda i: (0, 0))
    return pl.pallas_call(
        project_kernel,
        out_shape=[jax.ShapeDtypeStruct(x.shape, BF16)] * 5,
        grid=(count // (2 * BLOCK),),
        in_specs=[rows, rows, whole, whole, whole, vector, vector],
        out_specs=[rows] * 5,
        compiler_params=pltpu.CompilerParams(vmem_limit_bytes=48 * 2**20),
        cost_estimate=pl.CostEstimate(
            flops=10 * count * width * width, bytes_accessed=14 * count * width + 6 * width * width, transcendentals=0
        ),
        name="project",
    )(x, before, wq, wk, wv, qb[None], vb[None])


def return_kernel(gk_ref, gv_ref, wk_ref, wv_ref, via_ref):
    via_ref[...] = (dot_t(gk_ref[...], wk_ref[...]) + dot_t(gv_ref[...], wv_ref[...])).astype(BF16)


def returned(gk, gv, wk, wv):
    count, width = gk.shape
    rows = pl.BlockSpec((BLOCK, width), lambda i: (i, 0))
    whole = pl.BlockSpec((width, width), lambda i: (0, 0))
    return pl.pallas_call(
        return_kernel,
        out_shape=jax.ShapeDtypeStruct(gk.shape, BF16),
        grid=(count // BLOCK,),
        in_specs=[rows, rows, whole, whole],
        out_specs=rows,
        compiler_params=pltpu.CompilerParams(vmem_limit_bytes=48 * 2**20),
        cost_estimate=pl.CostEstimate(
            flops=4 * count * width * width, bytes_accessed=6 * count * width + 4 * width * width, transcendentals=0
        ),
        name="returned",
    )(gk, gv, wk, wv)


def unproject_kernel(
    x_ref, before_ref, sum1_ref, gq_ref, gk0_ref, gk1_ref, gv0_ref, gv1_ref, wq_ref, wk_ref, wv_ref,
    gx_ref, gwq_ref, gwk_ref, gwv_ref, sums_ref, acc_q, acc_k, acc_v,
):
    step = pl.program_id(0)

    @pl.when(step == 0)
    def _():
        for ref in (acc_q, acc_k, acc_v, sums_ref):
            ref[...] = jnp.zeros_like(ref)

    x, before = x_ref[...], before_ref[...]
    gq, gk0, gk1, gv0, gv1 = gq_ref[...], gk0_ref[...], gk1_ref[...], gv0_ref[...], gv1_ref[...]
    gx_ref[...] = sum1_ref[...] + dot_t(gq, wq_ref[...]) + dot_t(gk0, wk_ref[...]) + dot_t(gv0, wv_ref[...])
    acc_q[...] += t_dot(x, gq)
    acc_k[...] += t_dot(x, gk0) + t_dot(before, gk1)
    acc_v[...] += t_dot(x, gv0) + t_dot(before, gv1)
    sums_ref[0:1] += jnp.sum(gq.astype(F32), axis=0, keepdims=True)
    sums_ref[1:2] += jnp.sum(gv0.astype(F32) + gv1.astype(F32), axis=0, keepdims=True)

    @pl.when(step == pl.num_programs(0) - 1)
    def _():
        gwq_ref[...] = acc_q[...].astype(BF16)
        gwk_ref[...] = acc_k[...].astype(BF16)
        gwv_ref[...] = acc_v[...].astype(BF16)


def unproject(x, before, sum1, gq, gk, gv, wq, wk, wv):
    count, width = x.shape
    rows = pl.BlockSpec((BLOCK, width), lambda i: (i, 0))
    whole = pl.BlockSpec((width, width), lambda i: (0, 0))
    return pl.pallas_call(
        unproject_kernel,
        out_shape=[jax.ShapeDtypeStruct(x.shape, F32)]
        + [jax.ShapeDtypeStruct(wq.shape, BF16)] * 3
        + [jax.ShapeDtypeStruct((8, width), F32)],
        grid=(count // BLOCK,),
        in_specs=[rows] * 8 + [whole] * 3,
        out_specs=[rows] + [whole] * 3 + [pl.BlockSpec((8, width), lambda i: (0, 0))],
        scratch_shapes=[pltpu.VMEM(wq.shape, F32)] * 3,
        compiler_params=pltpu.CompilerParams(vmem_limit_bytes=56 * 2**20),
        cost_estimate=pl.CostEstimate(
            flops=16 * count * width * width, bytes_accessed=24 * count * width + 12 * width * width, transcendentals=0
        ),
        name="unproject",
    )(x, before, sum1, gq, *gk, *gv, wq, wk, wv)


def on_device(
    inputs,
    query_weight,
    key_weight,
    value_weight,
    query_bias,
    value_bias,
    output_weight,
    output_bias,
    first_gain,
    first_shift,
    inner_weight,
    inner_bias,
    outer_weight,
    outer_bias,
    second_gain,
    second_shift,
    prefix,
    cotangent,
):
    micros, rows, width = inputs.shape[1:]
    own = query_weight.shape[0]
    hidden_width = inner_weight.shape[1]
    per = hidden_width // width
    seqs = lax.axis_size("seq")
    x = inputs[0]
    flat_x = x.reshape(micros * rows, width)

    if seqs == 2:
        before = lax.ppermute(x, "seq", [(0, 1)])
        key_x = [flat_x, before.reshape(micros * rows, width)]
    else:
        key_x = [lax.all_gather(x, "seq", axis=1, tiled=True).reshape(-1, width)]

    vectors = (query_bias, value_bias, output_bias, first_gain, first_shift, outer_bias, second_gain, second_shift)
    small = jnp.concatenate([jnp.stack(vectors, axis=1), inner_bias.reshape(own, per)], axis=1)
    small_count = small.shape[1]
    small = jnp.pad(small, ((0, 0), (0, 128 - small_count)))
    full = gather_all(
        [query_weight, key_weight, value_weight, small, output_weight, inner_weight, outer_weight], 1
    )
    full_query, full_key, full_value, small_all, full_output, full_inner, full_outer = full
    small_all = small_all[:, :small_count].astype(F32)
    qb, vb, ob, fg, fs, ub, sg, ss = [small_all[:, i] for i in range(8)]
    ib = small_all[:, 8:].reshape(hidden_width)

    if seqs == 2:
        queries, *kv = project(flat_x, key_x[1], full_query, full_key, full_value, qb, vb)
        keys, values = kv[:2], kv[2:]
    else:
        queries = (dot(flat_x, full_query) + qb).astype(BF16)
        keys = [dot(t, full_key).astype(BF16) for t in key_x]
        values = [(dot(t, full_value) + vb).astype(BF16) for t in key_x]
    queries = queries.reshape(micros, rows, width)
    keys = [t.reshape(micros, -1, width) for t in keys]
    values = [t.reshape(micros, -1, width) for t in values]

    mixed_parts, lse = attention(queries, keys, values, prefix[0])
    mixed = mixed_parts.reshape(micros * rows, width)

    unit1, inv1 = norm_parts(flat_x.astype(F32) + dot(mixed, full_output) + ob)
    middle = unit1 * fg + fs
    middle_low = middle.astype(BF16)
    inner = dot(middle_low, full_inner) + ib
    half_cdf = 0.5 * (1.0 + lax.erf(inner * (0.5**0.5)))
    hidden = (inner * half_cdf).astype(BF16)
    slope = half_cdf + inner * jnp.exp(-0.5 * inner * inner) * 0.3989422804014327
    unit2, inv2 = norm_parts(middle + dot(hidden, full_outer) + ub)
    result = (unit2 * sg + ss).astype(BF16)

    cot = cotangent[0].reshape(micros * rows, width).astype(F32)
    g_sgain = jnp.sum(cot * unit2, axis=0)
    g_sshift = jnp.sum(cot, axis=0)
    grad_mid2 = norm_grad(cot, unit2, inv2, sg)
    grad_outer = grad_mid2.astype(BF16)
    g_ubias = jnp.sum(grad_outer.astype(F32), axis=0)
    g_outer = t_dot(hidden, grad_outer).astype(BF16)
    grad_hidden = dot_t(grad_outer, full_outer).astype(BF16)
    grad_inner = (grad_hidden.astype(F32) * slope).astype(BF16)
    g_ibias = jnp.sum(grad_inner.astype(F32), axis=0)
    g_inner = t_dot(middle_low, grad_inner)
    grad_middle = grad_mid2 + dot_t(grad_inner, full_inner)
    g_fgain = jnp.sum(grad_middle * unit1, axis=0)
    g_fshift = jnp.sum(grad_middle, axis=0)
    grad_sum1 = norm_grad(grad_middle, unit1, inv1, fg)
    grad_branch = grad_sum1.astype(BF16)
    g_obias = jnp.sum(grad_branch.astype(F32), axis=0)
    g_output = t_dot(mixed, grad_branch)
    grad_mixed = dot_t(grad_branch, full_output).astype(BF16).reshape(micros, rows, width)

    grad_q, grad_k, grad_v = attention_back(
        queries, keys, values, mixed_parts, lse, grad_mixed, prefix[0]
    )
    grad_q = grad_q.reshape(micros * rows, width)
    grad_k = [t.reshape(-1, width) for t in grad_k]
    grad_v = [t.reshape(-1, width) for t in grad_v]
    if seqs == 2:
        via_kv = returned(grad_k[1], grad_v[1], full_key, full_value)
        sent = lax.ppermute(via_kv, "seq", [(1, 0)])
        grad_q, _ = lax.optimization_barrier((grad_q, via_kv))
        grad_x, g_query, g_key, g_value, sums = unproject(
            flat_x, key_x[1], grad_sum1, grad_q, grad_k, grad_v, full_query, full_key, full_value
        )
        g_qbias, g_vbias = sums[0], sums[1]
    else:
        g_qbias = jnp.sum(grad_q.astype(F32), axis=0)
        g_vbias = sum(jnp.sum(t.astype(F32), axis=0) for t in grad_v)
        g_query = t_dot(flat_x, grad_q)
        g_key = sum(t_dot(t, g) for t, g in zip(key_x, grad_k))
        g_value = sum(t_dot(t, g) for t, g in zip(key_x, grad_v))
        via_kv = sum(dot_t(k, full_key) + dot_t(v, full_value) for k, v in zip(grad_k, grad_v))
        grad_x = grad_sum1 + dot_t(grad_q, full_query)
        sent = lax.psum_scatter(via_kv.reshape(micros, -1, width), "seq", scatter_dimension=1, tiled=True)
    g_small = jnp.concatenate(
        [
            jnp.stack([g_qbias, g_vbias, g_obias, g_fgain, g_fshift, g_ubias, g_sgain, g_sshift], axis=1),
            g_ibias.reshape(width, per),
        ],
        axis=1,
    )
    g_small = jnp.pad(g_small, ((0, 0), (0, 128 - small_count)))
    own_grads = scatter_all([g_outer, g_inner, g_output, g_query, g_key, g_value, g_small], 3)
    own_outer, own_inner, own_output, own_query, own_key, own_value, own_small = own_grads

    grad_x = grad_x.reshape(micros, rows, width) + sent.reshape(micros, rows, width).astype(F32)

    vec = own_small[:, :small_count]
    v_of = [vec[:, i] for i in range(8)]
    outputs = result.reshape(micros, rows, width)[None]
    return (
        outputs,
        grad_x[None],
        own_query,
        own_key,
        own_value,
        v_of[0],
        v_of[1],
        own_output,
        v_of[2],
        v_of[3],
        v_of[4],
        own_inner,
        vec[:, 8:].reshape(own * per),
        own_outer,
        v_of[5],
        v_of[6],
        v_of[7],
    )


def solution(mesh):
    act = P("dp", None, "seq", None)
    mat = P(BOTH, None)
    vec = P(BOTH)
    params = (mat, mat, mat, vec, vec, mat, vec, vec, vec, mat, vec, mat, vec, vec, vec)
    return jax.shard_map(
        on_device,
        mesh=mesh,
        in_specs=(act,) + params + (P("dp", None), act),
        out_specs=(act, act) + params,
        check_vma=False,
    )
```

```python
import functools

import jax
import jax.numpy as jnp
from jax import lax
from jax.experimental import pallas as pl
from jax.experimental.pallas import tpu as pltpu
from jax.sharding import PartitionSpec as P

HEADS = 12
HEAD_DIM = 64
EPS = 1e-05
BOTH = ("seq", "dp")
F32 = jnp.float32
BF16 = jnp.bfloat16
MESH = pl.DeviceIdType.MESH
LINE = 4
SQUARE = 4
CHIPS = LINE * SQUARE


def device_coords(p, z, core):
    return ((p + 1) // 2) % 2, 4 * z + 2 * (p // 2) + core


def device_index(p, z, core):
    y, dp = device_coords(p, z, core)
    return y * CHIPS + dp


def whereabouts():
    y, dp = lax.axis_index("seq"), lax.axis_index("dp")
    z, x, core = dp // 4, (dp // 2) % 2, dp % 2
    return 2 * x + (x + y) % 2, z, core


def heights(z):
    code = jnp.where(z == 0, 1 + 4 * 2 + 16 * 3, jnp.where(z == 1, 0 + 4 * 2 + 16 * 3, jnp.where(z == 2, 1 + 4 * 3, 2 + 4 * 1)))
    return [z, code % 4, (code // 4) % 4, (code // 16) % 4]


def meet(z, always, up, down):
    barrier = pltpu.get_barrier_semaphore()

    def greet(target):
        pl.semaphore_signal(barrier, inc=1, device_id=target, device_id_type=MESH)

    for target in always:
        greet(target)
    pl.when(z < LINE - 1)(lambda: greet(up))
    pl.when(z > 0)(lambda: greet(down))
    ends = jnp.where(z == 0, 1, 0) + jnp.where(z == LINE - 1, 1, 0)
    pl.semaphore_wait(barrier, len(always) + 2 - ends)


def remote(src, dst, send, recv, target):
    return pltpu.make_async_remote_copy(
        src_ref=src, dst_ref=dst, send_sem=send, recv_sem=recv, device_id=target, device_id_type=MESH
    )


def neighbours():
    p, z, core = whereabouts()
    turn = 1 + 2 * core
    ahead, behind, across = (p + turn) % SQUARE, (p + SQUARE - turn) % SQUARE, (p + 2) % SQUARE
    to_ahead, to_behind = device_coords(ahead, z, core), device_coords(behind, z, core)
    partner = device_coords(p, z, 1 - core)
    up = device_coords(p, jnp.minimum(z + 1, LINE - 1), core)
    down = device_coords(p, jnp.maximum(z - 1, 0), core)
    return p, z, core, ahead, behind, across, to_ahead, to_behind, partner, up, down


def gather_kernel(count, *refs):
    s, o = refs[:count], refs[count : 2 * count]
    sems = refs[2 * count :]
    local_sem, pair_send, pair_recv, up_send, down_send, line_recv = sems[:6]
    one_send, one_recv, two_send, two_recv, far_send, far_recv = sems[6:]
    p, z, core, ahead, behind, across, to_ahead, to_behind, partner, up, down = neighbours()

    def place(k, q, t):
        return o[k].at[device_index(q, t, core)]

    def local(k):
        return pltpu.make_async_copy(s[k], place(k, p, z), local_sem.at[k])

    def to_pair(k, q, t, src):
        return remote(src, place(k, q, t), pair_send.at[k, q, t], pair_recv.at[k, q, t], partner)

    def rise(k, t, src):
        return remote(src, place(k, p, t), up_send.at[k, t], line_recv.at[k, t], up)

    def sink(k, t, src):
        return remote(src, place(k, p, t), down_send.at[k, t], line_recv.at[k, t], down)

    def one(k, t, src):
        return remote(src, place(k, p, t), one_send.at[k, t], one_recv.at[k, t], to_ahead)

    def two(k, t, src):
        return remote(src, place(k, p, t), two_send.at[k, t], two_recv.at[k, t], to_behind)

    def far(k, t, src):
        return remote(src, place(k, behind, t), far_send.at[k, t], far_recv.at[k, t], to_ahead)

    meet(z, (to_ahead, to_behind, partner), up, down)
    order = heights(z)

    def spread(k, t, src):
        pl.when((t <= z) & (z < LINE - 1))(lambda: rise(k, t, src).start())
        pl.when((t >= z) & (z > 0))(lambda: sink(k, t, src).start())
        one(k, t, src).start()
        two(k, t, src).start()
        to_pair(k, p, t, src).start()

    def column(k, t):
        rise(k, t, place(k, p, t)).wait_recv()
        spread(k, t, place(k, p, t))

    def sides(k, t):
        one(k, t, place(k, behind, t)).wait_recv()
        far(k, t, place(k, behind, t)).start()
        to_pair(k, behind, t, place(k, behind, t)).start()
        two(k, t, place(k, ahead, t)).wait_recv()
        to_pair(k, ahead, t, place(k, ahead, t)).start()

    def corner(k, t):
        far(k, t, place(k, across, t)).wait_recv()
        to_pair(k, across, t, place(k, across, t)).start()

    for k in range(count):
        spread(k, z, s[k])
        local(k).start()
    for i in range(1, LINE):
        for k in range(count):
            column(k, order[i])
            sides(k, order[i - 1])
            if i > 1:
                corner(k, order[i - 2])
    for k in range(count):
        sides(k, order[LINE - 1])
        corner(k, order[LINE - 2])
    for k in range(count):
        corner(k, order[LINE - 1])

    def drain(i, _):
        q, t = i // LINE, i % LINE
        for k in range(count):
            copy = to_pair(k, q, t, place(k, q, t))
            copy.wait_send()
            copy.wait_recv()
        return 0

    lax.fori_loop(0, CHIPS, drain, 0)

    def drain_line(t, _):
        for k in range(count):
            src = place(k, p, t)
            pl.when((t <= z) & (z < LINE - 1))(lambda: rise(k, t, src).wait_send())
            pl.when((t >= z) & (z > 0))(lambda: sink(k, t, src).wait_send())
            one(k, t, src).wait_send()
            two(k, t, src).wait_send()
            far(k, t, src).wait_send()
        return 0

    lax.fori_loop(0, LINE, drain_line, 0)
    for k in range(count):
        local(k).wait()


def grid_gather(parts, collective_id):
    count = len(parts)
    dma = lambda *n: pltpu.SemaphoreType.DMA((count,) + n)
    return pl.pallas_call(
        functools.partial(gather_kernel, count),
        out_shape=[jax.ShapeDtypeStruct((2 * CHIPS,) + p.shape, p.dtype) for p in parts],
        in_specs=[pl.BlockSpec(memory_space=pltpu.VMEM)] * count,
        out_specs=[pl.BlockSpec(memory_space=pl.ANY)] * count,
        scratch_shapes=[dma(), dma(SQUARE, LINE), dma(SQUARE, LINE)] + [dma(LINE)] * 9,
        compiler_params=pltpu.CompilerParams(collective_id=collective_id, has_side_effects=True),
        name="grid_gather",
    )(*parts)


def scatter_kernel(count, *refs):
    g, out = refs[:count], refs[count : 2 * count]
    own, pair, far_in, one_in, two_in, up_in, down_in = [
        refs[(2 + i) * count : (3 + i) * count] for i in range(7)
    ]
    sems = refs[9 * count :]
    local_sem, pair_send, pair_recv = sems[:3]
    far_send, far_recv, one_send, one_recv, two_send, two_recv, up_send, up_recv, down_send, down_recv = sems[3:]
    p, z, core, ahead, behind, across, to_ahead, to_behind, partner, up, down = neighbours()

    def local(k, q, t):
        return pltpu.make_async_copy(g[k].at[device_index(q, t, core)], own[k].at[q, t], local_sem.at[k, q, t])

    def to_pair(k, q, t):
        return remote(
            g[k].at[device_index(q, t, 1 - core)],
            pair[k].at[q, t],
            pair_send.at[k, q, t],
            pair_recv.at[k, q, t],
            partner,
        )

    def far(k, t, src):
        return remote(src, far_in[k].at[t], far_send.at[k, t], far_recv.at[k, t], to_behind)

    def one(k, t, src):
        return remote(src, one_in[k].at[t], one_send.at[k, t], one_recv.at[k, t], to_behind)

    def two(k, t, src):
        return remote(src, two_in[k].at[t], two_send.at[k, t], two_recv.at[k, t], to_ahead)

    def rise(k, t, src):
        return remote(src, up_in[k].at[t], up_send.at[k, t], up_recv.at[k, t], up)

    def sink(k, t, src):
        return remote(src, down_in[k].at[t], down_send.at[k, t], down_recv.at[k, t], down)

    def term(k, q, t):
        local(k, q, t).wait()
        to_pair(k, q, t).wait_recv()
        return own[k][q, t].astype(F32) + pair[k][q, t].astype(F32)

    meet(z, (to_ahead, to_behind, partner), up, down)
    order = heights(z)[::-1]
    for t in order:
        for q in (across, behind, ahead, p):
            for k in range(count):
                to_pair(k, q, t).start()
                local(k, q, t).start()

    def open_square(k, t):
        pair[k][across, t] = term(k, across, t).astype(BF16)
        far(k, t, pair[k].at[across, t]).start()
        pair[k][ahead, t] = term(k, ahead, t).astype(BF16)
        two(k, t, pair[k].at[ahead, t]).start()

    def pass_square(k, t):
        mine = term(k, behind, t)
        far(k, t, pair[k].at[across, t]).wait_recv()
        far_in[k][t] = (far_in[k][t].astype(F32) + mine).astype(BF16)
        one(k, t, far_in[k].at[t]).start()

    def close_square(k, t):
        mine = term(k, p, t)
        two(k, t, pair[k].at[ahead, t]).wait_recv()
        mine = mine + two_in[k][t].astype(F32)
        one(k, t, far_in[k].at[t]).wait_recv()
        return mine + one_in[k][t].astype(F32)

    def column(k, t):
        mine = close_square(k, t)

        @pl.when((t > z) & (z > 0))
        def _():
            rise(k, t, one_in[k].at[t]).wait_recv()

        @pl.when((t < z) & (z < LINE - 1))
        def _():
            sink(k, t, one_in[k].at[t]).wait_recv()

        @pl.when(((t > z) & (z == 0)) | ((t < z) & (z == LINE - 1)))
        def _():
            one_in[k][t] = mine.astype(BF16)

        @pl.when((t > z) & (z > 0))
        def _():
            one_in[k][t] = (mine + up_in[k][t].astype(F32)).astype(BF16)

        @pl.when((t < z) & (z < LINE - 1))
        def _():
            one_in[k][t] = (mine + down_in[k][t].astype(F32)).astype(BF16)

        pl.when(t > z)(lambda: rise(k, t, one_in[k].at[t]).start())
        pl.when(t < z)(lambda: sink(k, t, one_in[k].at[t]).start())

    def finish(k):
        out[k][...] = close_square(k, z)

        @pl.when(z > 0)
        def _():
            rise(k, z, one_in[k].at[z]).wait_recv()
            out[k][...] += up_in[k][z].astype(F32)

        @pl.when(z < LINE - 1)
        def _():
            sink(k, z, one_in[k].at[z]).wait_recv()
            out[k][...] += down_in[k][z].astype(F32)

    for k in range(count):
        open_square(k, order[0])

    code = order[0] + 4 * order[1] + 16 * order[2] + 64 * order[3]

    def at(i):
        return (code // jnp.where(i == 0, 1, jnp.where(i == 1, 4, jnp.where(i == 2, 16, 64)))) % 4

    def step(i, _):
        for k in range(count):
            open_square(k, at(i + 1))
            pass_square(k, at(i))
        for k in range(count):
            column(k, at(i))
        return 0

    lax.fori_loop(0, LINE - 1, step, 0)
    for k in range(count):
        pass_square(k, z)
    for k in range(count):
        finish(k)

    def drain(i, _):
        q, t = i // LINE, i % LINE
        for k in range(count):
            to_pair(k, q, t).wait_send()
        return 0

    lax.fori_loop(0, CHIPS, drain, 0)

    def drain_line(t, _):
        for k in range(count):
            src = one_in[k].at[t]
            far(k, t, src).wait_send()
            one(k, t, src).wait_send()
            two(k, t, src).wait_send()
            pl.when(t > z)(lambda: rise(k, t, src).wait_send())
            pl.when(t < z)(lambda: sink(k, t, src).wait_send())
        return 0

    lax.fori_loop(0, LINE, drain_line, 0)


def grid_scatter(parts, collective_id):
    count = len(parts)
    slots = lambda *n: [pltpu.VMEM(n + p.shape[1:], BF16) for p in parts]
    dma = lambda *n: pltpu.SemaphoreType.DMA((count,) + n)
    return pl.pallas_call(
        functools.partial(scatter_kernel, count),
        out_shape=[jax.ShapeDtypeStruct(p.shape[1:], F32) for p in parts],
        in_specs=[pl.BlockSpec(memory_space=pl.ANY)] * count,
        out_specs=[pl.BlockSpec(memory_space=pltpu.VMEM)] * count,
        scratch_shapes=slots(SQUARE, LINE) * 2 + slots(LINE) * 5 + [dma(SQUARE, LINE)] * 3 + [dma(LINE)] * 10,
        compiler_params=pltpu.CompilerParams(
            collective_id=collective_id, has_side_effects=True, vmem_limit_bytes=60 * 2**20
        ),
        name="grid_scatter",
    )(*parts)


def on_grid():
    return lax.axis_size("seq") == 2 and lax.axis_size("dp") == CHIPS


def gather_all(parts, collective_id):
    if on_grid():
        full = grid_gather(parts, collective_id)
        return [f.reshape((-1,) + f.shape[2:]) for f in full]
    return [lax.all_gather(p, BOTH, axis=0, tiled=True) for p in parts]


def scatter_all(parts, collective_id):
    if on_grid():
        split = [p.astype(BF16).reshape(2 * CHIPS, -1, p.shape[1]) for p in parts]
        return grid_scatter(split, collective_id)
    return [lax.psum_scatter(p.astype(BF16), BOTH, scatter_dimension=0, tiled=True).astype(F32) for p in parts]


def dot(a, b):
    return jnp.dot(a, b, preferred_element_type=F32)


def dot_t(a, b):
    return lax.dot_general(a, b, (((1,), (1,)), ((), ())), preferred_element_type=F32)


def t_dot(a, b):
    return lax.dot_general(a, b, (((0,), (0,)), ((), ())), preferred_element_type=F32)


def norm_parts(v):
    center = v - jnp.mean(v, axis=-1, keepdims=True)
    inv = lax.rsqrt(jnp.mean(center * center, axis=-1, keepdims=True) + EPS)
    return center * inv, inv


def norm_grad(grad, unit, inv, gain):
    g = grad * gain
    mean_g = jnp.mean(g, axis=-1, keepdims=True)
    mean_gu = jnp.mean(g * unit, axis=-1, keepdims=True)
    return inv * (g - mean_g - unit * mean_gu)


BLOCK = 256


def head_lanes(v, a):
    lane = lax.broadcasted_iota(jnp.int32, v.shape, 1)
    return jnp.where(lane // HEAD_DIM == a, v, jnp.zeros_like(v))


def row_plans(rows, blocks, total, first):
    if blocks == 1:
        return [(0, rows, [(0, 0, total, True)])]
    if first:
        return [(0, rows, [(0, 0, rows, True)])]
    plans = []
    for r0 in range(0, rows, BLOCK):
        parts = [(1, 0, rows, False)]
        if r0:
            parts.append((0, 0, r0, False))
        plans.append((r0, BLOCK, parts + [(0, r0, BLOCK, True)]))
    return plans


def key_plans(rows, blocks, total, first):
    if blocks == 1:
        return [(0, 0, total, 0, rows, True)]
    if first:
        return [(0, k0, BLOCK, 0, rows, True) for k0 in range(0, rows, BLOCK)]
    plans = [(1, k0, BLOCK, 0, rows, False) for k0 in range(0, rows, BLOCK)]
    return plans + [(0, k0, BLOCK, k0, rows - k0, True) for k0 in range(0, rows, BLOCK)]


def by_half(blocks, run):
    if blocks == 1:
        run(False)
    else:
        pl.when(lax.axis_index("seq") == 0)(lambda: run(True))
        pl.when(lax.axis_index("seq") != 0)(lambda: run(False))


def allowed_of(own_first, k0, keys, r0, rows, first_pos, prefix_len, key_axis):
    shape = (keys, rows) if key_axis == 0 else (rows, keys)
    key_base = first_pos if own_first else 0
    key_at = key_base + k0 + lax.broadcasted_iota(jnp.int32, shape, key_axis)
    row_at = first_pos + r0 + lax.broadcasted_iota(jnp.int32, shape, 1 - key_axis)
    return key_at <= jnp.maximum(row_at, prefix_len - 1)


def forward_kernel(blocks, prefix_ref, q_ref, *refs):
    k_refs, v_refs, (o_ref, lse_ref) = refs[:blocks], refs[blocks : 2 * blocks], refs[2 * blocks :]
    rows, total = q_ref.shape[1], k_refs[0].shape[1]
    prefix_len = prefix_ref[pl.program_id(0)]
    first_pos = lax.axis_index("seq") * rows
    own_first = blocks == 2

    def run(first):
        for r0, n, parts in row_plans(rows, blocks, total, first):
            q = q_ref[0, r0 : r0 + n] * jnp.asarray(HEAD_DIM**-0.5, BF16)
            mixed = jnp.zeros((n, 2 * HEAD_DIM), F32)
            logs = jnp.zeros((n, 2 * HEAD_DIM), F32)
            lane = lax.broadcasted_iota(jnp.int32, mixed.shape, 1)
            for a in range(2):
                q_a = head_lanes(q, a)
                scores = []
                for b, k0, keys, masked in parts:
                    s = dot_t(q_a, k_refs[b][0, k0 : k0 + keys])
                    if masked:
                        ok = allowed_of(own_first, k0, keys, r0, n, first_pos, prefix_len, 1)
                        s = jnp.where(ok, s, -1e30)
                    scores.append(s)
                top = functools.reduce(jnp.maximum, [jnp.max(s, axis=1, keepdims=True) for s in scores])
                total_exp = jnp.zeros_like(top)
                out = jnp.zeros_like(mixed)
                for s, (b, k0, keys, _) in zip(scores, parts):
                    p = jnp.exp(s - top)
                    total_exp = total_exp + jnp.sum(p, axis=1, keepdims=True)
                    out = out + dot(p.astype(BF16), v_refs[b][0, k0 : k0 + keys])
                mine = lane // HEAD_DIM == a
                mixed = jnp.where(mine, out / total_exp, mixed)
                logs = jnp.where(mine, top + jnp.log(total_exp), logs)
            o_ref[0, r0 : r0 + n] = mixed.astype(BF16)
            logs = logs.T
            lse_ref[0, 0, 0:1, r0 : r0 + n] = logs[0:1]
            lse_ref[0, 0, 1:2, r0 : r0 + n] = logs[HEAD_DIM : HEAD_DIM + 1]

    by_half(blocks, run)


def backward_kernel(blocks, prefix_ref, q_ref, o_ref, lse_ref, g_ref, *refs):
    k_refs, v_refs, gq_ref = refs[:blocks], refs[blocks : 2 * blocks], refs[2 * blocks]
    gk_refs, gv_refs = refs[2 * blocks + 1 : 3 * blocks + 1], refs[3 * blocks + 1 : 4 * blocks + 1]
    dots, acc = refs[4 * blocks + 1 :]
    rows, total = q_ref.shape[1], k_refs[0].shape[1]
    prefix_len = prefix_ref[pl.program_id(0)]
    first_pos = lax.axis_index("seq") * rows
    own_first = blocks == 2
    scale = HEAD_DIM**-0.5
    product = (g_ref[0].astype(F32) * o_ref[0].astype(F32)).T
    for a in range(2):
        dots[a : a + 1] = jnp.sum(product[a * HEAD_DIM : (a + 1) * HEAD_DIM], axis=0, keepdims=True)
    acc[...] = jnp.zeros_like(acc)

    def run(first):
        for b, k0, keys, r0, n, masked in key_plans(rows, blocks, total, first):
            k = k_refs[b][0, k0 : k0 + keys]
            v = v_refs[b][0, k0 : k0 + keys]
            q = q_ref[0, r0 : r0 + n] * jnp.asarray(scale, BF16)
            g = g_ref[0, r0 : r0 + n]
            gk = jnp.zeros((keys, 2 * HEAD_DIM), F32)
            gv = jnp.zeros((keys, 2 * HEAD_DIM), F32)
            gq = jnp.zeros((n, 2 * HEAD_DIM), F32)
            for a in range(2):
                q_a, g_a = head_lanes(q, a), head_lanes(g, a)
                s = dot_t(k, q_a)
                if masked:
                    ok = allowed_of(own_first, k0, keys, r0, n, first_pos, prefix_len, 0)
                    s = jnp.where(ok, s, -1e30)
                p = jnp.exp(s - lse_ref[0, 0, a : a + 1, r0 : r0 + n])
                gv = gv + dot(p.astype(BF16), g_a)
                grad_p = dot_t(v, g_a)
                grad_s = (p * (grad_p - dots[a : a + 1, r0 : r0 + n])).astype(BF16)
                gk = gk + dot(grad_s, q_a)
                gq = gq + t_dot(grad_s, head_lanes(k, a))
            gk_refs[b][0, k0 : k0 + keys] = gk.astype(BF16)
            gv_refs[b][0, k0 : k0 + keys] = gv.astype(BF16)
            acc[r0 : r0 + n] = acc[r0 : r0 + n] + gq
        if first:
            gk_refs[1][...] = jnp.zeros_like(gk_refs[1])
            gv_refs[1][...] = jnp.zeros_like(gv_refs[1])

    by_half(blocks, run)
    gq_ref[0] = (acc[...] * scale).astype(BF16)


def pair_spec(length):
    return pl.BlockSpec((1, length, 2 * HEAD_DIM), lambda m, h, prefix: (m, 0, h))


def attention(q, keys, values, prefix):
    micros, rows, width = q.shape
    blocks, total = len(keys), keys[0].shape[1]
    pairs = HEADS // 2
    return pl.pallas_call(
        functools.partial(forward_kernel, blocks),
        out_shape=[
            jax.ShapeDtypeStruct(q.shape, BF16),
            jax.ShapeDtypeStruct((micros, pairs, 8, rows), F32),
        ],
        grid_spec=pltpu.PrefetchScalarGridSpec(
            num_scalar_prefetch=1,
            grid=(micros, pairs),
            in_specs=[pair_spec(rows)] + [pair_spec(total)] * (2 * blocks),
            out_specs=[pair_spec(rows), pl.BlockSpec((1, 1, 8, rows), lambda m, h, prefix: (m, h, 0, 0))],
        ),
        compiler_params=pltpu.CompilerParams(vmem_limit_bytes=48 * 2**20),
        cost_estimate=pl.CostEstimate(
            flops=8 * micros * rows * blocks * total * width,
            bytes_accessed=4 * micros * (rows + blocks * total) * width,
            transcendentals=micros * rows * blocks * total * HEADS,
        ),
        name="attention_forward",
    )(prefix, q, *keys, *values)


def attention_back(q, keys, values, mixed, lse, grad, prefix):
    micros, rows, width = q.shape
    blocks, total = len(keys), keys[0].shape[1]
    pairs = HEADS // 2
    grads = pl.pallas_call(
        functools.partial(backward_kernel, blocks),
        out_shape=[jax.ShapeDtypeStruct(t.shape, BF16) for t in (q, *keys, *values)],
        grid_spec=pltpu.PrefetchScalarGridSpec(
            num_scalar_prefetch=1,
            grid=(micros, pairs),
            in_specs=[
                pair_spec(rows),
                pair_spec(rows),
                pl.BlockSpec((1, 1, 8, rows), lambda m, h, prefix: (m, h, 0, 0)),
                pair_spec(rows),
            ]
            + [pair_spec(total)] * (2 * blocks),
            out_specs=[pair_spec(rows)] + [pair_spec(total)] * (2 * blocks),
            scratch_shapes=[pltpu.VMEM((8, rows), F32), pltpu.VMEM((rows, 2 * HEAD_DIM), F32)],
        ),
        compiler_params=pltpu.CompilerParams(vmem_limit_bytes=48 * 2**20),
        cost_estimate=pl.CostEstimate(
            flops=20 * micros * rows * blocks * total * width,
            bytes_accessed=8 * micros * (rows + blocks * total) * width,
            transcendentals=micros * rows * blocks * total * HEADS,
        ),
        name="attention_backward",
    )(prefix, q, mixed, lse, grad, *keys, *values)
    return grads[0], grads[1 : 1 + blocks], grads[1 + blocks :]


def project_kernel(x_ref, before_ref, wq_ref, wk_ref, wv_ref, qb_ref, vb_ref, q_ref, k0_ref, k1_ref, v0_ref, v1_ref):
    x = x_ref[...]
    q_ref[...] = (dot(x, wq_ref[...]) + qb_ref[...]).astype(BF16)
    for rows_in, k_ref, v_ref in ((x, k0_ref, v0_ref), (before_ref[...], k1_ref, v1_ref)):
        k_ref[...] = dot(rows_in, wk_ref[...]).astype(BF16)
        v_ref[...] = (dot(rows_in, wv_ref[...]) + vb_ref[...]).astype(BF16)


def project(x, before, wq, wk, wv, qb, vb):
    count, width = x.shape
    rows = pl.BlockSpec((2 * BLOCK, width), lambda i: (i, 0))
    whole = pl.BlockSpec((width, width), lambda i: (0, 0))
    vector = pl.BlockSpec((1, width), lambda i: (0, 0))
    return pl.pallas_call(
        project_kernel,
        out_shape=[jax.ShapeDtypeStruct(x.shape, BF16)] * 5,
        grid=(count // (2 * BLOCK),),
        in_specs=[rows, rows, whole, whole, whole, vector, vector],
        out_specs=[rows] * 5,
        compiler_params=pltpu.CompilerParams(vmem_limit_bytes=48 * 2**20),
        cost_estimate=pl.CostEstimate(
            flops=10 * count * width * width, bytes_accessed=14 * count * width + 6 * width * width, transcendentals=0
        ),
        name="project",
    )(x, before, wq, wk, wv, qb[None], vb[None])


def return_kernel(gk_ref, gv_ref, wk_ref, wv_ref, via_ref):
    via_ref[...] = (dot_t(gk_ref[...], wk_ref[...]) + dot_t(gv_ref[...], wv_ref[...])).astype(BF16)


def returned(gk, gv, wk, wv):
    count, width = gk.shape
    rows = pl.BlockSpec((BLOCK, width), lambda i: (i, 0))
    whole = pl.BlockSpec((width, width), lambda i: (0, 0))
    return pl.pallas_call(
        return_kernel,
        out_shape=jax.ShapeDtypeStruct(gk.shape, BF16),
        grid=(count // BLOCK,),
        in_specs=[rows, rows, whole, whole],
        out_specs=rows,
        compiler_params=pltpu.CompilerParams(vmem_limit_bytes=48 * 2**20),
        cost_estimate=pl.CostEstimate(
            flops=4 * count * width * width, bytes_accessed=6 * count * width + 4 * width * width, transcendentals=0
        ),
        name="returned",
    )(gk, gv, wk, wv)


def unproject_kernel(
    x_ref, before_ref, sum1_ref, gq_ref, gk0_ref, gk1_ref, gv0_ref, gv1_ref, wq_ref, wk_ref, wv_ref,
    gx_ref, gwq_ref, gwk_ref, gwv_ref, sums_ref, acc_q, acc_k, acc_v,
):
    step = pl.program_id(0)

    @pl.when(step == 0)
    def _():
        for ref in (acc_q, acc_k, acc_v, sums_ref):
            ref[...] = jnp.zeros_like(ref)

    x, before = x_ref[...], before_ref[...]
    gq, gk0, gk1, gv0, gv1 = gq_ref[...], gk0_ref[...], gk1_ref[...], gv0_ref[...], gv1_ref[...]
    gx_ref[...] = sum1_ref[...] + dot_t(gq, wq_ref[...]) + dot_t(gk0, wk_ref[...]) + dot_t(gv0, wv_ref[...])
    acc_q[...] += t_dot(x, gq)
    acc_k[...] += t_dot(x, gk0) + t_dot(before, gk1)
    acc_v[...] += t_dot(x, gv0) + t_dot(before, gv1)
    sums_ref[0:1] += jnp.sum(gq.astype(F32), axis=0, keepdims=True)
    sums_ref[1:2] += jnp.sum(gv0.astype(F32) + gv1.astype(F32), axis=0, keepdims=True)

    @pl.when(step == pl.num_programs(0) - 1)
    def _():
        gwq_ref[...] = acc_q[...].astype(BF16)
        gwk_ref[...] = acc_k[...].astype(BF16)
        gwv_ref[...] = acc_v[...].astype(BF16)


def unproject(x, before, sum1, gq, gk, gv, wq, wk, wv):
    count, width = x.shape
    rows = pl.BlockSpec((BLOCK, width), lambda i: (i, 0))
    whole = pl.BlockSpec((width, width), lambda i: (0, 0))
    return pl.pallas_call(
        unproject_kernel,
        out_shape=[jax.ShapeDtypeStruct(x.shape, F32)]
        + [jax.ShapeDtypeStruct(wq.shape, BF16)] * 3
        + [jax.ShapeDtypeStruct((8, width), F32)],
        grid=(count // BLOCK,),
        in_specs=[rows] * 8 + [whole] * 3,
        out_specs=[rows] + [whole] * 3 + [pl.BlockSpec((8, width), lambda i: (0, 0))],
        scratch_shapes=[pltpu.VMEM(wq.shape, F32)] * 3,
        compiler_params=pltpu.CompilerParams(vmem_limit_bytes=56 * 2**20),
        cost_estimate=pl.CostEstimate(
            flops=16 * count * width * width, bytes_accessed=24 * count * width + 12 * width * width, transcendentals=0
        ),
        name="unproject",
    )(x, before, sum1, gq, *gk, *gv, wq, wk, wv)


def on_device(
    inputs,
    query_weight,
    key_weight,
    value_weight,
    query_bias,
    value_bias,
    output_weight,
    output_bias,
    first_gain,
    first_shift,
    inner_weight,
    inner_bias,
    outer_weight,
    outer_bias,
    second_gain,
    second_shift,
    prefix,
    cotangent,
):
    micros, rows, width = inputs.shape[1:]
    own = query_weight.shape[0]
    hidden_width = inner_weight.shape[1]
    per = hidden_width // width
    seqs = lax.axis_size("seq")
    x = inputs[0]
    flat_x = x.reshape(micros * rows, width)

    if seqs == 2:
        before = lax.ppermute(x, "seq", [(0, 1)])
        key_x = [flat_x, before.reshape(micros * rows, width)]
    else:
        key_x = [lax.all_gather(x, "seq", axis=1, tiled=True).reshape(-1, width)]

    vectors = (query_bias, value_bias, output_bias, first_gain, first_shift, outer_bias, second_gain, second_shift)
    lanes = lambda v: jnp.pad(v, ((0, 0),) * (v.ndim - 1) + ((0, 128 - v.shape[-1]),))
    small = jnp.stack([lanes(v) for v in vectors + (inner_bias,)])
    small = jnp.pad(small, ((0, 16 - small.shape[0]), (0, 0)))
    full = gather_all(
        [query_weight, key_weight, value_weight, small, output_weight, inner_weight, outer_weight], 1
    )
    full_query, full_key, full_value, small_all, full_output, full_inner, full_outer = full
    small_all = small_all.reshape(-1, 16, 128)
    shares = small_all.shape[0]
    by_vector = small_all[:, :8, :own].transpose(1, 0, 2).reshape(8, width).astype(F32)
    qb, vb, ob, fg, fs, ub, sg, ss = [by_vector[i] for i in range(8)]
    ib = small_all[:, 8, : own * per].reshape(hidden_width).astype(F32)

    if seqs == 2:
        queries, *kv = project(flat_x, key_x[1], full_query, full_key, full_value, qb, vb)
        keys, values = kv[:2], kv[2:]
    else:
        queries = (dot(flat_x, full_query) + qb).astype(BF16)
        keys = [dot(t, full_key).astype(BF16) for t in key_x]
        values = [(dot(t, full_value) + vb).astype(BF16) for t in key_x]
    queries = queries.reshape(micros, rows, width)
    keys = [t.reshape(micros, -1, width) for t in keys]
    values = [t.reshape(micros, -1, width) for t in values]

    mixed_parts, lse = attention(queries, keys, values, prefix[0])
    mixed = mixed_parts.reshape(micros * rows, width)

    unit1, inv1 = norm_parts(flat_x.astype(F32) + dot(mixed, full_output) + ob)
    middle = unit1 * fg + fs
    middle_low = middle.astype(BF16)
    inner = dot(middle_low, full_inner) + ib
    half_cdf = 0.5 * (1.0 + lax.erf(inner * (0.5**0.5)))
    hidden = (inner * half_cdf).astype(BF16)
    slope = half_cdf + inner * jnp.exp(-0.5 * inner * inner) * 0.3989422804014327
    unit2, inv2 = norm_parts(middle + dot(hidden, full_outer) + ub)
    result = (unit2 * sg + ss).astype(BF16)

    cot = cotangent[0].reshape(micros * rows, width).astype(F32)
    g_sgain = jnp.sum(cot * unit2, axis=0)
    g_sshift = jnp.sum(cot, axis=0)
    grad_mid2 = norm_grad(cot, unit2, inv2, sg)
    grad_outer = grad_mid2.astype(BF16)
    g_ubias = jnp.sum(grad_outer.astype(F32), axis=0)
    g_outer = t_dot(hidden, grad_outer).astype(BF16)
    grad_hidden = dot_t(grad_outer, full_outer).astype(BF16)
    grad_inner = (grad_hidden.astype(F32) * slope).astype(BF16)
    g_ibias = jnp.sum(grad_inner.astype(F32), axis=0)
    g_inner = t_dot(middle_low, grad_inner)
    grad_middle = grad_mid2 + dot_t(grad_inner, full_inner)
    g_fgain = jnp.sum(grad_middle * unit1, axis=0)
    g_fshift = jnp.sum(grad_middle, axis=0)
    grad_sum1 = norm_grad(grad_middle, unit1, inv1, fg)
    grad_branch = grad_sum1.astype(BF16)
    g_obias = jnp.sum(grad_branch.astype(F32), axis=0)
    g_output = t_dot(mixed, grad_branch)
    grad_mixed = dot_t(grad_branch, full_output).astype(BF16).reshape(micros, rows, width)

    grad_q, grad_k, grad_v = attention_back(
        queries, keys, values, mixed_parts, lse, grad_mixed, prefix[0]
    )
    grad_q = grad_q.reshape(micros * rows, width)
    grad_k = [t.reshape(-1, width) for t in grad_k]
    grad_v = [t.reshape(-1, width) for t in grad_v]
    if seqs == 2:
        via_kv = returned(grad_k[1], grad_v[1], full_key, full_value)
        sent = lax.ppermute(via_kv, "seq", [(1, 0)])
        grad_q, _ = lax.optimization_barrier((grad_q, via_kv))
        grad_x, g_query, g_key, g_value, sums = unproject(
            flat_x, key_x[1], grad_sum1, grad_q, grad_k, grad_v, full_query, full_key, full_value
        )
        g_qbias, g_vbias = sums[0], sums[1]
    else:
        g_qbias = jnp.sum(grad_q.astype(F32), axis=0)
        g_vbias = sum(jnp.sum(t.astype(F32), axis=0) for t in grad_v)
        g_query = t_dot(flat_x, grad_q)
        g_key = sum(t_dot(t, g) for t, g in zip(key_x, grad_k))
        g_value = sum(t_dot(t, g) for t, g in zip(key_x, grad_v))
        via_kv = sum(dot_t(k, full_key) + dot_t(v, full_value) for k, v in zip(grad_k, grad_v))
        grad_x = grad_sum1 + dot_t(grad_q, full_query)
        sent = lax.psum_scatter(via_kv.reshape(micros, -1, width), "seq", scatter_dimension=1, tiled=True)
    g_vectors = jnp.stack([g_qbias, g_vbias, g_obias, g_fgain, g_fshift, g_ubias, g_sgain, g_sshift])
    g_vectors = lanes(g_vectors.reshape(8, shares, own).transpose(1, 0, 2).astype(BF16))
    g_wide = lanes(g_ibias.reshape(shares, 1, own * per).astype(BF16))
    g_small = jnp.pad(jnp.concatenate([g_vectors, g_wide], axis=1), ((0, 0), (0, 7), (0, 0))).reshape(-1, 128)
    own_grads = scatter_all([g_outer, g_inner, g_output, g_query, g_key, g_value, g_small], 3)
    own_outer, own_inner, own_output, own_query, own_key, own_value, own_small = own_grads

    grad_x = grad_x.reshape(micros, rows, width) + sent.reshape(micros, rows, width).astype(F32)

    v_of = [own_small[i, :own] for i in range(8)]
    outputs = result.reshape(micros, rows, width)[None]
    return (
        outputs,
        grad_x[None],
        own_query,
        own_key,
        own_value,
        v_of[0],
        v_of[1],
        own_output,
        v_of[2],
        v_of[3],
        v_of[4],
        own_inner,
        own_small[8, : own * per],
        own_outer,
        v_of[5],
        v_of[6],
        v_of[7],
    )


def solution(mesh):
    act = P("dp", None, "seq", None)
    mat = P(BOTH, None)
    vec = P(BOTH)
    params = (mat, mat, mat, vec, vec, mat, vec, vec, vec, mat, vec, mat, vec, vec, vec)
    return jax.shard_map(
        on_device,
        mesh=mesh,
        in_specs=(act,) + params + (P("dp", None), act),
        out_specs=(act, act) + params,
        check_vma=False,
    )
```
